32 devices in a mesh: tp: 8 (over z, y), cp: 4 (over x, core).
Axes of the slice: x: 2, y: 2, z: 4, core: 2. Of those that a mesh axis runs over, the one named last changes fastest.
Arguments:
- x_in: bfloat16 [4, 512, 2048], P(None, 'cp')
- d_y: bfloat16 [4, 512, 2048], P(None, 'cp')
- key_mask: int32 [4, 512], P(None, 'cp')
- rel_bias: float32 [32, 32], P(None, 'tp')
- g_attn: float32 [2, 2048], replicated
- g_mlp: float32 [2, 2048], replicated
- w_q: bfloat16 [2, 2048, 2048], P(None, None, 'tp')
- w_k: bfloat16 [2, 2048, 2048], P(None, None, 'tp')
- w_v: bfloat16 [2, 2048, 2048], P(None, None, 'tp')
- w_o: bfloat16 [2, 2048, 2048], P(None, 'tp')
- w_gate: bfloat16 [2, 2048, 5120], P(None, None, 'tp')
- w_lin: bfloat16 [2, 2048, 5120], P(None, None, 'tp')
- w_out: bfloat16 [2, 5120, 2048], P(None, 'tp')
Outputs:
- output 1: bfloat16 [4, 512, 2048], P(None, 'cp')
- output 2: float32 [32, 32], P(None, 'tp')
- output 3: float32 [2, 2048], replicated
- output 4: float32 [2, 2048], replicated
- output 5: bfloat16 [2, 2048, 2048], P(None, None, 'tp')
- output 6: bfloat16 [2, 2048, 2048], P(None, None, 'tp')
- output 7: bfloat16 [2, 2048, 2048], P(None, None, 'tp')
- output 8: bfloat16 [2, 2048, 2048], P(None, 'tp')
- output 9: bfloat16 [2, 2048, 5120], P(None, None, 'tp')
- output 10: bfloat16 [2, 2048, 5120], P(None, None, 'tp')
- output 11: bfloat16 [2, 5120, 2048], P(None, 'tp')
All inputs are finite; a program needn't handle non-finite values.
Results may differ from the reference program's by a relative error of at most 0.02.
Values are sent between devices in bfloat16 or wider.
A program may use at most 1 GiB of HBM per device.

```python
import jax
import jax.numpy as jnp
from jax import lax

BATCH_SIZE = 4
SEQ_LEN = 512
D_MODEL = 2048
N_HEADS = 32
HEAD_DIM = 64
FF_DIM = 5120
N_LAYERS = 2
NUM_BUCKETS = 32
MAX_DISTANCE = 128
QUERY_ROWS = 128
NORM_EPS = 1e-6
MASK_NEG = -1e9


def rel_bucket(rel_pos):
    distance = jnp.minimum(jnp.abs(rel_pos), MAX_DISTANCE)
    distance_sq = distance * distance
    log_part = 8 + sum((distance_sq >= 64 * 2 ** power).astype(jnp.int32) for power in range(1, 8))
    return jnp.where(distance < 8, distance, log_part) + 16 * (rel_pos > 0).astype(jnp.int32)


def rms_scale(x_f, gain):
    inv_rms = lax.rsqrt(jnp.mean(x_f * x_f, axis=-1, keepdims=True) + NORM_EPS)
    return (x_f * inv_rms * gain).astype(jnp.bfloat16)


def mat_f32(lhs, rhs):
    return jnp.dot(lhs.astype(jnp.float32), rhs.astype(jnp.float32))


def attention(queries, key_rows, val_rows, rel_bias, key_add):
    q_f = queries.astype(jnp.float32)
    k_f = key_rows.astype(jnp.float32)
    v_f = val_rows.astype(jnp.float32)
    n_blocks = SEQ_LEN // QUERY_ROWS
    q_blocks = jnp.moveaxis(q_f.reshape(BATCH_SIZE, n_blocks, QUERY_ROWS, N_HEADS, HEAD_DIM), 1, 0)
    key_pos = jnp.arange(SEQ_LEN)
    bias_table = rel_bias.T

    def one_block(block_args):
        q_blk, start = block_args
        rel_pos = key_pos[None, :] - (start + jnp.arange(QUERY_ROWS))[:, None]
        bias = jnp.take(bias_table, rel_bucket(rel_pos), axis=1)
        scores = jnp.einsum('bqhd,bkhd->bhqk', q_blk, k_f) + bias[None] + key_add[:, None, None, :]
        probs = jax.nn.softmax(scores, axis=-1)
        return jnp.einsum('bhqk,bkhd->bqhd', probs, v_f)

    outs = lax.map(jax.checkpoint(one_block), (q_blocks, jnp.arange(n_blocks) * QUERY_ROWS))
    return jnp.moveaxis(outs, 0, 1).reshape(BATCH_SIZE, SEQ_LEN, N_HEADS * HEAD_DIM).astype(jnp.bfloat16)


def encoder_layer(hidden, weights, rel_bias, key_add):
    g_attn, g_mlp, w_q, w_k, w_v, w_o, w_gate, w_lin, w_out = weights
    head_shape = (BATCH_SIZE, SEQ_LEN, N_HEADS, HEAD_DIM)
    x_f = hidden.astype(jnp.float32)
    h_attn = rms_scale(x_f, g_attn)
    queries = mat_f32(h_attn, w_q).astype(jnp.bfloat16).reshape(head_shape)
    key_rows = mat_f32(h_attn, w_k).astype(jnp.bfloat16).reshape(head_shape)
    val_rows = mat_f32(h_attn, w_v).astype(jnp.bfloat16).reshape(head_shape)
    attn_flat = attention(queries, key_rows, val_rows, rel_bias, key_add)
    after_attn = (x_f + mat_f32(attn_flat, w_o)).astype(jnp.bfloat16)
    after_f = after_attn.astype(jnp.float32)
    h_mlp = rms_scale(after_f, g_mlp)
    gated = (jax.nn.gelu(mat_f32(h_mlp, w_gate), approximate=True) * mat_f32(h_mlp, w_lin)).astype(jnp.bfloat16)
    return (after_f + mat_f32(gated, w_out)).astype(jnp.bfloat16)


def setup_inputs(seed: int = 0) -> dict:
    base_key = jax.random.key(seed)
    sub_keys = jax.random.split(base_key, 13)
    width = N_HEADS * HEAD_DIM

    def normal(slot, shape, scale):
        return jax.random.normal(sub_keys[slot], shape, jnp.float32) * scale

    lengths = jax.random.randint(sub_keys[2], (BATCH_SIZE,), SEQ_LEN // 2, SEQ_LEN + 1)
    last_row = jnp.logical_and(jnp.arange(BATCH_SIZE) == BATCH_SIZE - 1, BATCH_SIZE > 1)
    lengths = jnp.where(last_row, SEQ_LEN // 2, lengths)
    key_mask = (jnp.arange(SEQ_LEN)[None, :] < lengths[:, None]).astype(jnp.int32)
    return {
        'x_in': normal(0, (BATCH_SIZE, SEQ_LEN, D_MODEL), 1.0).astype(jnp.bfloat16),
        'd_y': normal(1, (BATCH_SIZE, SEQ_LEN, D_MODEL), 1.0).astype(jnp.bfloat16),
        'key_mask': key_mask,
        'rel_bias': normal(3, (NUM_BUCKETS, N_HEADS), 1.0),
        'g_attn': 1.0 + normal(4, (N_LAYERS, D_MODEL), 0.3),
        'g_mlp': 1.0 + normal(5, (N_LAYERS, D_MODEL), 0.3),
        'w_q': normal(6, (N_LAYERS, D_MODEL, width), (D_MODEL * HEAD_DIM) ** -0.5).astype(jnp.bfloat16),
        'w_k': normal(7, (N_LAYERS, D_MODEL, width), D_MODEL ** -0.5).astype(jnp.bfloat16),
        'w_v': normal(8, (N_LAYERS, D_MODEL, width), D_MODEL ** -0.5).astype(jnp.bfloat16),
        'w_o': normal(9, (N_LAYERS, width, D_MODEL), width ** -0.5).astype(jnp.bfloat16),
        'w_gate': normal(10, (N_LAYERS, D_MODEL, FF_DIM), D_MODEL ** -0.5).astype(jnp.bfloat16),
        'w_lin': normal(11, (N_LAYERS, D_MODEL, FF_DIM), D_MODEL ** -0.5).astype(jnp.bfloat16),
        'w_out': normal(12, (N_LAYERS, FF_DIM, D_MODEL), FF_DIM ** -0.5).astype(jnp.bfloat16),
    }


def reference(x_in, d_y, key_mask, rel_bias, g_attn, g_mlp, w_q, w_k, w_v, w_o, w_gate, w_lin, w_out):
    key_add = jnp.where(key_mask > 0, 0.0, MASK_NEG).astype(jnp.float32)

    def forward(hidden, bias_tab, gain_a, gain_m, wq_all, wk_all, wv_all, wo_all, wg_all, wl_all, wf_all):
        def body(carry, weights):
            return encoder_layer(carry, weights, bias_tab, key_add), None
        final, _ = lax.scan(body, hidden, (gain_a, gain_m, wq_all, wk_all, wv_all, wo_all, wg_all, wl_all, wf_all))
        return final

    _, pull_back = jax.vjp(forward, x_in, rel_bias, g_attn, g_mlp, w_q, w_k, w_v, w_o, w_gate, w_lin, w_out)
    d_x, d_rel, d_gain_a, d_gain_m, d_wq, d_wk, d_wv, d_wo, d_wg, d_wl, d_wf = pull_back(d_y)
    return (d_x, d_rel, d_gain_a, d_gain_m, d_wq, d_wk, d_wv, d_wo, d_wg, d_wl, d_wf)
```

```python
import functools

import jax
import jax.numpy as jnp
from jax import lax
from jax.experimental import pallas as pl
from jax.experimental.pallas import tpu as pltpu
from jax.sharding import PartitionSpec as P

NORM_EPS = 1e-6
MASK_NEG = -1e9
BF16 = jnp.bfloat16
F32 = jnp.float32
VMEM = pltpu.VMEM
MESH = pl.DeviceIdType.MESH
HEAD_DIM = 64
VMEM_SPEC = pl.BlockSpec(memory_space=pltpu.VMEM)
SMEM_SPEC = pl.BlockSpec(memory_space=pltpu.SMEM)


def rel_bucket(rel_pos):
    distance = jnp.minimum(jnp.abs(rel_pos), 128)
    distance_sq = distance * distance
    log_part = 8 + sum((distance_sq >= 64 * 2 ** power).astype(jnp.int32) for power in range(1, 8))
    return jnp.where(distance < 8, distance, log_part) + 16 * (rel_pos > 0).astype(jnp.int32)


def dot_nt(a, b):
    return lax.dot_general(a, b, (((1,), (1,)), ((), ())), preferred_element_type=F32)


def dot_nn(a, b):
    return lax.dot_general(a, b, (((1,), (0,)), ((), ())), preferred_element_type=F32)


def dot_tn(a, b):
    return lax.dot_general(a, b, (((0,), (0,)), ((), ())), preferred_element_type=F32)


def stack_heads(block, heads):
    wide = block.astype(F32)
    lane_head = lax.broadcasted_iota(jnp.int32, block.shape, 1) // HEAD_DIM
    return jnp.concatenate([jnp.where(lane_head == h, wide, 0.0).astype(BF16) for h in range(heads)], axis=0)


def pick_heads(stacked, heads, rows):
    lane_head = lax.broadcasted_iota(jnp.int32, (rows, stacked.shape[1]), 1) // HEAD_DIM
    out = stacked[:rows]
    for h in range(1, heads):
        out = jnp.where(lane_head == h, stacked[h * rows:(h + 1) * rows], out)
    return out


def cp_places():
    me = lax.axis_index('cp')
    mate = me + 1 - 2 * lax.rem(me, 2)
    across = lax.rem(me + 2, 4)
    diagonal = lax.rem(mate + 2, 4)
    return me, mate, across, diagonal


def entry_barrier(axis, peers):
    barrier = pltpu.get_barrier_semaphore()
    for peer in peers:
        pl.semaphore_signal(barrier, inc=1, device_id={axis: peer}, device_id_type=MESH)
    pl.semaphore_wait(barrier, len(peers))


def attn_fwd_kernel(heads, q_ref, kv_ref, bias_ref, mask_ref, o_ref, all_ref, send, recv):
    batch, rows, width = q_ref.shape
    me, mate, across, _ = cp_places()
    entry_barrier('cp', (mate, across))

    def to_mate(b):
        return pltpu.make_async_remote_copy(src_ref=kv_ref.at[b], dst_ref=all_ref.at[b, me], send_sem=send.at[0, b], recv_sem=recv.at[0, b], device_id={'cp': mate}, device_id_type=MESH)

    def to_across(b):
        return pltpu.make_async_remote_copy(src_ref=kv_ref.at[b], dst_ref=all_ref.at[b, me], send_sem=send.at[1, b], recv_sem=recv.at[1, b], device_id={'cp': across}, device_id_type=MESH)

    def forward(b):
        return pltpu.make_async_remote_copy(src_ref=all_ref.at[b, across], dst_ref=all_ref.at[b, across], send_sem=send.at[2, b], recv_sem=recv.at[2, b], device_id={'cp': mate}, device_id_type=MESH)

    for b in range(batch):
        to_across(b).start()
        to_mate(b).start()

    def step(b, carry):
        to_across(b).wait_recv()
        forward(b).start()
        all_ref[b, me] = kv_ref[b]
        to_mate(b).wait_recv()
        forward(b).wait_recv()
        kv = all_ref[b].reshape(-1, 2 * width)
        stacked = stack_heads(q_ref[b], heads)
        scores = dot_nt(stacked, kv[:, :width]) + bias_ref[...] + mask_ref[b]
        top = jnp.max(scores, axis=1, keepdims=True)
        probs = jnp.exp(scores - top)
        total = jnp.sum(probs, axis=1, keepdims=True)
        out = dot_nn(probs.astype(BF16), kv[:, width:]) / total
        o_ref[b] = pick_heads(out, heads, rows).astype(BF16)
        return carry

    lax.fori_loop(0, batch, step, 0)

    def finish(b, carry):
        to_across(b).wait_send()
        to_mate(b).wait_send()
        forward(b).wait_send()
        return carry

    lax.fori_loop(0, batch, finish, 0)


def attn_fwd(q, kv, bias_rows, mask_rows, cp_size, cid):
    batch, rows, width = q.shape
    heads = width // HEAD_DIM
    return pl.pallas_call(
        functools.partial(attn_fwd_kernel, heads),
        out_shape=(jax.ShapeDtypeStruct(q.shape, BF16), jax.ShapeDtypeStruct((batch, cp_size, rows, 2 * width), BF16)),
        in_specs=[VMEM_SPEC] * 4,
        out_specs=(VMEM_SPEC, VMEM_SPEC),
        scratch_shapes=[pltpu.SemaphoreType.DMA((3, batch)), pltpu.SemaphoreType.DMA((3, batch))],
        compiler_params=pltpu.CompilerParams(collective_id=cid, has_side_effects=True, vmem_limit_bytes=32 * 2 ** 20),
        cost_estimate=pl.CostEstimate(flops=4 * 10 ** 9, bytes_accessed=6 * 10 ** 6, transcendentals=10 ** 6),
        name='attn_fwd',
    )(q, kv, bias_rows, mask_rows)


def attn_bwd_kernel(heads, qdo_ref, kv_ref, bias_r_ref, bias_c_ref, mask_r_ref, mask_c_ref, dq_ref, dkv_ref, ds_ref, all_ref, own_stats, all_stats, send, recv, send_st, recv_st):
    batch, rows, wide = qdo_ref.shape
    width = wide // 2
    n_blocks = kv_ref.shape[1]
    me, mate, across, diagonal = cp_places()
    entry_barrier('cp', (mate, across, diagonal))

    def to_mate(b):
        return pltpu.make_async_remote_copy(src_ref=qdo_ref.at[b], dst_ref=all_ref.at[b, me], send_sem=send.at[0, b], recv_sem=recv.at[0, b], device_id={'cp': mate}, device_id_type=MESH)

    def to_across(b):
        return pltpu.make_async_remote_copy(src_ref=qdo_ref.at[b], dst_ref=all_ref.at[b, me], send_sem=send.at[1, b], recv_sem=recv.at[1, b], device_id={'cp': across}, device_id_type=MESH)

    def forward(b):
        return pltpu.make_async_remote_copy(src_ref=all_ref.at[b, across], dst_ref=all_ref.at[b, across], send_sem=send.at[2, b], recv_sem=recv.at[2, b], device_id={'cp': mate}, device_id_type=MESH)

    def stats_to(which, b):
        peer = (mate, across, diagonal)[which]
        return pltpu.make_async_remote_copy(src_ref=own_stats.at[b], dst_ref=all_stats.at[b, me], send_sem=send_st.at[which, b], recv_sem=recv_st.at[which, b], device_id={'cp': peer}, device_id_type=MESH)

    for b in range(batch):
        to_across(b).start()
        to_mate(b).start()

    ds_ref[...] = jnp.zeros_like(ds_ref)

    def row_step(b, carry):
        kv = kv_ref[b].reshape(-1, wide)
        keys, vals = kv[:, :width], kv[:, width:]
        qdo = qdo_ref[b]
        all_ref[b, me] = qdo
        scores = dot_nt(stack_heads(qdo[:, :width], heads), keys) + bias_r_ref[...] + mask_r_ref[b]
        top = jnp.max(scores, axis=1, keepdims=True)
        unnorm = jnp.exp(scores - top)
        total = jnp.sum(unnorm, axis=1, keepdims=True)
        log_norm = top + jnp.log(total)
        probs = unnorm * (1.0 / total)
        d_probs = dot_nt(stack_heads(qdo[:, width:], heads), vals)
        row_dot = jnp.sum(probs * d_probs, axis=1, keepdims=True)
        lane = lax.broadcasted_iota(jnp.int32, (rows, rows), 1)
        table = jnp.zeros((rows, rows), F32)
        for h in range(heads):
            table = jnp.where(lane == h, log_norm[h * rows:(h + 1) * rows], table)
            table = jnp.where(lane == heads + h, row_dot[h * rows:(h + 1) * rows], table)
        stats = jnp.transpose(table)[:2 * heads]
        own_stats[b] = stats
        all_stats[b, me] = stats
        d_scores = probs * (d_probs - row_dot)
        ds_ref[...] += d_scores
        d_q = dot_nn(d_scores.astype(BF16), keys)
        dq_ref[b] = pick_heads(d_q, heads, rows).astype(BF16)
        for which in range(3):
            stats_to(which, b).start()
        to_across(b).wait_recv()
        forward(b).start()
        return carry

    lax.fori_loop(0, batch, row_step, 0)

    def col_step(b, carry):
        to_mate(b).wait_recv()
        forward(b).wait_recv()
        for which in range(3):
            stats_to(which, b).wait_recv()
        own = kv_ref[b, me]
        keys, vals = own[:, :width], own[:, width:]
        mask_col = mask_c_ref[b]

        def block(src, acc):
            d_k, d_v = acc
            qdo = all_ref[b, src]
            stats = all_stats[b, src]
            log_norm = jnp.concatenate([stats[h:h + 1] for h in range(heads)], axis=1)
            row_dot = jnp.concatenate([stats[heads + h:heads + h + 1] for h in range(heads)], axis=1)
            q_st = stack_heads(qdo[:, :width], heads)
            do_st = stack_heads(qdo[:, width:], heads)
            scores = dot_nt(keys, q_st) + bias_c_ref[src] + mask_col
            probs = jnp.exp(scores - log_norm)
            d_scores = probs * (dot_nt(vals, do_st) - row_dot)
            d_k = d_k + dot_nn(d_scores.astype(BF16), q_st)
            d_v = d_v + dot_nn(probs.astype(BF16), do_st)
            return d_k, d_v

        zero = jnp.zeros((rows, width), F32)
        d_k, d_v = lax.fori_loop(0, n_blocks, block, (zero, zero))
        dkv_ref[b] = jnp.concatenate([d_k, d_v], axis=1).astype(BF16)
        return carry

    lax.fori_loop(0, batch, col_step, 0)

    def finish(b, carry):
        to_across(b).wait_send()
        to_mate(b).wait_send()
        forward(b).wait_send()
        for which in range(3):
            stats_to(which, b).wait_send()
        return carry

    lax.fori_loop(0, batch, finish, 0)


def attn_bwd(qdo, kv_all, bias_rows, bias_cols, mask_rows, mask_cols, cid):
    batch, rows, wide = qdo.shape
    width = wide // 2
    heads = width // HEAD_DIM
    n_blocks = kv_all.shape[1]
    return pl.pallas_call(
        functools.partial(attn_bwd_kernel, heads),
        out_shape=(jax.ShapeDtypeStruct((batch, rows, width), BF16), jax.ShapeDtypeStruct((batch, rows, wide), BF16), jax.ShapeDtypeStruct((heads * rows, n_blocks * rows), F32)),
        in_specs=[VMEM_SPEC] * 6,
        out_specs=(VMEM_SPEC,) * 3,
        scratch_shapes=[
            pltpu.VMEM((batch, n_blocks, rows, wide), BF16),
            pltpu.VMEM((batch, 2 * heads, rows), F32),
            pltpu.VMEM((batch, n_blocks, 2 * heads, rows), F32),
            pltpu.SemaphoreType.DMA((3, batch)),
            pltpu.SemaphoreType.DMA((3, batch)),
            pltpu.SemaphoreType.DMA((3, batch)),
            pltpu.SemaphoreType.DMA((3, batch)),
        ],
        compiler_params=pltpu.CompilerParams(collective_id=cid, has_side_effects=True, vmem_limit_bytes=40 * 2 ** 20),
        cost_estimate=pl.CostEstimate(flops=10 * 10 ** 9, bytes_accessed=10 ** 7, transcendentals=2 * 10 ** 6),
        name='attn_bwd',
    )(qdo, kv_all, bias_rows, bias_cols, mask_rows, mask_cols)


def bias_grad_kernel(heads, n_buckets, pos_ref, ds0_ref, ds1_ref, out_ref):
    rows = ds0_ref.shape[0] // heads
    cols = ds0_ref.shape[1]
    rel = lax.broadcasted_iota(jnp.int32, (rows, cols), 1) - lax.broadcasted_iota(jnp.int32, (rows, cols), 0) - pos_ref[0]
    buckets = rel_bucket(rel)
    sums = [ds0_ref[h * rows:(h + 1) * rows] + ds1_ref[h * rows:(h + 1) * rows] for h in range(heads)]

    def step(k, carry):
        hit = buckets == k
        out_ref[k] = jnp.concatenate([jnp.sum(jnp.where(hit, part, 0.0), axis=0, keepdims=True) for part in sums], axis=0)
        return carry

    lax.fori_loop(0, n_buckets, step, 0)


def bias_grad(ds0, ds1, start, heads, n_buckets):
    out = pl.pallas_call(
        functools.partial(bias_grad_kernel, heads, n_buckets),
        out_shape=jax.ShapeDtypeStruct((n_buckets, heads, ds0.shape[1]), F32),
        in_specs=[SMEM_SPEC, VMEM_SPEC, VMEM_SPEC],
        out_specs=VMEM_SPEC,
        compiler_params=pltpu.CompilerParams(vmem_limit_bytes=16 * 2 ** 20),
        name='bias_grad',
    )(start.reshape(1), ds0, ds1)
    return jnp.sum(out, axis=-1)


def bias_from(rel_bias, rel):
    buckets = rel_bucket(rel)
    table = rel_bias.T
    shape = (table.shape[0],) + rel.shape
    out = jnp.zeros(shape, F32)
    for k in range(table.shape[1]):
        out = jnp.where((buckets == k)[None], table[:, k].reshape((-1,) + (1,) * rel.ndim), out)
    return out


def rms_parts(x_f, gain):
    inv_rms = lax.rsqrt(jnp.mean(x_f * x_f, axis=-1, keepdims=True) + NORM_EPS)
    return (x_f * inv_rms * gain).astype(BF16)


def rms_backward(d_norm, x_f, gain):
    inv_rms = lax.rsqrt(jnp.mean(x_f * x_f, axis=-1, keepdims=True) + NORM_EPS)
    normed = x_f * inv_rms
    d_gain = jnp.sum(d_norm * normed, axis=0)
    d_normed = d_norm * gain
    d_x = inv_rms * (d_normed - normed * jnp.mean(d_normed * normed, axis=-1, keepdims=True))
    return d_x, d_gain


def reduce_rows(partial):
    return lax.psum_scatter(partial, 'tp', scatter_dimension=0, tiled=True)


def gather_rows(shard):
    return lax.all_gather(shard, 'tp', axis=0, tiled=True)


def cp_sum(partial):
    own = lax.psum_scatter(partial, 'cp', scatter_dimension=0, tiled=True).astype(BF16)
    return lax.all_gather(own, 'cp', axis=0, tiled=True)


def solution(mesh):
    cp_size = mesh.shape['cp']
    tp_size = mesh.shape['tp']
    seq_spec = P(None, 'cp', None)
    col_spec = P(None, None, 'tp')
    row_spec = P(None, 'tp', None)
    weight_specs = (P(), P(), col_spec, col_spec, col_spec, row_spec, col_spec, col_spec, row_spec)

    def local_program(x_in, d_y, key_mask, rel_bias, g_attn, g_mlp, w_q, w_k, w_v, w_o, w_gate, w_lin, w_out):
        batch, rows, d_model = x_in.shape
        tokens = batch * rows
        n_layers = w_q.shape[0]
        n_buckets, heads = rel_bias.shape
        width = heads * HEAD_DIM
        cp_index = lax.axis_index('cp')
        tp_index = lax.axis_index('tp')
        seq = cp_size * rows
        start = (cp_index * rows).astype(jnp.int32)

        mask_all = lax.all_gather(key_mask, 'cp', axis=1, tiled=True)
        mask_rows = jnp.where(mask_all > 0, 0.0, MASK_NEG).astype(F32)[:, None, :]
        mask_cols = jnp.where(key_mask > 0, 0.0, MASK_NEG).astype(F32)[:, :, None]
        pos = jnp.arange(rows)
        bias_rows = bias_from(rel_bias, jnp.arange(seq)[None, :] - start - pos[:, None]).reshape(heads * rows, seq)
        rel_cols = start + pos[None, :, None] - (jnp.arange(cp_size) * rows)[:, None, None] - pos[None, None, :]
        bias_cols = jnp.transpose(bias_from(rel_bias, rel_cols), (1, 2, 0, 3)).reshape(cp_size, rows, heads * rows)

        def own_rows(full):
            return lax.dynamic_slice_in_dim(full, tp_index * (tokens // tp_size), tokens // tp_size, axis=0)

        x = x_in.reshape(tokens, d_model)
        x_s = own_rows(x)
        saved = []
        for l in range(n_layers):
            h = rms_parts(x.astype(F32), g_attn[l])
            q = jnp.dot(h, w_q[l], preferred_element_type=F32).astype(BF16)
            k = jnp.dot(h, w_k[l], preferred_element_type=F32).astype(BF16)
            v = jnp.dot(h, w_v[l], preferred_element_type=F32).astype(BF16)
            kv = jnp.concatenate([k, v], axis=1).reshape(batch, rows, 2 * width)
            o, kv_all = attn_fwd(q.reshape(batch, rows, width), kv, bias_rows, mask_rows, cp_size, 2 * l)
            o = o.reshape(tokens, width)
            x1_s = (x_s.astype(F32) + reduce_rows(jnp.dot(o, w_o[l], preferred_element_type=F32))).astype(BF16)
            x1 = gather_rows(x1_s)
            h2 = rms_parts(x1.astype(F32), g_mlp[l])
            gate = jnp.dot(h2, w_gate[l], preferred_element_type=F32)
            lin = jnp.dot(h2, w_lin[l], preferred_element_type=F32)
            u = (jax.nn.gelu(gate, approximate=True) * lin).astype(BF16)
            saved.append((x_s, h, q, kv_all, o, x1_s, h2, gate, lin, u))
            if l + 1 < n_layers:
                x_s = (x1_s.astype(F32) + reduce_rows(jnp.dot(u, w_out[l], preferred_element_type=F32))).astype(BF16)
                x = gather_rows(x_s)

        d = d_y.reshape(tokens, d_model)
        d_s = own_rows(d)
        big = [[None] * n_layers for _ in range(7)]
        gains = [[None] * n_layers for _ in range(2)]
        ds_all = []
        for l in reversed(range(n_layers)):
            x_s, h, q, kv_all, o, x1_s, h2, gate, lin, u = saved[l]
            big[6][l] = cp_sum(dot_tn(u, d))
            d_u = dot_nt(d, w_out[l]).astype(BF16).astype(F32)
            gelu_val, gelu_pull = jax.vjp(lambda g: jax.nn.gelu(g, approximate=True), gate)
            d_lin = (d_u * gelu_val).astype(BF16)
            d_gate = gelu_pull(d_u * lin)[0].astype(BF16)
            big[4][l] = cp_sum(dot_tn(h2, d_gate))
            big[5][l] = cp_sum(dot_tn(h2, d_lin))
            dh2_s = reduce_rows(dot_nt(d_gate, w_gate[l]) + dot_nt(d_lin, w_lin[l]))
            d_mid, gains[1][l] = rms_backward(dh2_s, x1_s.astype(F32), g_mlp[l])
            dm_s = (d_mid + d_s.astype(F32)).astype(BF16)
            dm = gather_rows(dm_s)
            big[3][l] = cp_sum(dot_tn(o, dm))
            d_o = dot_nt(dm, w_o[l]).astype(BF16)
            qdo = jnp.concatenate([q, d_o], axis=1).reshape(batch, rows, 2 * width)
            d_q, d_kv, ds = attn_bwd(qdo, kv_all, bias_rows, bias_cols, mask_rows, mask_cols, 2 * l + 1)
            ds_all.append(ds)
            d_q = d_q.reshape(tokens, width)
            d_kv = d_kv.reshape(tokens, 2 * width)
            d_k, d_v = d_kv[:, :width], d_kv[:, width:]
            big[0][l] = cp_sum(dot_tn(h, d_q))
            big[1][l] = cp_sum(dot_tn(h, d_k))
            big[2][l] = cp_sum(dot_tn(h, d_v))
            dh_s = reduce_rows(dot_nt(d_q, w_q[l]) + dot_nt(d_k, w_k[l]) + dot_nt(d_v, w_v[l]))
            d_x, gains[0][l] = rms_backward(dh_s, x_s.astype(F32), g_attn[l])
            d_s = (d_x + dm_s.astype(F32)).astype(BF16)
            d = gather_rows(d_s)

        d_bias = bias_grad(ds_all[0], ds_all[1], start, heads, n_buckets)
        slots = jnp.zeros((tp_size, n_buckets * heads), F32)
        slots = lax.dynamic_update_slice(slots, d_bias.reshape(1, -1), (tp_index, jnp.int32(0)))
        small = lax.psum(jnp.concatenate([jnp.stack(gains[0]).reshape(-1), jnp.stack(gains[1]).reshape(-1), slots.reshape(-1)]), ('tp', 'cp'))
        n_gain = n_layers * d_model
        d_g_attn = small[:n_gain].reshape(n_layers, d_model)
        d_g_mlp = small[n_gain:2 * n_gain].reshape(n_layers, d_model)
        d_rel = lax.dynamic_slice(small[2 * n_gain:].reshape(tp_size, -1), (tp_index, jnp.int32(0)), (1, n_buckets * heads)).reshape(n_buckets, heads)
        return (d.reshape(batch, rows, d_model), d_rel, d_g_attn, d_g_mlp) + tuple(jnp.stack(parts) for parts in big)

    return jax.shard_map(local_program, mesh=mesh, in_specs=(seq_spec, seq_spec, P(None, 'cp'), P(None, 'tp')) + weight_specs, out_specs=(seq_spec, P(None, 'tp')) + weight_specs, check_vma=False)
```

```python
import functools

import jax
import jax.numpy as jnp
from jax import lax
from jax.experimental import pallas as pl
from jax.experimental.pallas import tpu as pltpu
from jax.sharding import PartitionSpec as P

NORM_EPS = 1e-6
MASK_NEG = -1e9
BF16 = jnp.bfloat16
F32 = jnp.float32
VMEM = pltpu.VMEM
MESH = pl.DeviceIdType.MESH
HEAD_DIM = 64
VMEM_SPEC = pl.BlockSpec(memory_space=pltpu.VMEM)
SMEM_SPEC = pl.BlockSpec(memory_space=pltpu.SMEM)


def rel_bucket(rel_pos):
    distance = jnp.minimum(jnp.abs(rel_pos), 128)
    distance_sq = distance * distance
    log_part = 8 + sum((distance_sq >= 64 * 2 ** power).astype(jnp.int32) for power in range(1, 8))
    return jnp.where(distance < 8, distance, log_part) + 16 * (rel_pos > 0).astype(jnp.int32)


def dot_nt(a, b):
    return lax.dot_general(a, b, (((1,), (1,)), ((), ())), preferred_element_type=F32)


def dot_nn(a, b):
    return lax.dot_general(a, b, (((1,), (0,)), ((), ())), preferred_element_type=F32)


def dot_tn(a, b):
    return lax.dot_general(a, b, (((0,), (0,)), ((), ())), preferred_element_type=F32)


def stack_heads(block, heads):
    wide = block.astype(F32)
    lane_head = lax.broadcasted_iota(jnp.int32, block.shape, 1) // HEAD_DIM
    return jnp.concatenate([jnp.where(lane_head == h, wide, 0.0).astype(BF16) for h in range(heads)], axis=0)


def pick_heads(stacked, heads, rows):
    lane_head = lax.broadcasted_iota(jnp.int32, (rows, stacked.shape[1]), 1) // HEAD_DIM
    out = stacked[:rows]
    for h in range(1, heads):
        out = jnp.where(lane_head == h, stacked[h * rows:(h + 1) * rows], out)
    return out


def cp_places():
    me = lax.axis_index('cp')
    mate = me + 1 - 2 * lax.rem(me, 2)
    across = lax.rem(me + 2, 4)
    diagonal = lax.rem(mate + 2, 4)
    return me, mate, across, diagonal


def entry_barrier(axis, peers):
    barrier = pltpu.get_barrier_semaphore()
    for peer in peers:
        pl.semaphore_signal(barrier, inc=1, device_id={axis: peer}, device_id_type=MESH)
    pl.semaphore_wait(barrier, len(peers))


def attn_fwd_kernel(heads, q_ref, kv_ref, bias_ref, mask_ref, o_ref, all_ref, send, recv):
    batch, rows, width = q_ref.shape
    me, mate, across, _ = cp_places()
    entry_barrier('cp', (mate, across))

    def to_mate(b):
        return pltpu.make_async_remote_copy(src_ref=kv_ref.at[b], dst_ref=all_ref.at[b, me], send_sem=send.at[0, b], recv_sem=recv.at[0, b], device_id={'cp': mate}, device_id_type=MESH)

    def to_across(b):
        return pltpu.make_async_remote_copy(src_ref=kv_ref.at[b], dst_ref=all_ref.at[b, me], send_sem=send.at[1, b], recv_sem=recv.at[1, b], device_id={'cp': across}, device_id_type=MESH)

    def forward(b):
        return pltpu.make_async_remote_copy(src_ref=all_ref.at[b, across], dst_ref=all_ref.at[b, across], send_sem=send.at[2, b], recv_sem=recv.at[2, b], device_id={'cp': mate}, device_id_type=MESH)

    for b in range(batch):
        to_across(b).start()
        to_mate(b).start()

    def step(b, carry):
        to_across(b).wait_recv()
        forward(b).start()
        all_ref[b, me] = kv_ref[b]
        to_mate(b).wait_recv()
        forward(b).wait_recv()
        kv = all_ref[b].reshape(-1, 2 * width)
        stacked = stack_heads(q_ref[b], heads)
        scores = dot_nt(stacked, kv[:, :width]) + bias_ref[...] + mask_ref[b]
        top = jnp.max(scores, axis=1, keepdims=True)
        probs = jnp.exp(scores - top)
        total = jnp.sum(probs, axis=1, keepdims=True)
        out = dot_nn(probs.astype(BF16), kv[:, width:]) / total
        o_ref[b] = pick_heads(out, heads, rows).astype(BF16)
        return carry

    lax.fori_loop(0, batch, step, 0)

    def finish(b, carry):
        to_across(b).wait_send()
        to_mate(b).wait_send()
        forward(b).wait_send()
        return carry

    lax.fori_loop(0, batch, finish, 0)


def attn_fwd(q, kv, bias_rows, mask_rows, cp_size, cid):
    batch, rows, width = q.shape
    heads = width // HEAD_DIM
    return pl.pallas_call(
        functools.partial(attn_fwd_kernel, heads),
        out_shape=(jax.ShapeDtypeStruct(q.shape, BF16), jax.ShapeDtypeStruct((batch, cp_size, rows, 2 * width), BF16)),
        in_specs=[VMEM_SPEC] * 4,
        out_specs=(VMEM_SPEC, VMEM_SPEC),
        scratch_shapes=[pltpu.SemaphoreType.DMA((3, batch)), pltpu.SemaphoreType.DMA((3, batch))],
        compiler_params=pltpu.CompilerParams(collective_id=cid, has_side_effects=True, vmem_limit_bytes=32 * 2 ** 20),
        cost_estimate=pl.CostEstimate(flops=4 * 10 ** 9, bytes_accessed=6 * 10 ** 6, transcendentals=10 ** 6),
        name='attn_fwd',
    )(q, kv, bias_rows, mask_rows)


def attn_bwd_kernel(heads, qdo_ref, kv_ref, bias_r_ref, bias_c_ref, mask_r_ref, mask_c_ref, dq_ref, dkv_ref, ds_ref, all_ref, own_stats, all_stats, send, recv, send_st, recv_st):
    batch, rows, wide = qdo_ref.shape
    width = wide // 2
    n_blocks = kv_ref.shape[1]
    me, mate, across, diagonal = cp_places()
    entry_barrier('cp', (mate, across, diagonal))

    def to_mate(b):
        return pltpu.make_async_remote_copy(src_ref=qdo_ref.at[b], dst_ref=all_ref.at[b, me], send_sem=send.at[0, b], recv_sem=recv.at[0, b], device_id={'cp': mate}, device_id_type=MESH)

    def to_across(b):
        return pltpu.make_async_remote_copy(src_ref=qdo_ref.at[b], dst_ref=all_ref.at[b, me], send_sem=send.at[1, b], recv_sem=recv.at[1, b], device_id={'cp': across}, device_id_type=MESH)

    def forward(b):
        return pltpu.make_async_remote_copy(src_ref=all_ref.at[b, across], dst_ref=all_ref.at[b, across], send_sem=send.at[2, b], recv_sem=recv.at[2, b], device_id={'cp': mate}, device_id_type=MESH)

    def stats_to(which, b):
        peer = (mate, across, diagonal)[which]
        return pltpu.make_async_remote_copy(src_ref=own_stats.at[b], dst_ref=all_stats.at[b, me], send_sem=send_st.at[which, b], recv_sem=recv_st.at[which, b], device_id={'cp': peer}, device_id_type=MESH)

    for b in range(batch):
        to_across(b).start()
        to_mate(b).start()

    ds_ref[...] = jnp.zeros_like(ds_ref)

    def row_step(b, carry):
        kv = kv_ref[b].reshape(-1, wide)
        keys, vals = kv[:, :width], kv[:, width:]
        qdo = qdo_ref[b]
        all_ref[b, me] = qdo
        scores = dot_nt(stack_heads(qdo[:, :width], heads), keys) + bias_r_ref[...] + mask_r_ref[b]
        top = jnp.max(scores, axis=1, keepdims=True)
        unnorm = jnp.exp(scores - top)
        total = jnp.sum(unnorm, axis=1, keepdims=True)
        log_norm = top + jnp.log(total)
        probs = unnorm * (1.0 / total)
        d_probs = dot_nt(stack_heads(qdo[:, width:], heads), vals)
        row_dot = jnp.sum(probs * d_probs, axis=1, keepdims=True)
        lane = lax.broadcasted_iota(jnp.int32, (rows, rows), 1)
        table = jnp.zeros((rows, rows), F32)
        for h in range(heads):
            table = jnp.where(lane == h, log_norm[h * rows:(h + 1) * rows], table)
            table = jnp.where(lane == heads + h, row_dot[h * rows:(h + 1) * rows], table)
        stats = jnp.transpose(table)[:2 * heads]
        own_stats[b] = stats
        all_stats[b, me] = stats
        d_scores = probs * (d_probs - row_dot)
        ds_ref[...] += d_scores
        d_q = dot_nn(d_scores.astype(BF16), keys)
        dq_ref[b] = pick_heads(d_q, heads, rows).astype(BF16)
        for which in range(3):
            stats_to(which, b).start()
        to_across(b).wait_recv()
        forward(b).start()
        return carry

    lax.fori_loop(0, batch, row_step, 0)

    def col_step(b, carry):
        to_mate(b).wait_recv()
        forward(b).wait_recv()
        for which in range(3):
            stats_to(which, b).wait_recv()
        own = kv_ref[b, me]
        keys, vals = own[:, :width], own[:, width:]
        mask_col = mask_c_ref[b]

        def block(src, acc):
            d_k, d_v = acc
            qdo = all_ref[b, src]
            stats = all_stats[b, src]
            log_norm = jnp.concatenate([stats[h:h + 1] for h in range(heads)], axis=1)
            row_dot = jnp.concatenate([stats[heads + h:heads + h + 1] for h in range(heads)], axis=1)
            q_st = stack_heads(qdo[:, :width], heads)
            do_st = stack_heads(qdo[:, width:], heads)
            scores = dot_nt(keys, q_st) + bias_c_ref[src] + mask_col
            probs = jnp.exp(scores - log_norm)
            d_scores = probs * (dot_nt(vals, do_st) - row_dot)
            d_k = d_k + dot_nn(d_scores.astype(BF16), q_st)
            d_v = d_v + dot_nn(probs.astype(BF16), do_st)
            return d_k, d_v

        zero = jnp.zeros((rows, width), F32)
        d_k, d_v = lax.fori_loop(0, n_blocks, block, (zero, zero))
        dkv_ref[b] = jnp.concatenate([d_k, d_v], axis=1).astype(BF16)
        return carry

    lax.fori_loop(0, batch, col_step, 0)

    def finish(b, carry):
        to_across(b).wait_send()
        to_mate(b).wait_send()
        forward(b).wait_send()
        for which in range(3):
            stats_to(which, b).wait_send()
        return carry

    lax.fori_loop(0, batch, finish, 0)


def attn_bwd(qdo, kv_all, bias_rows, bias_cols, mask_rows, mask_cols, cid):
    batch, rows, wide = qdo.shape
    width = wide // 2
    heads = width // HEAD_DIM
    n_blocks = kv_all.shape[1]
    return pl.pallas_call(
        functools.partial(attn_bwd_kernel, heads),
        out_shape=(jax.ShapeDtypeStruct((batch, rows, width), BF16), jax.ShapeDtypeStruct((batch, rows, wide), BF16), jax.ShapeDtypeStruct((heads * rows, n_blocks * rows), F32)),
        in_specs=[VMEM_SPEC] * 6,
        out_specs=(VMEM_SPEC,) * 3,
        scratch_shapes=[
            pltpu.VMEM((batch, n_blocks, rows, wide), BF16),
            pltpu.VMEM((batch, 2 * heads, rows), F32),
            pltpu.VMEM((batch, n_blocks, 2 * heads, rows), F32),
            pltpu.SemaphoreType.DMA((3, batch)),
            pltpu.SemaphoreType.DMA((3, batch)),
            pltpu.SemaphoreType.DMA((3, batch)),
            pltpu.SemaphoreType.DMA((3, batch)),
        ],
        compiler_params=pltpu.CompilerParams(collective_id=cid, has_side_effects=True, vmem_limit_bytes=40 * 2 ** 20),
        cost_estimate=pl.CostEstimate(flops=10 * 10 ** 9, bytes_accessed=10 ** 7, transcendentals=2 * 10 ** 6),
        name='attn_bwd',
    )(qdo, kv_all, bias_rows, bias_cols, mask_rows, mask_cols)


def bias_grad_kernel(heads, n_buckets, pos_ref, ds0_ref, ds1_ref, out_ref):
    rows = ds0_ref.shape[0] // heads
    cols = ds0_ref.shape[1]
    rel = lax.broadcasted_iota(jnp.int32, (rows, cols), 1) - lax.broadcasted_iota(jnp.int32, (rows, cols), 0) - pos_ref[0]
    buckets = rel_bucket(rel)
    sums = [ds0_ref[h * rows:(h + 1) * rows] + ds1_ref[h * rows:(h + 1) * rows] for h in range(heads)]

    def step(k, carry):
        hit = buckets == k
        out_ref[k] = jnp.concatenate([jnp.sum(jnp.where(hit, part, 0.0), axis=0, keepdims=True) for part in sums], axis=0)
        return carry

    lax.fori_loop(0, n_buckets, step, 0)


def bias_grad(ds0, ds1, start, heads, n_buckets):
    out = pl.pallas_call(
        functools.partial(bias_grad_kernel, heads, n_buckets),
        out_shape=jax.ShapeDtypeStruct((n_buckets, heads, ds0.shape[1]), F32),
        in_specs=[SMEM_SPEC, VMEM_SPEC, VMEM_SPEC],
        out_specs=VMEM_SPEC,
        compiler_params=pltpu.CompilerParams(vmem_limit_bytes=16 * 2 ** 20),
        name='bias_grad',
    )(start.reshape(1), ds0, ds1)
    return jnp.sum(out, axis=-1)


def bias_from(rel_bias, rel):
    buckets = rel_bucket(rel)
    table = rel_bias.T
    shape = (table.shape[0],) + rel.shape
    out = jnp.zeros(shape, F32)
    for k in range(table.shape[1]):
        out = jnp.where((buckets == k)[None], table[:, k].reshape((-1,) + (1,) * rel.ndim), out)
    return out


def rms_parts(x_f, gain):
    inv_rms = lax.rsqrt(jnp.mean(x_f * x_f, axis=-1, keepdims=True) + NORM_EPS)
    return (x_f * inv_rms * gain).astype(BF16)


def rms_backward(d_norm, x_f, gain):
    inv_rms = lax.rsqrt(jnp.mean(x_f * x_f, axis=-1, keepdims=True) + NORM_EPS)
    normed = x_f * inv_rms
    d_gain = jnp.sum(d_norm * normed, axis=0)
    d_normed = d_norm * gain
    d_x = inv_rms * (d_normed - normed * jnp.mean(d_normed * normed, axis=-1, keepdims=True))
    return d_x, d_gain


def tp_places():
    me = lax.axis_index('tp')
    z, y = me // 2, lax.rem(me, 2)
    return me, z, y


def rsag_kernel(cfg, *refs):
    n_mat, trans, layer, is_rms, n_big, n_small = cfg
    it = iter(refs)
    take = lambda n: [next(it) for _ in range(n)]
    acts, weights = take(n_mat), take(n_mat)
    res_ref = next(it)
    xs_ref, gain_ref = take(2) if is_rms else (None, None)
    bigs, smalls = take(n_big), take(n_small)
    shard_ref, full_ref = take(2)
    dgain_ref = next(it) if is_rms else None
    bigs_g, smalls_g = take(n_big), take(n_small)
    w_bufs = take(n_mat)
    part, from_y, from_z, w_sem, ry_s, ry_r, rz_s, rz_r, gz_s, gz_r, gy_s, gy_r, x_s, x_r = take(14)
    batch, _, _, seg, d_model = part.shape
    half = d_model // 2
    me, z, y = tp_places()
    my_seg = y * 4 + z
    pair = me + 1 - 2 * y
    z_peer = [2 * lax.rem(z + j, 4) + y for j in range(4)]
    cp_me, mate, across, diagonal = cp_places()
    core = lax.rem(cp_me, 2)

    loads = [pltpu.make_async_copy(w.at[layer], buf, w_sem.at[i]) for i, (w, buf) in enumerate(zip(weights, w_bufs))]
    for load in loads:
        load.start()

    barrier = pltpu.get_barrier_semaphore()
    for peer in [pair] + z_peer[1:]:
        pl.semaphore_signal(barrier, inc=1, device_id={'tp': peer}, device_id_type=MESH)
    n_peers = 4
    if n_big + n_small:
        n_peers = 7
        for peer in (mate, across, diagonal):
            pl.semaphore_signal(barrier, inc=1, device_id={'cp': peer}, device_id_type=MESH)
    pl.semaphore_wait(barrier, n_peers)

    def remote(src, dst, send, recv, axis, peer):
        return pltpu.make_async_remote_copy(src_ref=src, dst_ref=dst, send_sem=send, recv_sem=recv, device_id={axis: peer}, device_id_type=MESH)

    def big_copy(i, r):
        peer = (mate, across, diagonal)[r]
        want = core if r == 1 else 1 - core
        src = bigs[i].at[:, pl.ds(pl.multiple_of(want * half, half), half)]
        return remote(src, bigs_g[i].at[r], x_s.at[i, r], x_r.at[i, r], 'cp', peer)

    def small_copy(i, r):
        src = smalls[i] if r < 2 else smalls_g[i].at[1]
        peer = across if r == 1 else mate
        k = n_big + i
        return remote(src, smalls_g[i].at[r], x_s.at[k, r], x_r.at[k, r], 'cp', peer)

    for i in range(n_small):
        small_copy(i, 1).start()
        small_copy(i, 0).start()
    for i in range(n_big):
        for r in (1, 2, 0):
            big_copy(i, r).start()
    for load in loads:
        load.wait()
    if is_rms:
        dgain_ref[...] = jnp.zeros_like(dgain_ref)

    def y_sum(b):
        return remote(part.at[b, 1 - y], from_y.at[b], ry_s.at[b], ry_r.at[b], 'tp', pair)

    def z_sum(b, j):
        return remote(part.at[b, y, lax.rem(z + j, 4)], from_z.at[b, j - 1], rz_s.at[b, j - 1], rz_r.at[b, j - 1], 'tp', z_peer[j])

    def z_gather(b, j):
        return remote(full_ref.at[b, my_seg], full_ref.at[b, my_seg], gz_s.at[b, j - 1], gz_r.at[b, j - 1], 'tp', z_peer[j])

    def y_gather(b, j):
        seg_j = y * 4 + lax.rem(z - j + 4, 4)
        return remote(full_ref.at[b, seg_j], full_ref.at[b, seg_j], gy_s.at[b, j], gy_r.at[b, j], 'tp', pair)

    def stage0(b):
        total = None
        for a, w, t in zip(acts, w_bufs, trans):
            prod = dot_nt(a[b], w[...]) if t else dot_nn(a[b], w[...])
            total = prod if total is None else total + prod
        part[b] = total.reshape(2, 4, seg, d_model)
        y_sum(b).start()

    def stage1(b):
        y_sum(b).wait_recv()
        part[b, y] = part[b, y] + from_y[b]
        for j in (2, 1, 3):
            z_sum(b, j).start()

    def stage2(b):
        for j in (1, 2, 3):
            z_sum(b, j).wait_recv()
        total = part[b, y, z] + from_z[b, 0] + from_z[b, 1] + from_z[b, 2]
        res = res_ref[b].astype(F32)
        if is_rms:
            d_norm = total.astype(BF16).astype(F32)
            x_f = xs_ref[b].astype(F32)
            inv_rms = lax.rsqrt(jnp.mean(x_f * x_f, axis=-1, keepdims=True) + NORM_EPS)
            normed = x_f * inv_rms
            dgain_ref[...] += jnp.sum(d_norm * normed, axis=0, keepdims=True)
            d_normed = d_norm * gain_ref[...]
            total = inv_rms * (d_normed - normed * jnp.mean(d_normed * normed, axis=-1, keepdims=True))
        out = (res + total).astype(BF16)
        full_ref[b, my_seg] = out
        shard_ref[b] = out
        for j in (2, 1, 3):
            z_gather(b, j).start()
        y_gather(b, 0).start()

    def stage3(b):
        for j in (1, 2, 3):
            z_gather(b, j).wait_recv()
            y_gather(b, j).start()

    def slot_step(slot, carry):
        for k, stage in enumerate((stage0, stage1, stage2, stage3)):
            @pl.when(jnp.logical_and(slot >= k, slot < batch + k))
            def _():
                stage(slot - k)
        return carry

    lax.fori_loop(0, batch + 3, slot_step, 0)

    for i in range(n_small):
        small_copy(i, 1).wait_recv()
        small_copy(i, 2).start()

    def finish(b, carry):
        for j in range(4):
            y_gather(b, j).wait_recv()
            y_gather(b, j).wait_send()
        y_sum(b).wait_send()
        for j in (1, 2, 3):
            z_sum(b, j).wait_send()
            z_gather(b, j).wait_send()
        return carry

    lax.fori_loop(0, batch, finish, 0)
    for i in range(n_small):
        small_copy(i, 0).wait_recv()
        small_copy(i, 2).wait_recv()
        for r in range(3):
            small_copy(i, r).wait_send()
    for i in range(n_big):
        for r in range(3):
            big_copy(i, r).wait()


def rsag(acts, weights, trans, layer, res, cid, rms=None, bigs=(), smalls=()):
    batch, rows, _ = acts[0].shape
    seg, d_model = res.shape[1:]
    n_tp = rows // seg
    is_rms = rms is not None
    any_spec = pl.BlockSpec(memory_space=pl.ANY)
    dma = pltpu.SemaphoreType.DMA
    outs = [jax.ShapeDtypeStruct(res.shape, BF16), jax.ShapeDtypeStruct((batch, n_tp, seg, d_model), BF16)]
    if is_rms:
        outs.append(jax.ShapeDtypeStruct((1, d_model), F32))
    n_vmem = len(outs)
    outs += [jax.ShapeDtypeStruct((3, a.shape[0], a.shape[1] // 2), BF16) for a in bigs]
    outs += [jax.ShapeDtypeStruct((3,) + a.shape, BF16) for a in smalls]
    n_x = len(bigs) + len(smalls)
    result = pl.pallas_call(
        functools.partial(rsag_kernel, (len(acts), trans, layer, is_rms, len(bigs), len(smalls))),
        out_shape=tuple(outs),
        in_specs=[VMEM_SPEC] * len(acts) + [any_spec] * len(weights) + [VMEM_SPEC] * (3 if is_rms else 1) + [any_spec] * n_x,
        out_specs=tuple([VMEM_SPEC] * n_vmem + [any_spec] * n_x),
        scratch_shapes=[pltpu.VMEM(w.shape[1:], BF16) for w in weights] + [
            pltpu.VMEM((batch, 2, 4, seg, d_model), F32),
            pltpu.VMEM((batch, 4, seg, d_model), F32),
            pltpu.VMEM((batch, 3, seg, d_model), F32),
            dma((len(acts),)),
            dma((batch,)), dma((batch,)),
            dma((batch, 3)), dma((batch, 3)),
            dma((batch, 3)), dma((batch, 3)),
            dma((batch, 4)), dma((batch, 4)),
            dma((max(n_x, 1), 3)), dma((max(n_x, 1), 3)),
        ],
        compiler_params=pltpu.CompilerParams(collective_id=cid, has_side_effects=True, vmem_limit_bytes=40 * 2 ** 20),
        cost_estimate=pl.CostEstimate(flops=4 * 10 ** 10, bytes_accessed=10 ** 7, transcendentals=0),
        name='rsag',
    )(*acts, *weights, res, *(rms or ()), *bigs, *smalls)
    shard, full = result[:2]
    full = full.reshape(batch * rows, d_model)
    d_gain = result[2][0] if is_rms else None
    return shard, full, d_gain, list(result[n_vmem:n_vmem + len(bigs)]), list(result[n_vmem + len(bigs):])


def solution(mesh):
    cp_size = mesh.shape['cp']
    tp_size = mesh.shape['tp']
    seq_spec = P(None, 'cp', None)
    col_spec = P(None, None, 'tp')
    row_spec = P(None, 'tp', None)
    weight_specs = (P(), P(), col_spec, col_spec, col_spec, row_spec, col_spec, col_spec, row_spec)

    def local_program(x_in, d_y, key_mask, rel_bias, g_attn, g_mlp, w_q, w_k, w_v, w_o, w_gate, w_lin, w_out):
        batch, rows, d_model = x_in.shape
        tokens = batch * rows
        n_layers = w_q.shape[0]
        n_buckets, heads = rel_bias.shape
        width = heads * HEAD_DIM
        cp_index = lax.axis_index('cp')
        tp_index = lax.axis_index('tp')
        core = lax.rem(cp_index, 2)
        half = d_model // 2
        seg = rows // tp_size
        my_seg = lax.rem(tp_index, 2) * 4 + tp_index // 2
        seq = cp_size * rows
        start = (cp_index * rows).astype(jnp.int32)

        mask_all = lax.all_gather(key_mask, 'cp', axis=1, tiled=True)
        mask_rows = jnp.where(mask_all > 0, 0.0, MASK_NEG).astype(F32)[:, None, :]
        mask_cols = jnp.where(key_mask > 0, 0.0, MASK_NEG).astype(F32)[:, :, None]
        pos = jnp.arange(rows)
        bias_rows = bias_from(rel_bias, jnp.arange(seq)[None, :] - start - pos[:, None]).reshape(heads * rows, seq)
        rel_cols = start + pos[None, :, None] - (jnp.arange(cp_size) * rows)[:, None, None] - pos[None, None, :]
        bias_cols = jnp.transpose(bias_from(rel_bias, rel_cols), (1, 2, 0, 3)).reshape(cp_size, rows, heads * rows)

        def own_rows(full):
            return lax.dynamic_slice_in_dim(full, my_seg * seg, seg, axis=1)

        def rows3(flat):
            return flat.reshape(batch, rows, -1)

        def own_half(flat):
            return lax.dynamic_slice_in_dim(flat, core * half, half, axis=1)

        def wide_rows(big, small):
            (own, others), (s_own, s_others) = big, small
            return (dot_tn(own_half(own), s_own) + dot_tn(others.reshape(-1, half), s_others.reshape(-1, s_own.shape[1]))).astype(BF16)

        def wide_cols(small, big):
            (own, others), (s_own, s_others) = big, small
            return (dot_tn(s_own, own_half(own)) + dot_tn(s_others.reshape(-1, s_own.shape[1]), others.reshape(-1, half))).astype(BF16)

        cores = [[0, 1], [2, 3]]

        def join_rows(part):
            return lax.all_gather(part, 'cp', axis=0, tiled=True, axis_index_groups=cores)

        def join_cols(part):
            both = lax.all_gather(part, 'cp', axis=0, tiled=False, axis_index_groups=cores)
            return jnp.transpose(both, (1, 0, 2)).reshape(part.shape[0], 2 * part.shape[1])

        def norm(flat, gain):
            return rms_parts(flat.astype(F32), gain)

        def project(h, l):
            q = jnp.dot(h, w_q[l], preferred_element_type=F32).astype(BF16)
            k = jnp.dot(h, w_k[l], preferred_element_type=F32).astype(BF16)
            v = jnp.dot(h, w_v[l], preferred_element_type=F32).astype(BF16)
            return q, rows3(jnp.concatenate([k, v], axis=1))

        def mlp(h2, l):
            gate = jnp.dot(h2, w_gate[l], preferred_element_type=F32)
            lin = jnp.dot(h2, w_lin[l], preferred_element_type=F32)
            return gate, lin, (jax.nn.gelu(gate, approximate=True) * lin).astype(BF16)

        def mlp_grads(d, gate, lin, l):
            d_u = dot_nt(d, w_out[l]).astype(BF16).astype(F32)
            gelu_val, gelu_pull = jax.vjp(lambda g: jax.nn.gelu(g, approximate=True), gate)
            return gelu_pull(d_u * lin)[0].astype(BF16), (d_u * gelu_val).astype(BF16)

        def mlp_back(d_gate, d_lin, x1_s, d_s, l, cid, bigs, smalls):
            return rsag([rows3(d_gate), rows3(d_lin)], [w_gate, w_lin], (True, True), l, d_s, cid, (x1_s, g_mlp[l][None]), bigs, smalls)

        def attn_grads(q, kv_all, dm, l, cid):
            d_o = dot_nt(dm, w_o[l]).astype(BF16)
            d_q, d_kv, ds = attn_bwd(rows3(jnp.concatenate([q, d_o], axis=1)), kv_all, bias_rows, bias_cols, mask_rows, mask_cols, cid)
            d_k, d_v = d_kv[:, :, :width], d_kv[:, :, width:]
            d_qkv = jnp.concatenate([d_q, d_kv], axis=2).reshape(tokens, 3 * width)
            return [d_q, d_k, d_v], d_qkv, ds

        x = x_in.reshape(tokens, d_model)
        d1 = d_y.reshape(tokens, d_model)
        xs0 = own_rows(x_in)
        ds1 = own_rows(d_y)

        h0 = norm(x, g_attn[0])
        q0, kv = project(h0, 0)
        o0, kva0 = attn_fwd(rows3(q0), kv, bias_rows, mask_rows, cp_size, 0)
        x1s0, x1, _, (h0_g,), _ = rsag([o0], [w_o], (False,), 0, xs0, 1, bigs=[h0])
        h20 = norm(x1, g_mlp[0])
        gate0, lin0, u0 = mlp(h20, 0)
        o0 = o0.reshape(tokens, width)
        xs1, x, _, (h20_g,), (o0_g, u0_g) = rsag([rows3(u0)], [w_out], (False,), 0, x1s0, 2, bigs=[h20], smalls=[o0, u0])

        h1 = norm(x, g_attn[1])
        q1, kv = project(h1, 1)
        o1, kva1 = attn_fwd(rows3(q1), kv, bias_rows, mask_rows, cp_size, 3)
        x1s1, x1, _, (h1_g, d1_g), _ = rsag([o1], [w_o], (False,), 1, xs1, 4, bigs=[h1, d1])
        o1 = o1.reshape(tokens, width)
        h21 = norm(x1, g_mlp[1])
        gate1, lin1, u1 = mlp(h21, 1)
        dg1, dl1 = mlp_grads(d1, gate1, lin1, 1)
        dms1, dm1, dgm1, (h21_g,), (o1_g, u1_g, dg1_g, dl1_g) = mlp_back(dg1, dl1, x1s1, ds1, 1, 5, [h21], [o1, u1, dg1, dl1])
        dqkv, dqkv1, score_grad1 = attn_grads(q1, kva1, dm1, 1, 6)
        ds0, d0, dga1, (dm1_g,), (dqkv1_g,) = rsag(dqkv, [w_q, w_k, w_v], (True,) * 3, 1, dms1, 7, (xs1, g_attn[1][None]), [dm1], [dqkv1])

        dg0, dl0 = mlp_grads(d0, gate0, lin0, 0)
        dms0, dm0, dgm0, (d0_g,), (dg0_g, dl0_g) = mlp_back(dg0, dl0, x1s0, ds0, 0, 8, [d0], [dg0, dl0])
        dqkv, dqkv0, score_grad0 = attn_grads(q0, kva0, dm0, 0, 9)
        _, d_x, dga0, (dm0_g,), (dqkv0_g,) = rsag(dqkv, [w_q, w_k, w_v], (True,) * 3, 0, dms0, 10, (xs0, g_attn[0][None]), [dm0], [dqkv0])

        big = []
        for h, h_g, dqkv, dqkv_g in ((h0, h0_g, dqkv0, dqkv0_g), (h1, h1_g, dqkv1, dqkv1_g)):
            part = wide_rows((h, h_g), (dqkv, dqkv_g))
            big.append([join_rows(part[:, i * width:(i + 1) * width]) for i in range(3)])
        w_o_grads = [join_cols(wide_cols((o, o_g), (dm, dm_g))) for o, o_g, dm, dm_g in ((o0, o0_g, dm0, dm0_g), (o1, o1_g, dm1, dm1_g))]
        gate_grads = [join_rows(wide_rows((h, h_g), (d, d_g))) for h, h_g, d, d_g in ((h20, h20_g, dg0, dg0_g), (h21, h21_g, dg1, dg1_g))]
        lin_grads = [join_rows(wide_rows((h, h_g), (d, d_g))) for h, h_g, d, d_g in ((h20, h20_g, dl0, dl0_g), (h21, h21_g, dl1, dl1_g))]
        out_grads = [join_cols(wide_cols((u, u_g), (d, d_g))) for u, u_g, d, d_g in ((u0, u0_g, d0, d0_g), (u1, u1_g, d1, d1_g))]
        grads = [jnp.stack([big[0][i], big[1][i]]) for i in range(3)] + [jnp.stack(p) for p in (w_o_grads, gate_grads, lin_grads, out_grads)]

        d_bias = bias_grad(score_grad0, score_grad1, start, heads, n_buckets)
        slots = jnp.zeros((tp_size, n_buckets * heads), F32)
        slots = lax.dynamic_update_slice(slots, d_bias.reshape(1, -1), (tp_index, jnp.int32(0)))
        small = lax.psum(jnp.concatenate([dga0, dga1, dgm0, dgm1, slots.reshape(-1)]), ('tp', 'cp'))
        n_gain = n_layers * d_model
        d_g_attn = small[:n_gain].reshape(n_layers, d_model)
        d_g_mlp = small[n_gain:2 * n_gain].reshape(n_layers, d_model)
        d_rel = lax.dynamic_slice(small[2 * n_gain:].reshape(tp_size, -1), (tp_index, jnp.int32(0)), (1, n_buckets * heads)).reshape(n_buckets, heads)
        return (d_x.reshape(batch, rows, d_model), d_rel, d_g_attn, d_g_mlp) + tuple(grads)

    return jax.shard_map(local_program, mesh=mesh, in_specs=(seq_spec, seq_spec, P(None, 'cp'), P(None, 'tp')) + weight_specs, out_specs=(seq_spec, P(None, 'tp')) + weight_specs, check_vma=False)
```

```python
import functools

import jax
import jax.numpy as jnp
from jax import lax
from jax.experimental import pallas as pl
from jax.experimental.pallas import tpu as pltpu
from jax.sharding import PartitionSpec as P

NORM_EPS = 1e-6
MASK_NEG = -1e9
BF16 = jnp.bfloat16
F32 = jnp.float32
VMEM = pltpu.VMEM
MESH = pl.DeviceIdType.MESH
MIB = 2 ** 20
HEAD_DIM = 64
VMEM_SPEC = pl.BlockSpec(memory_space=pltpu.VMEM)
SMEM_SPEC = pl.BlockSpec(memory_space=pltpu.SMEM)


def rel_bucket(rel_pos):
    distance = jnp.minimum(jnp.abs(rel_pos), 128)
    distance_sq = distance * distance
    log_part = 8 + sum((distance_sq >= 64 * 2 ** power).astype(jnp.int32) for power in range(1, 8))
    return jnp.where(distance < 8, distance, log_part) + 16 * (rel_pos > 0).astype(jnp.int32)


def comm_params(cid, mib):
    return pltpu.CompilerParams(collective_id=cid, has_side_effects=True, vmem_limit_bytes=mib * MIB)


def cost(gflops):
    return pl.CostEstimate(flops=gflops * 1000 * MIB, bytes_accessed=8 * MIB, transcendentals=MIB)


def dot_nt(a, b):
    return lax.dot_general(a, b, (((1,), (1,)), ((), ())), preferred_element_type=F32)


def dot_nn(a, b):
    return lax.dot_general(a, b, (((1,), (0,)), ((), ())), preferred_element_type=F32)


def dot_tn(a, b):
    return lax.dot_general(a, b, (((0,), (0,)), ((), ())), preferred_element_type=F32)


def stack_heads(block, heads):
    wide = block.astype(F32)
    lane_head = lax.broadcasted_iota(jnp.int32, block.shape, 1) // HEAD_DIM
    return jnp.concatenate([jnp.where(lane_head == h, wide, 0.0).astype(BF16) for h in range(heads)], axis=0)


def pick_heads(stacked, heads, rows):
    lane_head = lax.broadcasted_iota(jnp.int32, (rows, stacked.shape[1]), 1) // HEAD_DIM
    out = stacked[:rows]
    for h in range(1, heads):
        out = jnp.where(lane_head == h, stacked[h * rows:(h + 1) * rows], out)
    return out


def cp_places():
    me = lax.axis_index('cp')
    mate = me + 1 - 2 * lax.rem(me, 2)
    across = lax.rem(me + 2, 4)
    diagonal = lax.rem(mate + 2, 4)
    return me, mate, across, diagonal


def entry_barrier(axis, peers):
    barrier = pltpu.get_barrier_semaphore()
    for peer in peers:
        pl.semaphore_signal(barrier, inc=1, device_id={axis: peer}, device_id_type=MESH)
    pl.semaphore_wait(barrier, len(peers))


def mask_row(mask_ref, b):
    return jnp.concatenate([mask_ref[c, b] for c in range(mask_ref.shape[0])], axis=1)


def attn_fwd_kernel(heads, q_ref, kv_ref, bias_ref, mask_ref, o_ref, all_ref, send, recv):
    batch, rows, width = q_ref.shape
    me, mate, across, _ = cp_places()
    entry_barrier('cp', (mate, across))

    def to_mate(b):
        return pltpu.make_async_remote_copy(src_ref=kv_ref.at[b], dst_ref=all_ref.at[b, me], send_sem=send.at[0, b], recv_sem=recv.at[0, b], device_id={'cp': mate}, device_id_type=MESH)

    def to_across(b):
        return pltpu.make_async_remote_copy(src_ref=kv_ref.at[b], dst_ref=all_ref.at[b, me], send_sem=send.at[1, b], recv_sem=recv.at[1, b], device_id={'cp': across}, device_id_type=MESH)

    def forward(b):
        return pltpu.make_async_remote_copy(src_ref=all_ref.at[b, across], dst_ref=all_ref.at[b, across], send_sem=send.at[2, b], recv_sem=recv.at[2, b], device_id={'cp': mate}, device_id_type=MESH)

    for b in range(batch):
        to_across(b).start()
        to_mate(b).start()

    def step(b, carry):
        to_across(b).wait_recv()
        forward(b).start()
        all_ref[b, me] = kv_ref[b]
        to_mate(b).wait_recv()
        forward(b).wait_recv()
        kv = all_ref[b].reshape(-1, 2 * width)
        stacked = stack_heads(q_ref[b], heads)
        scores = dot_nt(stacked, kv[:, :width]) + bias_ref[:] + mask_row(mask_ref, b)
        top = jnp.max(scores, axis=1, keepdims=True)
        probs = jnp.exp(scores - top)
        total = jnp.sum(probs, axis=1, keepdims=True)
        out = dot_nn(probs.astype(BF16), kv[:, width:]) / total
        o_ref[b] = pick_heads(out, heads, rows).astype(BF16)
        return carry

    lax.fori_loop(0, batch, step, 0)

    def finish(b, carry):
        to_across(b).wait_send()
        to_mate(b).wait_send()
        forward(b).wait_send()
        return carry

    lax.fori_loop(0, batch, finish, 0)


def attn_fwd(q, kv, bias_rows, mask_rows, cp_size, cid):
    batch, rows, width = q.shape
    heads = width // HEAD_DIM
    return pl.pallas_call(
        functools.partial(attn_fwd_kernel, heads),
        out_shape=(jax.ShapeDtypeStruct(q.shape, BF16), jax.ShapeDtypeStruct((batch, cp_size, rows, 2 * width), BF16)),
        in_specs=[VMEM_SPEC] * 4,
        out_specs=(VMEM_SPEC, VMEM_SPEC),
        scratch_shapes=[pltpu.SemaphoreType.DMA((3, batch)), pltpu.SemaphoreType.DMA((3, batch))],
        compiler_params=comm_params(cid, 32),
        cost_estimate=cost(4),
        name='attn_fwd',
    )(q, kv, bias_rows, mask_rows)


def attn_bwd_kernel(heads, qdo_ref, kv_ref, bias_r_ref, bias_c_ref, mask_r_ref, mask_c_ref, dq_ref, dkv_ref, ds_ref, all_ref, own_stats, all_stats, send, recv, send_st, recv_st):
    batch, rows, wide = qdo_ref.shape
    width = wide // 2
    n_blocks = kv_ref.shape[1]
    me, mate, across, diagonal = cp_places()
    entry_barrier('cp', (mate, across, diagonal))

    def to_mate(b):
        return pltpu.make_async_remote_copy(src_ref=qdo_ref.at[b], dst_ref=all_ref.at[b, me], send_sem=send.at[0, b], recv_sem=recv.at[0, b], device_id={'cp': mate}, device_id_type=MESH)

    def to_across(b):
        return pltpu.make_async_remote_copy(src_ref=qdo_ref.at[b], dst_ref=all_ref.at[b, me], send_sem=send.at[1, b], recv_sem=recv.at[1, b], device_id={'cp': across}, device_id_type=MESH)

    def forward(b):
        return pltpu.make_async_remote_copy(src_ref=all_ref.at[b, across], dst_ref=all_ref.at[b, across], send_sem=send.at[2, b], recv_sem=recv.at[2, b], device_id={'cp': mate}, device_id_type=MESH)

    def stats_to(which, b):
        peer = (mate, across, diagonal)[which]
        return pltpu.make_async_remote_copy(src_ref=own_stats.at[b], dst_ref=all_stats.at[b, me], send_sem=send_st.at[which, b], recv_sem=recv_st.at[which, b], device_id={'cp': peer}, device_id_type=MESH)

    for b in range(batch):
        to_across(b).start()
        to_mate(b).start()

    ds_ref[:] = jnp.zeros_like(ds_ref)

    def row_step(b, carry):
        kv = kv_ref[b].reshape(-1, wide)
        keys, vals = kv[:, :width], kv[:, width:]
        qdo = qdo_ref[b]
        all_ref[b, me] = qdo
        scores = dot_nt(stack_heads(qdo[:, :width], heads), keys) + bias_r_ref[:] + mask_row(mask_r_ref, b)
        top = jnp.max(scores, axis=1, keepdims=True)
        unnorm = jnp.exp(scores - top)
        total = jnp.sum(unnorm, axis=1, keepdims=True)
        log_norm = top + jnp.log(total)
        probs = unnorm * (1.0 / total)
        d_probs = dot_nt(stack_heads(qdo[:, width:], heads), vals)
        row_dot = jnp.sum(probs * d_probs, axis=1, keepdims=True)
        lane = lax.broadcasted_iota(jnp.int32, (rows, rows), 1)
        table = jnp.zeros((rows, rows), F32)
        for h in range(heads):
            table = jnp.where(lane == h, log_norm[h * rows:(h + 1) * rows], table)
            table = jnp.where(lane == heads + h, row_dot[h * rows:(h + 1) * rows], table)
        stats = jnp.transpose(table)[:2 * heads]
        own_stats[b] = stats
        all_stats[b, me] = stats
        d_scores = probs * (d_probs - row_dot)
        ds_ref[:] += d_scores
        d_q = dot_nn(d_scores.astype(BF16), keys)
        dq_ref[b] = pick_heads(d_q, heads, rows).astype(BF16)
        for which in range(3):
            stats_to(which, b).start()
        to_across(b).wait_recv()
        forward(b).start()
        return carry

    lax.fori_loop(0, batch, row_step, 0)

    def col_step(b, carry):
        to_mate(b).wait_recv()
        forward(b).wait_recv()
        for which in range(3):
            stats_to(which, b).wait_recv()
        own = kv_ref[b, me]
        keys, vals = own[:, :width], own[:, width:]
        mask_col = mask_c_ref[b]

        def block(src, acc):
            d_k, d_v = acc
            qdo = all_ref[b, src]
            stats = all_stats[b, src]
            log_norm = jnp.concatenate([stats[h:h + 1] for h in range(heads)], axis=1)
            row_dot = jnp.concatenate([stats[heads + h:heads + h + 1] for h in range(heads)], axis=1)
            q_st = stack_heads(qdo[:, :width], heads)
            do_st = stack_heads(qdo[:, width:], heads)
            scores = dot_nt(keys, q_st) + bias_c_ref[src] + mask_col
            probs = jnp.exp(scores - log_norm)
            d_scores = probs * (dot_nt(vals, do_st) - row_dot)
            d_k = d_k + dot_nn(d_scores.astype(BF16), q_st)
            d_v = d_v + dot_nn(probs.astype(BF16), do_st)
            return d_k, d_v

        zero = jnp.zeros((rows, width), F32)
        d_k, d_v = lax.fori_loop(0, n_blocks, block, (zero, zero))
        dkv_ref[b] = jnp.concatenate([d_k, d_v], axis=1).astype(BF16)
        return carry

    lax.fori_loop(0, batch, col_step, 0)

    def finish(b, carry):
        to_across(b).wait_send()
        to_mate(b).wait_send()
        forward(b).wait_send()
        for which in range(3):
            stats_to(which, b).wait_send()
        return carry

    lax.fori_loop(0, batch, finish, 0)


def attn_bwd(qdo, kv_all, bias_rows, bias_cols, mask_rows, mask_cols, cid):
    batch, rows, wide = qdo.shape
    width = wide // 2
    heads = width // HEAD_DIM
    n_blocks = kv_all.shape[1]
    return pl.pallas_call(
        functools.partial(attn_bwd_kernel, heads),
        out_shape=(jax.ShapeDtypeStruct((batch, rows, width), BF16), jax.ShapeDtypeStruct((batch, rows, wide), BF16), jax.ShapeDtypeStruct((heads * rows, n_blocks * rows), F32)),
        in_specs=[VMEM_SPEC] * 6,
        out_specs=(VMEM_SPEC,) * 3,
        scratch_shapes=[
            pltpu.VMEM((batch, n_blocks, rows, wide), BF16),
            pltpu.VMEM((batch, 2 * heads, rows), F32),
            pltpu.VMEM((batch, n_blocks, 2 * heads, rows), F32),
            pltpu.SemaphoreType.DMA((3, batch)),
            pltpu.SemaphoreType.DMA((3, batch)),
            pltpu.SemaphoreType.DMA((3, batch)),
            pltpu.SemaphoreType.DMA((3, batch)),
        ],
        compiler_params=comm_params(cid, 40),
        cost_estimate=cost(10),
        name='attn_bwd',
    )(qdo, kv_all, bias_rows, bias_cols, mask_rows, mask_cols)


def bias_grad_kernel(heads, n_buckets, pos_ref, ds0_ref, ds1_ref, out_ref):
    rows = ds0_ref.shape[0] // heads
    cols = ds0_ref.shape[1]
    rel = lax.broadcasted_iota(jnp.int32, (rows, cols), 1) - lax.broadcasted_iota(jnp.int32, (rows, cols), 0) - pos_ref[0]
    buckets = rel_bucket(rel)
    sums = [ds0_ref[h * rows:(h + 1) * rows] + ds1_ref[h * rows:(h + 1) * rows] for h in range(heads)]

    def step(k, carry):
        hit = buckets == k
        out_ref[k] = jnp.concatenate([jnp.sum(jnp.where(hit, part, 0.0), axis=0, keepdims=True) for part in sums], axis=0)
        return carry

    lax.fori_loop(0, n_buckets, step, 0)


def bias_grad(ds0, ds1, start, heads, n_buckets):
    out = pl.pallas_call(
        functools.partial(bias_grad_kernel, heads, n_buckets),
        out_shape=jax.ShapeDtypeStruct((n_buckets, heads, ds0.shape[1]), F32),
        in_specs=[SMEM_SPEC, VMEM_SPEC, VMEM_SPEC],
        out_specs=VMEM_SPEC,
        compiler_params=pltpu.CompilerParams(vmem_limit_bytes=16 * MIB),
        name='bias_grad',
    )(start.reshape(1), ds0, ds1)
    return jnp.sum(out, axis=-1)


def rms_parts(x_f, gain):
    inv_rms = lax.rsqrt(jnp.mean(x_f * x_f, axis=-1, keepdims=True) + NORM_EPS)
    return (x_f * inv_rms * gain).astype(BF16)


GELU_C = 0.7978845608028654
GELU_A = 0.044715


def gelu_parts(x):
    t = jnp.tanh(GELU_C * (x + GELU_A * x * x * x))
    cdf = 0.5 * (1.0 + t)
    return x * cdf, cdf + 0.5 * x * (1.0 - t * t) * GELU_C * (1.0 + 3.0 * GELU_A * x * x)


def remote(src, dst, send, recv, axis, peer):
    return pltpu.make_async_remote_copy(src_ref=src, dst_ref=dst, send_sem=send, recv_sem=recv, device_id={axis: peer}, device_id_type=MESH)


def tp_places():
    me = lax.axis_index('tp')
    z, y = me // 2, lax.rem(me, 2)
    return me, z, y


def meet(tp_peers, cp_peers):
    barrier = pltpu.get_barrier_semaphore()
    for axis, peers in (('tp', tp_peers), ('cp', cp_peers)):
        for peer in peers:
            pl.semaphore_signal(barrier, inc=1, device_id={axis: peer}, device_id_type=MESH)
    pl.semaphore_wait(barrier, len(tp_peers) + len(cp_peers))


class Ring:
    def __init__(self, part, from_y, from_z, full, sems):
        self.part, self.from_y, self.from_z, self.full = part, from_y, from_z, full
        self.sems = sems
        me, self.z, self.y = tp_places()
        self.pair = me + 1 - 2 * self.y
        self.z_peer = [2 * lax.rem(self.z + j, 4) + self.y for j in range(4)]
        self.seg = self.y * 4 + self.z

    @staticmethod
    def scratch(batch, seg, d_model):
        dma = pltpu.SemaphoreType.DMA
        return [
            pltpu.VMEM((batch, 2, 4, seg, d_model), F32),
            pltpu.VMEM((batch, 4, seg, d_model), F32),
            pltpu.VMEM((batch, 3, seg, d_model), F32),
            dma((2, batch)), dma((2, batch, 3)), dma((2, batch, 3)), dma((2, batch, 4)),
        ]

    def y_sum(self, b):
        s = self.sems[0]
        return remote(self.part.at[b, 1 - self.y], self.from_y.at[b], s.at[0, b], s.at[1, b], 'tp', self.pair)

    def z_sum(self, b, j):
        s = self.sems[1]
        return remote(self.part.at[b, self.y, lax.rem(self.z + j, 4)], self.from_z.at[b, j - 1], s.at[0, b, j - 1], s.at[1, b, j - 1], 'tp', self.z_peer[j])

    def z_gather(self, b, j):
        s = self.sems[2]
        ref = self.full.at[b, self.seg]
        return remote(ref, ref, s.at[0, b, j - 1], s.at[1, b, j - 1], 'tp', self.z_peer[j])

    def y_gather(self, b, j):
        s = self.sems[3]
        ref = self.full.at[b, self.y * 4 + lax.rem(self.z - j + 4, 4)]
        return remote(ref, ref, s.at[0, b, j], s.at[1, b, j], 'tp', self.pair)

    def send_partial(self, b, partial):
        self.part[b] = partial.reshape(self.part.shape[1:])
        self.y_sum(b).start()

    def reduce_pair(self, b):
        self.y_sum(b).wait_recv()
        self.part[b, self.y] = self.part[b, self.y] + self.from_y[b]
        for j in (2, 1, 3):
            self.z_sum(b, j).start()

    def reduced(self, b):
        for j in (1, 2, 3):
            self.z_sum(b, j).wait_recv()
        return self.part[b, self.y, self.z] + self.from_z[b, 0] + self.from_z[b, 1] + self.from_z[b, 2]

    def publish(self, b, out):
        self.full[b, self.seg] = out
        for j in (2, 1, 3):
            self.z_gather(b, j).start()
        self.y_gather(b, 0).start()

    def forward(self, b):
        for j in (1, 2, 3):
            self.z_gather(b, j).wait_recv()
            self.y_gather(b, j).start()

    def rows(self, b):
        for j in range(4):
            self.y_gather(b, j).wait_recv()
        return self.full[b].reshape(-1, self.full.shape[-1])

    def drain(self, b):
        self.y_sum(b).wait_send()
        for j in range(4):
            self.y_gather(b, j).wait_send()
        for j in (1, 2, 3):
            self.z_sum(b, j).wait_send()
            self.z_gather(b, j).wait_send()


class Exchange:
    def __init__(self, wide, late, narrow, send, recv):
        self.wide, self.late, self.narrow, self.send, self.recv = wide, late, narrow, send, recv
        me, self.mate, self.across, self.diagonal = cp_places()
        self.core = lax.rem(me, 2)

    def columns(self, r, n):
        want = self.core if r == 1 else 1 - self.core
        return pl.ds(pl.multiple_of(want * n, n), n)

    def wide_copy(self, i, r):
        src, dst = self.wide[i]
        n = dst.shape[-1]
        return remote(src.at[:, :, self.columns(r, n)], dst.at[r], self.send.at[i, r, 0], self.recv.at[i, r, 0], 'cp', (self.mate, self.across, self.diagonal)[r])

    def late_copy(self, i, r, b):
        src, dst = self.late[i]
        k = len(self.wide) + i
        n = dst.shape[-1]
        return remote(src.at[b].at[..., self.columns(r, n)], dst.at[r, b], self.send.at[k, r, b], self.recv.at[k, r, b], 'cp', (self.mate, self.across, self.diagonal)[r])

    def narrow_copy(self, i, r):
        src, dst = self.narrow[i]
        k = len(self.wide) + len(self.late) + i
        return remote(src if r < 2 else dst.at[1], dst.at[r], self.send.at[k, r, 0], self.recv.at[k, r, 0], 'cp', self.across if r == 1 else self.mate)

    def start(self):
        for i in range(len(self.narrow)):
            self.narrow_copy(i, 1).start()
            self.narrow_copy(i, 0).start()
        for i in range(len(self.wide)):
            for r in (1, 2, 0):
                self.wide_copy(i, r).start()

    def start_late(self, i, b):
        for r in (1, 2, 0):
            self.late_copy(i, r, b).start()

    def pass_on(self):
        for i in range(len(self.narrow)):
            self.narrow_copy(i, 1).wait_recv()
            self.narrow_copy(i, 2).start()

    def finish(self, batch):
        for i in range(len(self.narrow)):
            self.narrow_copy(i, 0).wait_recv()
            self.narrow_copy(i, 2).wait_recv()
            for r in range(3):
                self.narrow_copy(i, r).wait_send()
        for i in range(len(self.wide)):
            for r in range(3):
                self.wide_copy(i, r).wait()
        if self.late:
            def each(b, carry):
                for i in range(len(self.late)):
                    for r in range(3):
                        self.late_copy(i, r, b).wait()
                return carry

            lax.fori_loop(0, batch, each, 0)


def run_slots(batch, stages):
    def slot_step(slot, carry):
        for k, stage in enumerate(stages):
            @pl.when(jnp.logical_and(slot >= k, slot < batch + k))
            def _():
                stage(slot - k)
        return carry

    lax.fori_loop(0, batch + len(stages) - 1, slot_step, 0)


def norm_rows(rows, gain):
    return rms_parts(rows.astype(F32), gain)


def rms_pull(total, x_shard, gain, res, d_gain_ref):
    d_norm = total.astype(BF16).astype(F32)
    x_f = x_shard.astype(F32)
    inv_rms = lax.rsqrt(jnp.mean(x_f * x_f, axis=-1, keepdims=True) + NORM_EPS)
    normed = x_f * inv_rms
    d_gain_ref[:] += jnp.sum(d_norm * normed, axis=0, keepdims=True)
    d_normed = d_norm * gain
    d_x = inv_rms * (d_normed - normed * jnp.mean(d_normed * normed, axis=-1, keepdims=True))
    return (res.astype(F32) + d_x).astype(BF16)


class Refs:
    pass


def chain(name, cid, ins, outs, loads, n_rings, wide, late, narrow, body, geometry):
    batch, seg, d_model = geometry
    any_spec = pl.BlockSpec(memory_space=pl.ANY)
    dma = pltpu.SemaphoreType.DMA
    shapes = {k: v[0].shape for k, v in ins.items()}
    shapes.update({k: v[0] for k, v in outs.items()})
    outs = dict(outs)
    x_names = []
    for group, halved in ((wide, True), (late, True), (narrow, False)):
        for src, dst in group:
            shape = shapes[src]
            outs[dst] = ((3,) + shape[:-1] + (shape[-1] // 2 if halved else shape[-1],), BF16)
            x_names.append(dst)
    n_x = len(x_names)
    in_names, out_names, load_names = list(ins), list(outs), list(loads)
    ring_parts = len(Ring.scratch(batch, seg, d_model))
    n_loads = sum(len(parts) for _, parts in loads.values())

    def kernel(*refs):
        it = iter(refs)
        r = Refs()
        for key in in_names + out_names + load_names:
            setattr(r, key, next(it))
        rings = []
        for i in range(n_rings):
            pieces = [next(it) for _ in range(ring_parts)]
            rings.append((pieces[:3], pieces[3:]))
        load_sem, x_send, x_recv = next(it), next(it), next(it)
        copies = []
        for buf, (_, parts) in loads.items():
            for src, layer, col in parts:
                array = getattr(r, src).at[layer]
                dst = getattr(r, buf)
                if array.shape[-1] != dst.shape[-1]:
                    dst = dst.at[:, pl.ds(col, array.shape[-1])]
                copies.append(pltpu.make_async_copy(array, dst, load_sem.at[len(copies)]))
        for copy in copies:
            copy.start()
        r.rings = [Ring(*pieces, getattr(r, 'full_%d' % i), sems) for i, (pieces, sems) in enumerate(rings)]
        pairs = [[(getattr(r, s), getattr(r, d)) for s, d in group] for group in (wide, late, narrow)]
        r.exchange = Exchange(*pairs, x_send, x_recv)
        first = r.rings[0]
        others = [r.exchange.mate, r.exchange.across, r.exchange.diagonal] if n_x else []
        meet([first.pair] + first.z_peer[1:], others)
        r.exchange.start()
        for copy in copies:
            copy.wait()
        run_slots(batch, body(r))
        r.exchange.pass_on()

        def finish(b, carry):
            for ring in r.rings:
                ring.drain(b)
            return carry

        lax.fori_loop(0, batch, finish, 0)
        r.exchange.finish(batch)

    scratch = [pltpu.VMEM(shape, BF16) for shape, _ in loads.values()]
    for _ in range(n_rings):
        scratch += Ring.scratch(batch, seg, d_model)
    scratch += [dma((max(n_loads, 1),)), dma((max(n_x, 1), 3, batch)), dma((max(n_x, 1), 3, batch))]
    result = pl.pallas_call(
        kernel,
        out_shape=tuple(jax.ShapeDtypeStruct(*outs[k]) for k in out_names),
        in_specs=[VMEM_SPEC if ins[k][1] else any_spec for k in in_names],
        out_specs=tuple(any_spec if k in x_names else VMEM_SPEC for k in out_names),
        scratch_shapes=scratch,
        compiler_params=comm_params(cid, 58),
        cost_estimate=cost(80),
        name=name,
    )(*[ins[k][0] for k in in_names])
    named = Refs()
    for key, value in zip(out_names, result):
        setattr(named, key, value)
    return named


def block_stages(ring, start, epilogue):
    return [start, ring.reduce_pair, lambda b: ring.publish(b, epilogue(b, ring.reduced(b))), ring.forward]


def mlp_rows(r, b, rows, gain, ff):
    h2 = norm_rows(rows, gain)
    r.h2[b] = h2
    both = dot_nn(h2, r.wgl[:])
    return both[:, :ff], both[:, ff:]


def prep_kernel(mask_ref, table_ref, all_ref, rows_ref, cols_ref, send, recv):
    me, mate, across, diagonal = cp_places()
    n_buckets, heads = table_ref.shape
    rows = rows_ref.shape[0] // heads
    seq = rows_ref.shape[1]
    peers = (mate, across, diagonal)
    meet([], peers)

    def copy(i):
        return remote(mask_ref, all_ref.at[me], send.at[i], recv.at[i], 'cp', peers[i])

    for i in range(3):
        copy(i).start()
    all_ref[me] = mask_ref[:]

    def strip(i, carry):
        first = pl.multiple_of(i * 8, 8)
        rel = lax.broadcasted_iota(jnp.int32, (8, seq), 1) - lax.broadcasted_iota(jnp.int32, (8, seq), 0) - me * rows - first
        for is_col in (False, True):
            buckets = rel_bucket(-rel if is_col else rel)
            vals = [jnp.zeros((8, seq), F32) for _ in range(heads)]
            for k in range(n_buckets):
                hit = buckets == k
                vals = [jnp.where(hit, table_ref[k, h], v) for h, v in enumerate(vals)]
            for h, v in enumerate(vals):
                if is_col:
                    for q in range(seq // rows):
                        cols_ref[q, pl.ds(first, 8), h * rows:(h + 1) * rows] = v[:, q * rows:(q + 1) * rows]
                else:
                    rows_ref[pl.ds(pl.multiple_of(h * rows + first, 8), 8), :] = v
        return carry

    lax.fori_loop(0, rows // 8, strip, 0)
    for i in range(3):
        copy(i).wait()


def prep(key_add, rel_bias, cp_size, cid):
    batch, rows = key_add.shape
    heads = rel_bias.shape[1]
    dma = pltpu.SemaphoreType.DMA
    return pl.pallas_call(
        prep_kernel,
        out_shape=(jax.ShapeDtypeStruct((cp_size, batch, 1, rows), F32), jax.ShapeDtypeStruct((heads * rows, cp_size * rows), F32), jax.ShapeDtypeStruct((cp_size, rows, heads * rows), F32)),
        in_specs=[VMEM_SPEC, SMEM_SPEC],
        out_specs=(VMEM_SPEC,) * 3,
        scratch_shapes=[dma((3,)), dma((3,))],
        compiler_params=comm_params(cid, 16),
        cost_estimate=cost(1),
        name='prep',
    )(key_add.reshape(batch, 1, rows), rel_bias)


def swap_kernel(n, *refs):
    halves, small, mates, total = refs[:n], refs[n], refs[n + 1:2 * n + 1], refs[2 * n + 1]
    stage, by_z, send, recv, s_send, s_recv = refs[2 * n + 2:]
    me, z, y = tp_places()
    pair = me + 1 - 2 * y
    z_peer = [2 * lax.rem(z + j, 4) + y for j in range(4)]
    _, mate, across, _ = cp_places()
    meet([pair] + z_peer[1:], [mate, across])

    def half(i):
        return remote(halves[i], mates[i], send.at[i], recv.at[i], 'cp', mate)

    for i in range(n):
        half(i).start()
    mine = small
    for k, (axis, peer) in enumerate((('cp', mate), ('cp', across), ('tp', pair))):
        copy = remote(mine, stage.at[2 * k], s_send.at[k], s_recv.at[k], axis, peer)
        copy.start()
        copy.wait()
        if k < 2:
            stage[2 * k + 1] = mine[:] + stage[2 * k]
            mine = stage.at[2 * k + 1]
        else:
            by_z[z] = mine[:] + stage[2 * k]
    copies = [remote(by_z.at[z], by_z.at[z], s_send.at[2 + j], s_recv.at[2 + j], 'tp', z_peer[j]) for j in (1, 2, 3)]
    for copy in copies:
        copy.start()
    for copy in copies:
        copy.wait()
    total[:] = by_z[0] + by_z[1] + by_z[2] + by_z[3]
    for i in range(n):
        half(i).wait()


def swap(halves, small, cid):
    n = len(halves)
    any_spec = pl.BlockSpec(memory_space=pl.ANY)
    dma = pltpu.SemaphoreType.DMA
    result = pl.pallas_call(
        functools.partial(swap_kernel, n),
        out_shape=tuple(jax.ShapeDtypeStruct(h.shape, h.dtype) for h in halves) + (jax.ShapeDtypeStruct(small.shape, F32),),
        in_specs=[any_spec] * n + [VMEM_SPEC],
        out_specs=tuple([any_spec] * n + [VMEM_SPEC]),
        scratch_shapes=[pltpu.VMEM((5,) + small.shape, F32), pltpu.VMEM((4,) + small.shape, F32), dma((n,)), dma((n,)), dma((6,)), dma((6,))],
        compiler_params=comm_params(cid, 8),
        cost_estimate=cost(10),
        name='swap',
    )(*halves, small)
    return list(result[:n]), result[n]


def place_kernel(plan, n_out, *refs):
    n = len(plan)
    owns, mates, outs = refs[:n], refs[n:2 * n], refs[2 * n:2 * n + n_out]
    bufs, in_sem, out_sem = refs[2 * n + n_out:4 * n + n_out], refs[4 * n + n_out], refs[4 * n + n_out + 1]
    core = lax.rem(lax.axis_index('cp'), 2)
    loads = [pltpu.make_async_copy(src, buf, in_sem.at[i]) for i, (src, buf) in enumerate(zip(owns + mates, bufs))]
    for load in loads:
        load.start()
    stores = []
    for i, load in enumerate(loads):
        layer, by_rows, first_out, n_pieces = plan[i % n]
        which = core if i < n else 1 - core
        buf = bufs[i]
        load.wait()
        width = buf.shape[1] // n_pieces
        for p in range(n_pieces):
            src = buf if n_pieces == 1 else buf.at[:, pl.ds(p * width, width)]
            size = buf.shape[0] if by_rows else width
            window = pl.ds(pl.multiple_of(which * size, size), size)
            out = outs[first_out + p].at[layer]
            dst = out.at[window, :] if by_rows else out.at[:, window]
            stores.append(pltpu.make_async_copy(src, dst, out_sem.at[len(stores)]))
            stores[-1].start()
    for store in stores:
        store.wait()


def place(plan, owns, mates, out_shapes):
    n = len(plan)
    any_spec = pl.BlockSpec(memory_space=pl.ANY)
    n_stores = 2 * sum(p[3] for p in plan)
    return pl.pallas_call(
        functools.partial(place_kernel, plan, len(out_shapes)),
        out_shape=tuple(jax.ShapeDtypeStruct(s, BF16) for s in out_shapes),
        in_specs=[any_spec] * (2 * n),
        out_specs=tuple([any_spec] * len(out_shapes)),
        scratch_shapes=[pltpu.VMEM(a.shape, BF16) for a in list(owns) + list(mates)] + [pltpu.SemaphoreType.DMA((2 * n,)), pltpu.SemaphoreType.DMA((n_stores,))],
        compiler_params=pltpu.CompilerParams(vmem_limit_bytes=40 * MIB),
        name='place',
    )(*owns, *mates)


def solution(mesh):
    cp_size = mesh.shape['cp']
    tp_size = mesh.shape['tp']
    seq_spec = P(None, 'cp', None)
    col_spec = P(None, None, 'tp')
    row_spec = P(None, 'tp', None)
    weight_specs = (P(), P(), col_spec, col_spec, col_spec, row_spec, col_spec, col_spec, row_spec)

    def local_program(x_in, d_y, key_mask, rel_bias, g_attn, g_mlp, w_q, w_k, w_v, w_o, w_gate, w_lin, w_out):
        batch, rows, d_model = x_in.shape
        tokens = batch * rows
        n_layers = w_q.shape[0]
        ff = w_gate.shape[2]
        n_buckets, heads = rel_bias.shape
        width = heads * HEAD_DIM
        cp_index = lax.axis_index('cp')
        tp_index = lax.axis_index('tp')
        core = lax.rem(cp_index, 2)
        half = d_model // 2
        seg = rows // tp_size
        my_seg = lax.rem(tp_index, 2) * 4 + tp_index // 2
        start = (cp_index * rows).astype(jnp.int32)
        geometry = (batch, seg, d_model)
        shard = ((batch, seg, d_model), BF16)
        whole = ((batch, rows, d_model), BF16)
        full = ((batch, tp_size, seg, d_model), BF16)
        gain_row = ((1, d_model), F32)

        key_add = jnp.where(key_mask > 0, 0.0, MASK_NEG).astype(F32)
        mask_rows, bias_rows, bias_cols = prep(key_add, rel_bias, cp_size, 0)
        mask_cols = key_add[:, :, None]

        def own_rows(array):
            return lax.dynamic_slice_in_dim(array, my_seg * seg, seg, axis=1)

        def mlp_pull(d_u, gate, lin):
            d_u = d_u.astype(BF16).astype(F32)
            value, slope = gelu_parts(gate)
            return jnp.concatenate([(d_u * lin * slope).astype(BF16), (d_u * value).astype(BF16)], axis=1)

        wgl = lambda l: ((d_model, 2 * ff), [('w_gate', l, 0), ('w_lin', l, ff)])
        wqkv = lambda l: ((d_model, 3 * width), [('w_q', l, 0), ('w_k', l, width), ('w_v', l, 2 * width)])
        wo = lambda l: ((width, d_model), [('w_o', l, 0)])
        wout = lambda l: ((ff, d_model), [('w_out', l, 0)])
        qkv_in = dict(w_q=(w_q, False), w_k=(w_k, False), w_v=(w_v, False))
        mlp_in = dict(w_gate=(w_gate, False), w_lin=(w_lin, False), w_out=(w_out, False))
        vm = lambda array: (array, True)
        hbm = lambda array: (array, False)

        x0 = x_in.reshape(tokens, d_model)
        h0 = norm_rows(x0, g_attn[0])
        q0, k0, v0 = [jnp.dot(h0, w[0], preferred_element_type=F32).astype(BF16) for w in (w_q, w_k, w_v)]
        h0 = h0.reshape(batch, rows, d_model)
        q0 = q0.reshape(batch, rows, width)
        kv0 = jnp.concatenate([k0, v0], axis=1).reshape(batch, rows, 2 * width)
        o0, kva0 = attn_fwd(q0, kv0, bias_rows, mask_rows, cp_size, 1)

        def body_f0(r):
            ring_a, ring_b = r.rings

            def add_a(b, total):
                out = (r.xs[b].astype(F32) + total).astype(BF16)
                r.x1s[b] = out
                return out

            def middle(b):
                gate, lin = mlp_rows(r, b, ring_a.rows(b), r.gain_m[:], ff)
                r.exchange.start_late(0, b)
                r.gate[b] = gate
                r.lin[b] = lin
                u = (gelu_parts(gate)[0] * lin).astype(BF16)
                r.u[b] = u
                ring_b.send_partial(b, dot_nn(u, r.wout[:]))

            def add_b(b, total):
                out = (r.x1s[b].astype(F32) + total).astype(BF16)
                r.xs1[b] = out
                return out

            def last(b):
                h = norm_rows(ring_b.rows(b), r.gain_a[:])
                r.h1[b] = h
                qkv = dot_nn(h, r.wqkv[:]).astype(BF16)
                r.q1[b] = qkv[:, :width]
                r.kv1[b] = qkv[:, width:]

            return block_stages(ring_a, lambda b: ring_a.send_partial(b, dot_nn(r.o[b], r.wo[:])), add_a) + block_stages(ring_b, middle, add_b) + [last]

        f0 = chain('fwd_0', 2,
                   dict(o=vm(o0), xs=vm(own_rows(x_in)), gain_m=vm(g_mlp[0][None]), gain_a=vm(g_attn[1][None]), h0=hbm(h0), w_o=hbm(w_o), **mlp_in, **qkv_in),
                   dict(x1s=shard, h2=whole, gate=((batch, rows, ff), F32), lin=((batch, rows, ff), F32), u=((batch, rows, ff), BF16), xs1=shard, h1=whole,
                        q1=((batch, rows, width), BF16), kv1=((batch, rows, 2 * width), BF16), full_0=full, full_1=full),
                   dict(wo=wo(0), wgl=wgl(0), wout=wout(0), wqkv=wqkv(1)), 2,
                   [('h0', 'h0_g')], [('h2', 'h2_g')], [('o', 'o_g')], body_f0, geometry)

        o1, kva1 = attn_fwd(f0.q1, f0.kv1, bias_rows, mask_rows, cp_size, 3)

        def body_fb1(r):
            ring_a, ring_b = r.rings
            r.dgain_m[:] = jnp.zeros_like(r.dgain_m)

            def add_a(b, total):
                out = (r.xs[b].astype(F32) + total).astype(BF16)
                r.x1s[b] = out
                return out

            def middle(b):
                gate, lin = mlp_rows(r, b, ring_a.rows(b), r.gain_m[:], ff)
                r.exchange.start_late(0, b)
                r.u[b] = (gelu_parts(gate)[0] * lin).astype(BF16)
                dgl = mlp_pull(dot_nt(r.d[b], r.wout[:]), gate, lin)
                r.dgl[b] = dgl
                ring_b.send_partial(b, dot_nt(dgl, r.wgl[:]))

            def pull_b(b, total):
                out = rms_pull(total, r.x1s[b], r.gain_m[:], r.ds[b], r.dgain_m)
                r.dms[b] = out
                return out

            def last(b):
                d_o = dot_nt(ring_b.rows(b), r.wo[:]).astype(BF16)
                r.qdo[b] = jnp.concatenate([r.q[b], d_o], axis=1)

            return block_stages(ring_a, lambda b: ring_a.send_partial(b, dot_nn(r.o[b], r.wo[:])), add_a) + block_stages(ring_b, middle, pull_b) + [last]

        fb1 = chain('fwd_bwd_1', 4,
                    dict(o=vm(o1), xs=vm(f0.xs1), gain_m=vm(g_mlp[1][None]), d=vm(d_y), ds=vm(own_rows(d_y)), q=vm(f0.q1), h1=hbm(f0.h1), u0=hbm(f0.u), w_o=hbm(w_o), **mlp_in),
                    dict(x1s=shard, h2=whole, u=((batch, rows, ff), BF16), dgl=((batch, rows, 2 * ff), BF16), dms=shard, qdo=((batch, rows, 2 * width), BF16), dgain_m=gain_row, full_0=full, full_1=full),
                    dict(wo=wo(1), wgl=wgl(1), wout=wout(1)), 2,
                    [('h1', 'h1_g'), ('d', 'd_g')], [('h2', 'h2_g')], [('u0', 'u0_g'), ('o', 'o_g')], body_fb1, geometry)

        dq1, dkv1, score_grad1 = attn_bwd(fb1.qdo, kva1, bias_rows, bias_cols, mask_rows, mask_cols, 5)

        def start_qkv(r, ring):
            return lambda b: ring.send_partial(b, dot_nt(jnp.concatenate([r.dq[b], r.dkv[b]], axis=1), r.wqkv[:]))

        def body_bb(r):
            ring_a, ring_b = r.rings
            r.dgain_a[:] = jnp.zeros_like(r.dgain_a)
            r.dgain_m[:] = jnp.zeros_like(r.dgain_m)

            def pull_a(b, total):
                out = rms_pull(total, r.xs[b], r.gain_a[:], r.dms_in[b], r.dgain_a)
                r.ds[b] = out
                return out

            def middle(b):
                d = ring_a.rows(b)
                r.exchange.start_late(0, b)
                dgl = mlp_pull(dot_nt(d, r.wout[:]), r.gate[b], r.lin[b])
                r.dgl[b] = dgl
                ring_b.send_partial(b, dot_nt(dgl, r.wgl[:]))

            def pull_b(b, total):
                out = rms_pull(total, r.x1s[b], r.gain_m[:], r.ds[b], r.dgain_m)
                r.dms[b] = out
                return out

            def last(b):
                d_o = dot_nt(ring_b.rows(b), r.wo[:]).astype(BF16)
                r.qdo[b] = jnp.concatenate([r.q[b], d_o], axis=1)

            return block_stages(ring_a, start_qkv(r, ring_a), pull_a) + block_stages(ring_b, middle, pull_b) + [last]

        dm1 = fb1.full_1.reshape(whole[0])
        bb = chain('bwd_1_0', 6,
                   dict(dq=vm(dq1), dkv=vm(dkv1), xs=vm(f0.xs1), gain_a=vm(g_attn[1][None]), dms_in=vm(fb1.dms), gate=vm(f0.gate), lin=vm(f0.lin), x1s=vm(f0.x1s), gain_m=vm(g_mlp[0][None]), q=vm(q0),
                        dm1=hbm(dm1), u1=hbm(fb1.u), dgl1=hbm(fb1.dgl), w_o=hbm(w_o), **mlp_in, **qkv_in),
                   dict(ds=shard, dgl=((batch, rows, 2 * ff), BF16), dms=shard, qdo=((batch, rows, 2 * width), BF16), dgain_a=gain_row, dgain_m=gain_row, full_0=full, full_1=full),
                   dict(wqkv=wqkv(1), wout=wout(0), wgl=wgl(0), wo=wo(0)), 2,
                   [('dm1', 'dm1_g')], [('full_0', 'd_g')], [('u1', 'u1_g'), ('dgl1', 'dgl1_g'), ('dq', 'dq_g'), ('dkv', 'dkv_g')], body_bb, geometry)

        dq0, dkv0, score_grad0 = attn_bwd(bb.qdo, kva0, bias_rows, bias_cols, mask_rows, mask_cols, 7)

        def body_bf(r):
            ring, = r.rings
            r.dgain_a[:] = jnp.zeros_like(r.dgain_a)

            def pull(b, total):
                return rms_pull(total, r.xs[b], r.gain_a[:], r.dms_in[b], r.dgain_a)

            def last(b):
                for j in range(4):
                    ring.y_gather(b, j).wait_recv()

            return block_stages(ring, start_qkv(r, ring), pull) + [last]

        dm0 = bb.full_1.reshape(whole[0])
        bf = chain('bwd_0', 8,
                   dict(dq=vm(dq0), dkv=vm(dkv0), xs=vm(own_rows(x_in)), gain_a=vm(g_attn[0][None]), dms_in=vm(bb.dms), dm0=hbm(dm0), dgl0=hbm(bb.dgl), **qkv_in),
                   dict(dgain_a=gain_row, full_0=full), dict(wqkv=wqkv(0)), 1,
                   [('dm0', 'dm0_g')], [], [('dgl0', 'dgl0_g'), ('dq', 'dq_g'), ('dkv', 'dkv_g')], body_bf, geometry)

        def own_half(array):
            return lax.dynamic_slice_in_dim(array.reshape(tokens, d_model), core * half, half, axis=1)

        def flat(array, n):
            return array.reshape(-1, n)

        def grad(left, right, left_wide):
            (a, a_g), (b, b_g) = left, right
            a_n, b_n = a_g.shape[-1], b_g.shape[-1]
            a = own_half(a) if left_wide else flat(a, a_n)
            b = flat(b, b_n) if left_wide else own_half(b)
            return (dot_tn(a, b) + dot_tn(flat(a_g, a_n), flat(b_g, b_n))).astype(BF16)

        dqkv1 = (jnp.concatenate([dq1, dkv1], axis=2), jnp.concatenate([bb.dq_g, bb.dkv_g], axis=3))
        dqkv0 = (jnp.concatenate([dq0, dkv0], axis=2), jnp.concatenate([bf.dq_g, bf.dkv_g], axis=3))
        owns = [
            grad((h0, f0.h0_g), dqkv0, True),
            grad((f0.h1, fb1.h1_g), dqkv1, True),
            grad((o0, f0.o_g), (dm0, bf.dm0_g), False),
            grad((o1, fb1.o_g), (dm1, bb.dm1_g), False),
            grad((f0.h2, f0.h2_g), (bb.dgl, bf.dgl0_g), True),
            grad((fb1.h2, fb1.h2_g), (fb1.dgl, bb.dgl1_g), True),
            grad((f0.u, fb1.u0_g), (bb.full_0, bb.d_g), False),
            grad((fb1.u, bb.u1_g), (d_y, fb1.d_g), False),
        ]

        d_bias = bias_grad(score_grad0, score_grad1, start, heads, n_buckets)
        slots = jnp.zeros((tp_size, n_buckets * heads), F32)
        slots = lax.dynamic_update_slice(slots, d_bias.reshape(1, -1), (tp_index, jnp.int32(0)))
        small = jnp.concatenate([part.reshape(-1, 128) for part in (bf.dgain_a, bb.dgain_a, bb.dgain_m, fb1.dgain_m, slots)], axis=0)
        mates, small = swap(owns, small, 9)
        n_gain = n_layers * d_model // 128
        d_g_attn = small[:n_gain].reshape(n_layers, d_model)
        d_g_mlp = small[n_gain:2 * n_gain].reshape(n_layers, d_model)
        d_rel = lax.dynamic_slice(small[2 * n_gain:].reshape(tp_size, -1), (tp_index, jnp.int32(0)), (1, n_buckets * heads)).reshape(n_buckets, heads)
        plan = tuple((layer, by_rows, first, n) for by_rows, first, n in ((True, 0, 3), (False, 3, 1), (True, 4, 2), (False, 6, 1)) for layer in range(n_layers))
        grads = place(plan, owns, mates, [w.shape for w in (w_q, w_k, w_v, w_o, w_gate, w_lin, w_out)])
        return (bf.full_0.reshape(batch, rows, d_model), d_rel, d_g_attn, d_g_mlp) + tuple(grads)

    return jax.shard_map(local_program, mesh=mesh, in_specs=(seq_spec, seq_spec, P(None, 'cp'), P(None, 'tp')) + weight_specs, out_specs=(seq_spec, P(None, 'tp')) + weight_specs, check_vma=False)
```

```python
import functools

import jax
import jax.numpy as jnp
from jax import lax
from jax.experimental import pallas as pl
from jax.experimental.pallas import tpu as pltpu
from jax.sharding import PartitionSpec as P

NORM_EPS = 1e-6
MASK_NEG = -1e9
BF16 = jnp.bfloat16
F32 = jnp.float32
VMEM = pltpu.VMEM
MESH = pl.DeviceIdType.MESH
MIB = 2 ** 20
HEAD_DIM = 64
VMEM_SPEC = pl.BlockSpec(memory_space=pltpu.VMEM)
SMEM_SPEC = pl.BlockSpec(memory_space=pltpu.SMEM)


def rel_bucket(rel_pos):
    distance = jnp.minimum(jnp.abs(rel_pos), 128)
    distance_sq = distance * distance
    log_part = 8 + sum((distance_sq >= 64 * 2 ** power).astype(jnp.int32) for power in range(1, 8))
    return jnp.where(distance < 8, distance, log_part) + 16 * (rel_pos > 0).astype(jnp.int32)


def comm_params(cid, mib):
    return pltpu.CompilerParams(collective_id=cid, has_side_effects=True, vmem_limit_bytes=mib * MIB)


def cost(gflops):
    return pl.CostEstimate(flops=gflops * 1000 * MIB, bytes_accessed=8 * MIB, transcendentals=MIB)


def dot_nt(a, b):
    return lax.dot_general(a, b, (((1,), (1,)), ((), ())), preferred_element_type=F32)


def dot_nn(a, b):
    return lax.dot_general(a, b, (((1,), (0,)), ((), ())), preferred_element_type=F32)


def dot_tn(a, b):
    return lax.dot_general(a, b, (((0,), (0,)), ((), ())), preferred_element_type=F32)


def stack_heads(block, heads):
    wide = block.astype(F32)
    lane_head = lax.broadcasted_iota(jnp.int32, block.shape, 1) // HEAD_DIM
    return jnp.concatenate([jnp.where(lane_head == h, wide, 0.0).astype(BF16) for h in range(heads)], axis=0)


def pick_heads(stacked, heads, rows):
    lane_head = lax.broadcasted_iota(jnp.int32, (rows, stacked.shape[1]), 1) // HEAD_DIM
    out = stacked[:rows]
    for h in range(1, heads):
        out = jnp.where(lane_head == h, stacked[h * rows:(h + 1) * rows], out)
    return out


def cp_places():
    me = lax.axis_index('cp')
    mate = me + 1 - 2 * lax.rem(me, 2)
    across = lax.rem(me + 2, 4)
    diagonal = lax.rem(mate + 2, 4)
    return me, mate, across, diagonal


def rms_parts(x_f, gain):
    inv_rms = lax.rsqrt(jnp.mean(x_f * x_f, axis=-1, keepdims=True) + NORM_EPS)
    return (x_f * inv_rms * gain).astype(BF16)


GELU_C = 0.7978845608028654
GELU_A = 0.044715


def gelu_parts(x):
    t = jnp.tanh(GELU_C * (x + GELU_A * x * x * x))
    cdf = 0.5 * (1.0 + t)
    return x * cdf, cdf + 0.5 * x * (1.0 - t * t) * GELU_C * (1.0 + 3.0 * GELU_A * x * x)


def remote(src, dst, send, recv, axis, peer):
    return pltpu.make_async_remote_copy(src_ref=src, dst_ref=dst, send_sem=send, recv_sem=recv, device_id={axis: peer}, device_id_type=MESH)


def tp_places():
    me = lax.axis_index('tp')
    z, y = me // 2, lax.rem(me, 2)
    pair = me + 1 - 2 * y
    return me, z, y, pair, [2 * lax.rem(z + j, 4) + y for j in range(4)]


def meet(tp_peers, cp_peers):
    barrier = pltpu.get_barrier_semaphore()
    for axis, peers in (('tp', tp_peers), ('cp', cp_peers)):
        for peer in peers:
            pl.semaphore_signal(barrier, inc=1, device_id={axis: peer}, device_id_type=MESH)
    pl.semaphore_wait(barrier, len(tp_peers) + len(cp_peers))


class Ring:
    def __init__(self, part, from_y, from_z, full, *sems):
        self.part, self.from_y, self.from_z, self.full, self.sems = part, from_y, from_z, full, sems
        _, self.z, self.y, self.pair, self.z_peer = tp_places()
        self.seg = self.y * 4 + self.z

    @staticmethod
    def scratch(batch, seg, d_model):
        dma = pltpu.SemaphoreType.DMA
        return [
            pltpu.VMEM((batch, 2, 4, seg, d_model), F32),
            pltpu.VMEM((batch, 4, seg, d_model), F32),
            pltpu.VMEM((batch, 3, seg, d_model), F32),
            pltpu.VMEM((batch, 8, seg, d_model), BF16),
            dma((2, batch)), dma((2, batch, 3)), dma((2, batch, 3)), dma((2, batch, 4)),
        ]

    def y_sum(self, b):
        s = self.sems[0]
        return remote(self.part.at[b, 1 - self.y], self.from_y.at[b], s.at[0, b], s.at[1, b], 'tp', self.pair)

    def z_sum(self, b, j):
        s = self.sems[1]
        return remote(self.part.at[b, self.y, lax.rem(self.z + j, 4)], self.from_z.at[b, j - 1], s.at[0, b, j - 1], s.at[1, b, j - 1], 'tp', self.z_peer[j])

    def z_gather(self, b, j):
        s = self.sems[2]
        ref = self.full.at[b, self.seg]
        return remote(ref, ref, s.at[0, b, j - 1], s.at[1, b, j - 1], 'tp', self.z_peer[j])

    def y_gather(self, b, j):
        s = self.sems[3]
        ref = self.full.at[b, self.y * 4 + lax.rem(self.z - j + 4, 4)]
        return remote(ref, ref, s.at[0, b, j], s.at[1, b, j], 'tp', self.pair)

    def send_partial(self, b, partial):
        self.part[b] = partial.reshape(self.part.shape[1:])
        self.y_sum(b).start()

    def reduce_pair(self, b):
        self.y_sum(b).wait_recv()
        self.part[b, self.y] = self.part[b, self.y] + self.from_y[b]
        for j in (2, 1, 3):
            self.z_sum(b, j).start()

    def reduced(self, b):
        for j in (1, 2, 3):
            self.z_sum(b, j).wait_recv()
        return self.part[b, self.y, self.z] + self.from_z[b, 0] + self.from_z[b, 1] + self.from_z[b, 2]

    def publish(self, b, out):
        self.full[b, self.seg] = out
        for j in (2, 1, 3):
            self.z_gather(b, j).start()
        self.y_gather(b, 0).start()

    def forward(self, b):
        for j in (1, 2, 3):
            self.z_gather(b, j).wait_recv()
            self.y_gather(b, j).start()

    def arrive(self, b):
        for j in range(4):
            self.y_gather(b, j).wait_recv()
        self.y_sum(b).wait_send()
        for j in range(4):
            self.y_gather(b, j).wait_send()
        for j in (1, 2, 3):
            self.z_sum(b, j).wait_send()
            self.z_gather(b, j).wait_send()

    def rows(self, b):
        return self.full[b].reshape(-1, self.full.shape[-1])


class Trade:
    def __init__(self, store, send, recv):
        self.store, self.send, self.recv = store, send, recv
        self.me, self.mate, self.across, self.diagonal = cp_places()

    def copy(self, b, r):
        ref = self.store.at[b, self.across if r == 2 else self.me]
        return remote(ref, ref, self.send.at[r, b], self.recv.at[r, b], 'cp', self.across if r == 1 else self.mate)

    def give(self, b):
        self.copy(b, 1).start()
        self.copy(b, 0).start()

    def pass_on(self, b):
        self.copy(b, 1).wait_recv()
        self.copy(b, 2).start()

    def take(self, b):
        self.copy(b, 0).wait_recv()
        self.copy(b, 2).wait_recv()

    def finish(self, b):
        for r in range(3):
            self.copy(b, r).wait_send()


class Wide:
    def __init__(self, src, dst, send, recv):
        self.src, self.dst, self.send, self.recv = src, dst, send, recv
        me, *self.peers = cp_places()
        mate, across, diagonal = self.peers
        self.peers = (mate, across, diagonal)
        self.core = lax.rem(me, 2)

    def copy(self, r, window):
        n = self.dst.shape[-1]
        want = self.core if r == 1 else 1 - self.core
        columns = pl.ds(pl.multiple_of(want * n, n), n)
        return remote(self.src.at[window].at[..., columns], self.dst.at[r].at[window], self.send.at[r], self.recv.at[r], 'cp', self.peers[r])

    def give(self, b):
        for r in (1, 2, 0):
            self.copy(r, pl.ds(b, 1)).start()

    def pass_on(self):
        pass

    def finish(self):
        for r in range(3):
            self.copy(r, pl.ds(0, self.src.shape[0])).wait()


class Narrow:
    def __init__(self, src, dst, send, recv):
        self.src, self.dst, self.send, self.recv = src, dst, send, recv
        _, self.mate, self.across, _ = cp_places()

    def copy(self, r, window):
        src = self.src if r < 2 else self.dst.at[1]
        return remote(src.at[window], self.dst.at[r].at[window], self.send.at[r], self.recv.at[r], 'cp', self.across if r == 1 else self.mate)

    def give(self, b):
        for r in (1, 0):
            self.copy(r, pl.ds(b, 1)).start()

    def pass_on(self):
        every = pl.ds(0, self.src.shape[0])
        self.copy(1, every).wait_recv()
        self.copy(2, every).start()

    def finish(self):
        every = pl.ds(0, self.src.shape[0])
        self.copy(0, every).wait()
        self.copy(1, every).wait_send()
        self.copy(2, every).wait()


class Spill:
    def __init__(self, slots, sem):
        self.slots, self.sem = slots, sem

    def copy(self, out, b):
        slot = lax.rem(b, 2)
        return pltpu.make_async_copy(self.slots.at[slot], out.at[b], self.sem.at[slot])

    def put(self, out, b, value):
        self.slots[lax.rem(b, 2)] = value
        self.copy(out, b).start()


def norm_rows(rows, gain):
    return rms_parts(rows.astype(F32), gain)


def rms_pull(total, x_shard, gain, res, d_gain_ref):
    d_norm = total.astype(BF16).astype(F32)
    x_f = x_shard.astype(F32)
    inv_rms = lax.rsqrt(jnp.mean(x_f * x_f, axis=-1, keepdims=True) + NORM_EPS)
    normed = x_f * inv_rms
    d_gain_ref[:] += jnp.sum(d_norm * normed, axis=0, keepdims=True)
    d_normed = d_norm * gain
    d_x = inv_rms * (d_normed - normed * jnp.mean(d_normed * normed, axis=-1, keepdims=True))
    return (res.astype(F32) + d_x).astype(BF16)


def mlp_pull(d_u, gate, lin):
    d_u = d_u.astype(BF16).astype(F32)
    value, slope = gelu_parts(gate)
    return jnp.concatenate([(d_u * lin * slope).astype(BF16), (d_u * value).astype(BF16)], axis=1)


def row_sum(x):
    return jnp.sum(x, axis=1, keepdims=True)


def row_max(x):
    return jnp.max(x, axis=1, keepdims=True)


def mask_row(mask_ref, b):
    return jnp.concatenate([mask_ref[c, b] for c in range(mask_ref.shape[0])], axis=1)


def attend(heads, q, kv, bias, mask):
    rows, width = q.shape
    scores = dot_nt(stack_heads(q, heads), kv[:, :width]) + bias + mask
    top = row_max(scores)
    probs = jnp.exp(scores - top)
    total = row_sum(probs)
    out = dot_nn(probs.astype(BF16), kv[:, width:]) / total
    return pick_heads(out, heads, rows).astype(BF16)


def attend_rows_back(heads, qdo, kv, bias, mask, ds_ref):
    rows, wide = qdo.shape
    width = wide // 2
    keys, vals = kv[:, :width], kv[:, width:]
    scores = dot_nt(stack_heads(qdo[:, :width], heads), keys) + bias + mask
    top = row_max(scores)
    unnorm = jnp.exp(scores - top)
    total = row_sum(unnorm)
    log_norm = top + jnp.log(total)
    probs = unnorm * (1.0 / total)
    d_probs = dot_nt(stack_heads(qdo[:, width:], heads), vals)
    row_dot = row_sum(probs * d_probs)
    lane = lax.broadcasted_iota(jnp.int32, (rows, rows), 1)
    table = jnp.zeros((rows, rows), F32)
    for h in range(heads):
        table = jnp.where(lane == h, log_norm[h * rows:(h + 1) * rows], table)
        table = jnp.where(lane == heads + h, row_dot[h * rows:(h + 1) * rows], table)
    d_scores = probs * (d_probs - row_dot)
    ds_ref[:] += d_scores
    d_q = dot_nn(d_scores.astype(BF16), keys)
    return pick_heads(d_q, heads, rows).astype(BF16), jnp.transpose(table)[:2 * heads]


def attend_cols_back(heads, own_kv, mask_col, bias_ref, qdo_of, stats_of):
    rows, wide = own_kv.shape
    width = wide // 2
    keys, vals = own_kv[:, :width], own_kv[:, width:]

    def block(src, acc):
        d_k, d_v = acc
        qdo, stats = qdo_of(src), stats_of(src)
        log_norm = jnp.concatenate([stats[h:h + 1] for h in range(heads)], axis=1)
        row_dot = jnp.concatenate([stats[heads + h:heads + h + 1] for h in range(heads)], axis=1)
        q_st = stack_heads(qdo[:, :width], heads)
        do_st = stack_heads(qdo[:, width:], heads)
        probs = jnp.exp(dot_nt(keys, q_st) + bias_ref[src] + mask_col - log_norm)
        d_scores = probs * (dot_nt(vals, do_st) - row_dot)
        return d_k + dot_nn(d_scores.astype(BF16), q_st), d_v + dot_nn(probs.astype(BF16), do_st)

    zero = jnp.zeros((rows, width), F32)
    d_k, d_v = lax.fori_loop(0, bias_ref.shape[0], block, (zero, zero))
    return jnp.concatenate([d_k, d_v], axis=1).astype(BF16)


def bias_tables(table_ref, me, rows_ref, cols_ref):
    n_buckets, heads = table_ref.shape
    rows = rows_ref.shape[0] // heads
    seq = rows_ref.shape[1]

    def strip(i, carry):
        first = pl.multiple_of(i * 8, 8)
        rel = lax.broadcasted_iota(jnp.int32, (8, seq), 1) - lax.broadcasted_iota(jnp.int32, (8, seq), 0) - me * rows - first
        for is_col in (False, True):
            buckets = rel_bucket(-rel if is_col else rel)
            vals = [jnp.zeros((8, seq), F32) for _ in range(heads)]
            for k in range(n_buckets):
                hit = buckets == k
                vals = [jnp.where(hit, table_ref[k, h], v) for h, v in enumerate(vals)]
            for h, v in enumerate(vals):
                if is_col:
                    for q in range(seq // rows):
                        cols_ref[q, pl.ds(first, 8), h * rows:(h + 1) * rows] = v[:, q * rows:(q + 1) * rows]
                else:
                    rows_ref[pl.ds(pl.multiple_of(h * rows + first, 8), 8), :] = v
        return carry

    lax.fori_loop(0, rows // 8, strip, 0)


def bucket_sums(ds_ref, me, out_ref):
    n_buckets, heads, seq = out_ref.shape
    rows = ds_ref.shape[0] // heads
    rel = lax.broadcasted_iota(jnp.int32, (rows, seq), 1) - lax.broadcasted_iota(jnp.int32, (rows, seq), 0) - me * rows

    def step(k, carry):
        hit = rel_bucket(rel) == k
        out_ref[k] = jnp.concatenate([jnp.sum(jnp.where(hit, ds_ref[h * rows:(h + 1) * rows], 0.0), axis=0, keepdims=True) for h in range(heads)], axis=0)
        return carry

    lax.fori_loop(0, n_buckets, step, 0)


class Refs:
    pass


WIDE = ('h0', 'h1', 'm0', 'm1', 'dy', 'd0')
NARROW = ('u0', 'u1', 'gl0', 'gl1', 'qkv0', 'qkv1')


def mega_kernel(names, heads, *refs):
    r = Refs()
    for key, ref in zip(names, refs):
        setattr(r, key, ref)
    batch, n_seg, seg, d_model = r.x.shape
    rows = n_seg * seg
    ff = r.w_out.shape[1]
    width = heads * HEAD_DIM
    ring = Ring(*[getattr(r, 'ring_%d' % i) for i in range(8)])
    me, mate, across, diagonal = cp_places()
    others = (mate, across, diagonal)

    def weight(buf, sem, sources, layer):
        out, col = [], 0
        for i, src in enumerate(sources):
            n = src.shape[-1]
            out.append(pltpu.make_async_copy(src.at[layer], buf.at[:, pl.ds(col, n)] if len(sources) > 1 else buf, sem.at[i]))
            col += n
        return out

    weights = dict(qkv=(r.wqkv, r.sem_qkv, (r.w_q, r.w_k, r.w_v)), o=(r.wo, r.sem_o, (r.w_o,)), gl=(r.wgl, r.sem_gl, (r.w_gate, r.w_lin)), out=(r.wout, r.sem_out, (r.w_out,)))

    def load(key, layer):
        def go():
            for copy in weight(*weights[key], layer):
                copy.start()
        return go

    def loaded(key, layer):
        def go():
            for copy in weight(*weights[key], layer):
                copy.wait()
        return go

    for key in ('qkv', 'o', 'gl', 'out'):
        load(key, 0)()
    rows_in = [pltpu.make_async_copy(r.x.at[b], ring.full.at[b], r.sem_in.at[b]) for b in range(batch)]
    shards_in = [pltpu.make_async_copy(src.at[:, ring.seg], dst, r.sem_in.at[batch + i]) for i, (src, dst) in enumerate(((r.x, r.xs0), (r.dy, r.ds1)))]
    for copy in rows_in + shards_in:
        copy.start()
    meet([ring.pair] + ring.z_peer[1:], others)
    masks = [remote(r.key_add, r.mask_all.at[me], r.sem_mask.at[0, i], r.sem_mask.at[1, i], 'cp', peer) for i, peer in enumerate(others)]
    for copy in masks:
        copy.start()
    r.mask_all[me] = r.key_add[:]
    for ref in (r.ds_sum, r.dga0, r.dga1, r.dgm0, r.dgm1):
        ref[:] = jnp.zeros_like(ref)
    for copy in rows_in + shards_in:
        copy.wait()
    loaded('qkv', 0)()

    hold = dict(h=Spill(r.hbuf, r.sem_h), u=Spill(r.ubuf, r.sem_u), gl=Spill(r.gbuf, r.sem_g), qkv=Spill(r.qbuf, r.sem_q), o=Spill(r.obuf, r.sem_ob))
    moves = {}
    for i, key in enumerate(WIDE):
        moves[key] = Wide(r.dy_rows if key == 'dy' else getattr(r, 'out_' + key), getattr(r, 'got_' + key), r.sem_wide.at[0, i], r.sem_wide.at[1, i])
    for i, key in enumerate(NARROW):
        moves[key] = Narrow(getattr(r, 'out_' + key), getattr(r, 'got_' + key), r.sem_narrow.at[0, i], r.sem_narrow.at[1, i])
    kv = [Trade(r.kv0, r.sem_kv.at[0, 0], r.sem_kv.at[1, 0]), Trade(r.kv1, r.sem_kv.at[0, 1], r.sem_kv.at[1, 1])]
    qdo = [Trade(r.qdo0, r.sem_qdo.at[0, 0], r.sem_qdo.at[1, 0]), Trade(r.qdo1, r.sem_qdo.at[0, 1], r.sem_qdo.at[1, 1])]
    q_own = (r.q0, r.q1)
    stats = (r.stats0, r.stats1)

    def send_stats(l, b, i):
        ref = stats[l].at[b, me]
        return remote(ref, ref, r.sem_stats.at[0, l, i, b], r.sem_stats.at[1, l, i, b], 'cp', others[i])

    def of(key, l):
        return getattr(r, '%s%d' % (key, l))

    def out(key, l):
        return getattr(r, 'out_%s%d' % (key, l))

    def project(l, b, flat):
        h = norm_rows(flat, r.g_attn[l])
        hold['h'].put(out('h', l), b, h)
        qkv = dot_nn(h, r.wqkv[:]).astype(BF16)
        q_own[l][b] = qkv[:, :width]
        kv[l].store[b, me] = qkv[:, width:]
        kv[l].give(b)

    def stage_first(b):
        project(0, b, ring.rows(b))

    def stage_attend(l):
        def go(b):
            kv[l].take(b)
            pairs = kv[l].store[b].reshape(-1, 2 * width)
            o = attend(heads, q_own[l][b], pairs, r.bias_rows[:], mask_row(r.mask_all, b))
            hold['o'].put(out('o', l), b, o)
            ring.send_partial(b, dot_nn(o, r.wo[:]))
        return go

    def add_stage(res, dst):
        def go(b):
            total = ring.reduced(b)
            value = (res[b].astype(F32) + total).astype(BF16)
            dst[b] = value
            ring.publish(b, value)
        return go

    def pull_stage(x_shard, gain, res, dst, d_gain):
        def go(b):
            value = rms_pull(ring.reduced(b), x_shard[b], gain[:], res[b], d_gain)
            if dst is not None:
                dst[b] = value
            ring.publish(b, value)
        return go

    def mlp_forward(l, b):
        ring.arrive(b)
        h2 = norm_rows(ring.rows(b), r.g_mlp[l])
        hold['h'].put(out('m', l), b, h2)
        both = dot_nn(h2, r.wgl[:])
        gate, lin = both[:, :ff], both[:, ff:]
        u = (gelu_parts(gate)[0] * lin).astype(BF16)
        hold['u'].put(out('u', l), b, u)
        return gate, lin, u

    def stage_mlp0(b):
        gate, lin, u = mlp_forward(0, b)
        r.gate[b] = gate
        r.lin[b] = lin
        ring.send_partial(b, dot_nn(u, r.wout[:]))

    def stage_next(b):
        ring.arrive(b)
        project(1, b, ring.rows(b))

    def dy_in(b):
        slot = lax.rem(b, 2)
        return pltpu.make_async_copy(r.dy_rows.at[b], r.dybuf.at[slot], r.sem_dy.at[slot])

    def mlp_backward(l, b, d, gate, lin):
        dgl = mlp_pull(dot_nt(d, r.wout[:]), gate, lin)
        hold['gl'].put(out('gl', l), b, dgl)
        ring.send_partial(b, dot_nt(dgl, r.wgl[:]))

    def stage_mlp1(b):
        gate, lin, _ = mlp_forward(1, b)
        dy_in(b).wait()
        mlp_backward(1, b, r.dybuf[lax.rem(b, 2)], gate, lin)

    def keep(dst, b):
        copy = pltpu.make_async_copy(ring.full.at[b], dst.at[b], r.sem_keep.at[b])
        copy.start()
        return copy

    def stage_rows_back(l, dst):
        def go(b):
            ring.arrive(b)
            copy = keep(dst, b)
            d_o = dot_nt(ring.rows(b), r.wo[:]).astype(BF16)
            both = jnp.concatenate([q_own[l][b], d_o], axis=1)
            qdo[l].store[b, me] = both
            qdo[l].give(b)
            pairs = kv[l].store[b].reshape(-1, 2 * width)
            d_q, table = attend_rows_back(heads, both, pairs, r.bias_rows[:], mask_row(r.mask_all, b), r.ds_sum)
            stats[l][b, me] = table
            r.dq[b] = d_q
            for i in range(3):
                send_stats(l, b, i).start()
            copy.wait()
        return go

    def stage_cols_back(l):
        def go(b):
            qdo[l].take(b)
            for i in range(3):
                send_stats(l, b, i).wait_recv()
            d_kv = attend_cols_back(heads, kv[l].store[b, me], r.mask_cols[b], r.bias_cols, lambda s: qdo[l].store[b, s], lambda s: stats[l][b, s])
            d_qkv = jnp.concatenate([r.dq[b], d_kv], axis=1)
            hold['qkv'].put(out('qkv', l), b, d_qkv)
            ring.send_partial(b, dot_nt(d_qkv, r.wqkv[:]))
        return go

    def stage_mlp_back0(b):
        ring.arrive(b)
        copy = keep(r.out_d0, b)
        mlp_backward(0, b, ring.rows(b), r.gate[b], r.lin[b])
        copy.wait()

    def stage_last(b):
        ring.arrive(b)
        keep(r.out_dx, b).wait()

    def kept(key, dst):
        return lambda b: hold[key].copy(dst, b).wait()

    def then(*parts):
        def go(b):
            for part in parts:
                part(b)
        return go

    def give(key):
        return lambda b: moves[key].give(b)

    stages = [
        stage_first,
        then(kv[0].pass_on, kept('h', r.out_h0)),
        stage_attend(0),
        then(ring.reduce_pair, kept('o', r.out_o0)),
        then(add_stage(r.xs0, r.x1s0), give('h0')),
        ring.forward,
        stage_mlp0,
        then(ring.reduce_pair, kept('h', r.out_m0), kept('u', r.out_u0), give('u0')),
        then(add_stage(r.x1s0, r.xs1), give('m0')),
        ring.forward,
        stage_next,
        then(kv[1].pass_on, kept('h', r.out_h1)),
        stage_attend(1),
        then(ring.reduce_pair, kept('o', r.out_o1)),
        then(add_stage(r.xs1, r.x1s1), give('h1')),
        then(lambda b: dy_in(b).start(), ring.forward),
        stage_mlp1,
        then(ring.reduce_pair, kept('h', r.out_m1), kept('u', r.out_u1), kept('gl', r.out_gl1), give('u1')),
        then(pull_stage(r.x1s1, r.g_mlp.at[1], r.ds1, r.dms1, r.dgm1), give('m1')),
        ring.forward,
        stage_rows_back(1, r.out_dm1),
        qdo[1].pass_on,
        stage_cols_back(1),
        then(ring.reduce_pair, kept('qkv', r.out_qkv1), give('gl1')),
        then(pull_stage(r.xs1, r.g_attn.at[1], r.dms1, r.ds0, r.dga1), give('dy')),
        then(ring.forward, give('qkv1')),
        stage_mlp_back0,
        then(ring.reduce_pair, kept('gl', r.out_gl0), give('d0')),
        pull_stage(r.x1s0, r.g_mlp.at[0], r.ds0, r.dms0, r.dgm0),
        ring.forward,
        stage_rows_back(0, r.out_dm0),
        qdo[0].pass_on,
        stage_cols_back(0),
        then(ring.reduce_pair, kept('qkv', r.out_qkv0), give('qkv0')),
        then(pull_stage(r.xs0, r.g_attn.at[0], r.dms0, None, r.dga0), give('gl0')),
        ring.forward,
        stage_last,
    ]

    def tables():
        bias_tables(r.rel_bias, me, r.bias_rows, r.bias_cols)
        for copy in masks:
            copy.wait()

    use = lambda k: k
    after = lambda k: k + batch
    hooks = [
        (use(2), tables), (use(2), loaded('o', 0)), (use(6), loaded('gl', 0)), (use(6), loaded('out', 0)),
        (after(0), load('qkv', 1)), (use(10), loaded('qkv', 1)),
        (after(2), load('o', 1)), (use(12), loaded('o', 1)),
        (after(6), load('gl', 1)), (after(6), load('out', 1)), (use(16), loaded('gl', 1)), (use(16), loaded('out', 1)),
        (after(16), load('gl', 0)), (after(16), load('out', 0)), (use(26), loaded('gl', 0)), (use(26), loaded('out', 0)),
        (after(20), load('o', 0)), (use(30), loaded('o', 0)),
        (after(22), load('qkv', 0)), (use(32), loaded('qkv', 0)),
        (after(20), moves['u0'].pass_on), (after(26), moves['u1'].pass_on), (after(30), moves['gl1'].pass_on), (after(32), moves['qkv1'].pass_on),
        (after(31), lambda: bucket_sums(r.ds_sum, me, r.bias_sum)),
    ]

    def slot_step(slot, carry):
        for at, work in hooks:
            pl.when(slot == at)(work)
        for k, stage in enumerate(stages):
            @pl.when(jnp.logical_and(slot >= k, slot < batch + k))
            def _():
                stage(slot - k)
        return carry

    lax.fori_loop(0, batch + len(stages) - 1, slot_step, 0)
    for key in ('gl0', 'qkv0'):
        moves[key].pass_on()

    def finish(b, carry):
        for l in range(2):
            kv[l].finish(b)
            qdo[l].finish(b)
            for i in range(3):
                send_stats(l, b, i).wait_send()
        return carry

    lax.fori_loop(0, batch, finish, 0)
    for key in WIDE + NARROW:
        moves[key].finish()


def mega(x, dy, key_add, rel_bias, g_attn, g_mlp, w_q, w_k, w_v, w_o, w_gate, w_lin, w_out, cid):
    batch, rows, d_model = x.shape
    heads = rel_bias.shape[1]
    width, ff = heads * HEAD_DIM, w_gate.shape[2]
    n_cp, n_tp = 4, 8
    seg = rows // n_tp
    dma = pltpu.SemaphoreType.DMA
    any_spec = pl.BlockSpec(memory_space=pl.ANY)
    by_seg = lambda a: a.reshape(batch, n_tp, seg, d_model)
    ins = dict(x=(by_seg(x), any_spec), dy=(by_seg(dy), any_spec), dy_rows=(dy, any_spec), key_add=(key_add[:, None, :], VMEM_SPEC), mask_cols=(key_add[:, :, None], VMEM_SPEC), rel_bias=(rel_bias, SMEM_SPEC),
               g_attn=(g_attn[:, None, :], VMEM_SPEC), g_mlp=(g_mlp[:, None, :], VMEM_SPEC), w_q=(w_q, any_spec), w_k=(w_k, any_spec), w_v=(w_v, any_spec), w_o=(w_o, any_spec),
               w_gate=(w_gate, any_spec), w_lin=(w_lin, any_spec), w_out=(w_out, any_spec))
    size = dict(h=d_model, m=d_model, u=ff, gl=2 * ff, qkv=3 * width, o=width)
    outs = {}
    for key, n in size.items():
        for l in range(2):
            outs['out_%s%d' % (key, l)] = ((batch, rows, n), BF16)
    for key in ('d0', 'dm0', 'dm1', 'dx'):
        outs['out_' + key] = ((batch, n_tp, seg, d_model), BF16)
    for key in WIDE:
        shape = outs['out_' + key][0] if key != 'dy' else x.shape
        outs['got_' + key] = ((3,) + shape[:-1] + (d_model // 2,), BF16)
    for key in NARROW:
        outs['got_' + key] = ((3,) + outs['out_' + key][0], BF16)
    n_any = len(outs)
    for key in ('dga0', 'dga1', 'dgm0', 'dgm1'):
        outs[key] = ((1, d_model), F32)
    outs['bias_sum'] = ((rel_bias.shape[0], heads, n_cp * rows), F32)
    shard = pltpu.VMEM((batch, seg, d_model), BF16)
    blocks = pltpu.VMEM((batch, n_cp, rows, 2 * width), BF16)
    table = pltpu.VMEM((batch, n_cp, 2 * heads, rows), F32)
    chunk_f32 = pltpu.VMEM((batch, rows, ff), F32)
    q_rows = pltpu.VMEM((batch, rows, width), BF16)
    two = lambda n: pltpu.VMEM((2, rows, n), BF16)
    scratch = dict(wqkv=pltpu.VMEM((d_model, 3 * width), BF16), wo=pltpu.VMEM((width, d_model), BF16), wgl=pltpu.VMEM((d_model, 2 * ff), BF16), wout=pltpu.VMEM((ff, d_model), BF16),
                   sem_qkv=dma((3,)), sem_o=dma((1,)), sem_gl=dma((2,)), sem_out=dma((1,)), sem_in=dma((batch + 2,)), sem_mask=dma((2, 3)), mask_all=pltpu.VMEM((n_cp, batch, 1, rows), F32),
                   bias_rows=pltpu.VMEM((heads * rows, n_cp * rows), F32), bias_cols=pltpu.VMEM((n_cp, rows, heads * rows), F32), ds_sum=pltpu.VMEM((heads * rows, n_cp * rows), F32),
                   xs0=shard, x1s0=shard, xs1=shard, x1s1=shard, ds1=shard, dms1=shard, ds0=shard, dms0=shard, kv0=blocks, kv1=blocks, qdo0=blocks, qdo1=blocks, stats0=table, stats1=table,
                   q0=q_rows, q1=q_rows, dq=q_rows, gate=chunk_f32, lin=chunk_f32, hbuf=two(d_model), ubuf=two(ff), gbuf=two(2 * ff), qbuf=two(3 * width), obuf=two(width), dybuf=two(d_model),
                   sem_h=dma((2,)), sem_u=dma((2,)), sem_g=dma((2,)), sem_q=dma((2,)), sem_ob=dma((2,)), sem_dy=dma((2,)), sem_keep=dma((batch,)),
                   sem_wide=dma((2, len(WIDE), 3)), sem_narrow=dma((2, len(NARROW), 3)), sem_kv=dma((2, 2, 3, batch)), sem_qdo=dma((2, 2, 3, batch)), sem_stats=dma((2, 2, 3, batch)))
    for i, piece in enumerate(Ring.scratch(batch, seg, d_model)):
        scratch['ring_%d' % i] = piece
    result = pl.pallas_call(
        functools.partial(mega_kernel, list(ins) + list(outs) + list(scratch), heads),
        out_shape=tuple(jax.ShapeDtypeStruct(*v) for v in outs.values()),
        in_specs=[v[1] for v in ins.values()],
        out_specs=tuple([any_spec] * n_any + [VMEM_SPEC] * (len(outs) - n_any)),
        scratch_shapes=list(scratch.values()),
        compiler_params=comm_params(cid, 62),
        cost_estimate=cost(300),
        name='mega',
    )(*[v[0] for v in ins.values()])
    return dict(zip(outs, result))


def swap_kernel(n, *refs):
    halves, wo_part, small, mates, wo_own, wo_mate, total = refs[:n], refs[n], refs[n + 1], refs[n + 2:2 * n + 2], refs[2 * n + 2], refs[2 * n + 3], refs[2 * n + 4]
    wo_in, wo_sum, wo_x, stage, by_z, send, recv, s_send, s_recv, w_send, w_recv = refs[2 * n + 5:]
    _, z, y, pair, z_peer = tp_places()
    me, mate, across, _ = cp_places()
    core, chip = lax.rem(me, 2), me // 2
    half = wo_in.shape[-1]
    meet([pair] + z_peer[1:], [mate, across])

    def columns(which):
        return pl.ds(pl.multiple_of(which * half, half), half)

    first = remote(wo_part.at[:, :, columns(1 - core)], wo_in, w_send.at[0], w_recv.at[0], 'cp', mate)
    first.start()
    swaps = [remote(halves[i], mates[i], send.at[i], recv.at[i], 'cp', mate) for i in range(n)]
    for copy in swaps:
        copy.start()
    first.wait()
    wo_sum[:] = wo_part[:, :, columns(core)] + wo_in[:]
    second = remote(wo_sum.at[1 - chip], wo_x, w_send.at[1], w_recv.at[1], 'cp', across)
    second.start()
    mine = small
    for k, (axis, peer) in enumerate((('cp', mate), ('cp', across), ('tp', pair))):
        copy = remote(mine, stage.at[2 * k], s_send.at[k], s_recv.at[k], axis, peer)
        copy.start()
        copy.wait()
        if k < 2:
            stage[2 * k + 1] = mine[:] + stage[2 * k]
            mine = stage.at[2 * k + 1]
        else:
            by_z[z] = mine[:] + stage[2 * k]
    copies = [remote(by_z.at[z], by_z.at[z], s_send.at[2 + j], s_recv.at[2 + j], 'tp', z_peer[j]) for j in (1, 2, 3)]
    for copy in copies:
        copy.start()
    second.wait()
    wo_own[chip] = (wo_sum[chip] + wo_x[:]).astype(BF16)
    third = remote(wo_own.at[chip], wo_own.at[chip], w_send.at[2], w_recv.at[2], 'cp', across)
    third.start()
    for copy in copies:
        copy.wait()
    total[:] = by_z[0] + by_z[1] + by_z[2] + by_z[3]
    third.wait()
    last = remote(wo_own, wo_mate, w_send.at[3], w_recv.at[3], 'cp', mate)
    last.start()
    for copy in swaps + [last]:
        copy.wait()


def swap(halves, wo_part, small, cid):
    n = len(halves)
    layers, width, d_model = wo_part.shape
    half = d_model // 2
    any_spec = pl.BlockSpec(memory_space=pl.ANY)
    dma = pltpu.SemaphoreType.DMA
    wo_shape = jax.ShapeDtypeStruct((layers, width, half), BF16)
    result = pl.pallas_call(
        functools.partial(swap_kernel, n),
        out_shape=tuple(jax.ShapeDtypeStruct(h.shape, h.dtype) for h in halves) + (wo_shape, wo_shape, jax.ShapeDtypeStruct(small.shape, F32)),
        in_specs=[any_spec] * n + [VMEM_SPEC] * 2,
        out_specs=tuple([any_spec] * n + [VMEM_SPEC] * 3),
        scratch_shapes=[pltpu.VMEM((layers, width, half), F32), pltpu.VMEM((layers, width, half), F32), pltpu.VMEM((width, half), F32),
                        pltpu.VMEM((5,) + small.shape, F32), pltpu.VMEM((4,) + small.shape, F32), dma((n,)), dma((n,)), dma((6,)), dma((6,)), dma((4,)), dma((4,))],
        compiler_params=comm_params(cid, 24),
        name='swap',
    )(*halves, wo_part, small)
    return list(result[:n]), result[n], result[n + 1], result[n + 2]


def place_kernel(plan, n_out, *refs):
    n = len(plan)
    owns, mates, outs = refs[:n], refs[n:2 * n], refs[2 * n:2 * n + n_out]
    bufs, in_sem, out_sem = refs[2 * n + n_out:4 * n + n_out], refs[4 * n + n_out], refs[4 * n + n_out + 1]
    core = lax.rem(lax.axis_index('cp'), 2)
    loads = [pltpu.make_async_copy(src, buf, in_sem.at[i]) for i, (src, buf) in enumerate(zip(owns + mates, bufs))]
    for load in loads:
        load.start()
    stores = []
    for i, load in enumerate(loads):
        layer, by_rows, first_out, n_pieces = plan[i % n]
        which = core if i < n else 1 - core
        buf = bufs[i]
        load.wait()
        width = buf.shape[1] // n_pieces
        for p in range(n_pieces):
            src = buf if n_pieces == 1 else buf.at[:, pl.ds(p * width, width)]
            size = buf.shape[0] if by_rows else width
            window = pl.ds(pl.multiple_of(which * size, size), size)
            out = outs[first_out + p].at[layer]
            dst = out.at[window, :] if by_rows else out.at[:, window]
            stores.append(pltpu.make_async_copy(src, dst, out_sem.at[len(stores)]))
            stores[-1].start()
    for store in stores:
        store.wait()


def place(plan, owns, mates, out_shapes):
    n = len(plan)
    any_spec = pl.BlockSpec(memory_space=pl.ANY)
    n_stores = 2 * sum(p[3] for p in plan)
    return pl.pallas_call(
        functools.partial(place_kernel, plan, len(out_shapes)),
        out_shape=tuple(jax.ShapeDtypeStruct(s, BF16) for s in out_shapes),
        in_specs=[any_spec] * (2 * n),
        out_specs=tuple([any_spec] * len(out_shapes)),
        scratch_shapes=[pltpu.VMEM(a.shape, BF16) for a in list(owns) + list(mates)] + [pltpu.SemaphoreType.DMA((2 * n,)), pltpu.SemaphoreType.DMA((n_stores,))],
        compiler_params=pltpu.CompilerParams(vmem_limit_bytes=40 * MIB),
        name='place',
    )(*owns, *mates)


def solution(mesh):
    seq_spec = P(None, 'cp', None)
    col_spec = P(None, None, 'tp')
    row_spec = P(None, 'tp', None)
    weight_specs = (P(), P(), col_spec, col_spec, col_spec, row_spec, col_spec, col_spec, row_spec)

    def local_program(x_in, d_y, key_mask, rel_bias, g_attn, g_mlp, w_q, w_k, w_v, w_o, w_gate, w_lin, w_out):
        batch, rows, d_model = x_in.shape
        tokens = batch * rows
        n_layers = w_q.shape[0]
        n_buckets, heads = rel_bias.shape
        tp_index = lax.axis_index('tp')
        core = lax.rem(lax.axis_index('cp'), 2)
        half = d_model // 2

        key_add = jnp.where(key_mask > 0, 0.0, MASK_NEG).astype(F32)
        m = mega(x_in, d_y, key_add, rel_bias, g_attn, g_mlp, w_q, w_k, w_v, w_o, w_gate, w_lin, w_out, 0)

        def flat(array):
            return array.reshape(-1, array.shape[-1])

        def own_half(array):
            return lax.dynamic_slice_in_dim(array.reshape(tokens, d_model), core * half, half, axis=1)

        def grad(left, right, left_wide):
            a, b = [d_y if key == 'dy' else m['out_' + key] for key in (left, right)]
            a_g, b_g = flat(m['got_' + left]), flat(m['got_' + right])
            a, b = (own_half(a), flat(b)) if left_wide else (flat(a), own_half(b))
            return (dot_tn(a, b) + dot_tn(a_g, b_g)).astype(BF16)

        owns = [grad('h0', 'qkv0', True), grad('h1', 'qkv1', True), grad('m0', 'gl0', True), grad('m1', 'gl1', True), grad('u0', 'd0', False), grad('u1', 'dy', False)]
        wo_part = jnp.stack([dot_tn(flat(m['out_o%d' % l]), m['out_dm%d' % l].reshape(tokens, d_model)) for l in range(n_layers)])
        slots = jnp.zeros((8, n_buckets * heads), F32)
        slots = lax.dynamic_update_slice(slots, jnp.sum(m['bias_sum'], axis=-1).reshape(1, -1), (tp_index, jnp.int32(0)))
        small = jnp.concatenate([part.reshape(-1, 128) for part in (m['dga0'], m['dga1'], m['dgm0'], m['dgm1'], slots)], axis=0)
        mates, wo_own, wo_mate, small = swap(owns, wo_part, small, 1)
        n_gain = n_layers * d_model // 128
        d_g_attn = small[:n_gain].reshape(n_layers, d_model)
        d_g_mlp = small[n_gain:2 * n_gain].reshape(n_layers, d_model)
        d_rel = lax.dynamic_slice(small[2 * n_gain:], (tp_index, jnp.int32(0)), (1, n_buckets * heads)).reshape(n_buckets, heads)
        plan = tuple((layer, by_rows, first, n) for by_rows, first, n in ((True, 0, 3), (True, 4, 2), (False, 6, 1), (False, 3, 1)) for layer in range(n_layers))
        wo_halves = [[w[l] for l in range(n_layers)] for w in (wo_own, wo_mate)]
        grads = place(plan, owns + wo_halves[0], mates + wo_halves[1], [w.shape for w in (w_q, w_k, w_v, w_o, w_gate, w_lin, w_out)])
        return (m['out_dx'].reshape(batch, rows, d_model), d_rel, d_g_attn, d_g_mlp) + tuple(grads)

    return jax.shard_map(local_program, mesh=mesh, in_specs=(seq_spec, seq_spec, P(None, 'cp'), P(None, 'tp')) + weight_specs, out_specs=(seq_spec, P(None, 'tp')) + weight_specs, check_vma=False)
```

```python
import functools
import itertools
import string

import jax
import jax.numpy as jnp
from jax import lax
from jax.experimental import pallas as pl
from jax.experimental.pallas import tpu as pltpu
from jax.sharding import PartitionSpec as P

NORM_EPS = 1e-6
MASK_NEG = -1e9
BF16 = jnp.bfloat16
F32 = jnp.float32
VMEM = pltpu.VMEM
MESH = pl.DeviceIdType.MESH
MIB = 2 ** 20
HEAD_DIM = 64
VMEM_SPEC = pl.BlockSpec(memory_space=pltpu.VMEM)
SMEM_SPEC = pl.BlockSpec(memory_space=pltpu.SMEM)


def rel_bucket(rel_pos):
    distance = jnp.minimum(jnp.abs(rel_pos), 128)
    distance_sq = distance * distance
    log_part = 8 + sum((distance_sq >= 64 * 2 ** power).astype(jnp.int32) for power in range(1, 8))
    return jnp.where(distance < 8, distance, log_part) + 16 * (rel_pos > 0).astype(jnp.int32)


def comm_params(cid, mib):
    return pltpu.CompilerParams(collective_id=cid, has_side_effects=True, vmem_limit_bytes=mib * MIB)


def cost(gflops):
    return pl.CostEstimate(flops=gflops * 1000 * MIB, bytes_accessed=8 * MIB, transcendentals=MIB)


def dot_nt(a, b):
    return lax.dot_general(a, b, (((1,), (1,)), ((), ())), preferred_element_type=F32)


def dot_nn(a, b):
    return lax.dot_general(a, b, (((1,), (0,)), ((), ())), preferred_element_type=F32)


def dot_tn(a, b):
    return lax.dot_general(a, b, (((0,), (0,)), ((), ())), preferred_element_type=F32)


def stack_heads(block, heads):
    wide = block.astype(F32)
    lane_head = lax.broadcasted_iota(jnp.int32, block.shape, 1) // HEAD_DIM
    return jnp.concatenate([jnp.where(lane_head == h, wide, 0.0).astype(BF16) for h in range(heads)], axis=0)


def pick_heads(stacked, heads, rows):
    lane_head = lax.broadcasted_iota(jnp.int32, (rows, stacked.shape[1]), 1) // HEAD_DIM
    out = stacked[:rows]
    for h in range(1, heads):
        out = jnp.where(lane_head == h, stacked[h * rows:(h + 1) * rows], out)
    return out


def cp_places():
    me = lax.axis_index('cp')
    mate = me + 1 - 2 * lax.rem(me, 2)
    across = lax.rem(me + 2, 4)
    diagonal = lax.rem(mate + 2, 4)
    return me, mate, across, diagonal


def rms_parts(x_f, gain):
    inv_rms = lax.rsqrt(jnp.mean(x_f * x_f, axis=-1, keepdims=True) + NORM_EPS)
    return (x_f * inv_rms * gain).astype(BF16)


GELU_C = 0.7978845608028654
GELU_A = 0.044715


def gelu_parts(x):
    t = jnp.tanh(GELU_C * (x + GELU_A * x * x * x))
    cdf = 0.5 * (1.0 + t)
    return x * cdf, cdf + 0.5 * x * (1.0 - t * t) * GELU_C * (1.0 + 3.0 * GELU_A * x * x)


Z_STEPS = (2, 1, 3)


def remote(src, dst, sem, at, axis, peer):
    return pltpu.make_async_remote_copy(src_ref=src, dst_ref=dst, send_sem=sem.at[(0,) + at], recv_sem=sem.at[(1,) + at], device_id={axis: peer}, device_id_type=MESH)


def tp_places():
    me = lax.axis_index('tp')
    z, y = me // 2, lax.rem(me, 2)
    pair = me + 1 - 2 * y
    return me, z, y, pair, [2 * lax.rem(z + j, 4) + y for j in range(4)]


def meet(tp_peers, cp_peers):
    barrier = pltpu.get_barrier_semaphore()
    for axis, peers in (('tp', tp_peers), ('cp', cp_peers)):
        for peer in peers:
            pl.semaphore_signal(barrier, inc=1, device_id={axis: peer}, device_id_type=MESH)
    pl.semaphore_wait(barrier, len(tp_peers) + len(cp_peers))


class Ring:
    def __init__(self, part, from_y, from_z, full, *sems):
        self.part, self.from_y, self.from_z, self.full = part, from_y, from_z, full
        self.sem_ys, self.sem_zs, self.sem_zg, self.sem_yg = sems
        _, self.z, self.y, self.pair, self.z_peer = tp_places()
        self.seg = self.y * 4 + self.z

    @staticmethod
    def scratch(batch, seg, d_model):
        dma = pltpu.SemaphoreType.DMA
        return [
            pltpu.VMEM((batch, 2, 4, seg, d_model), F32),
            pltpu.VMEM((batch, 4, seg, d_model), F32),
            pltpu.VMEM((batch, 3, seg, d_model), F32),
            pltpu.VMEM((batch, 8, seg, d_model), BF16),
            dma((2, batch)), dma((2, batch, 3)), dma((2, batch, 3)), dma((2, batch, 4)),
        ]

    def y_sum(self, b):
        return remote(self.part.at[b, 1 - self.y], self.from_y.at[b], self.sem_ys, (b,), 'tp', self.pair)

    def z_sum(self, b, j):
        return remote(self.part.at[b, self.y, lax.rem(self.z + j, 4)], self.from_z.at[b, j - 1], self.sem_zs, (b, j - 1), 'tp', self.z_peer[j])

    def z_gather(self, b, j):
        ref = self.full.at[b, self.seg]
        return remote(ref, ref, self.sem_zg, (b, j - 1), 'tp', self.z_peer[j])

    def y_gather(self, b, j):
        ref = self.full.at[b, self.y * 4 + lax.rem(self.z - j + 4, 4)]
        return remote(ref, ref, self.sem_yg, (b, j), 'tp', self.pair)

    def send_partial(self, b, partial):
        self.part[b] = partial.reshape(self.part.shape[1:])
        self.y_sum(b).start()

    def reduce_pair(self, b):
        self.y_sum(b).wait_recv()
        self.part[b, self.y] = self.part[b, self.y] + self.from_y[b]
        for j in Z_STEPS:
            self.z_sum(b, j).start()

    def reduced(self, b):
        for j in Z_STEPS:
            self.z_sum(b, j).wait_recv()
        return self.part[b, self.y, self.z] + self.from_z[b, 0] + self.from_z[b, 1] + self.from_z[b, 2]

    def publish(self, b, out):
        self.full[b, self.seg] = out
        for j in Z_STEPS:
            self.z_gather(b, j).start()
        self.y_gather(b, 0).start()

    def forward(self, b):
        for j in Z_STEPS:
            self.z_gather(b, j).wait_recv()
            self.y_gather(b, j).start()

    def arrive(self, b):
        for j in range(4):
            self.y_gather(b, j).wait_recv()
        self.y_sum(b).wait_send()
        for j in range(4):
            self.y_gather(b, j).wait_send()
        for j in Z_STEPS:
            self.z_sum(b, j).wait_send()
            self.z_gather(b, j).wait_send()

    def rows(self, b):
        return self.full[b].reshape(-1, self.full.shape[-1])


class Columns:
    def __init__(self, store, z_sem, y_sem):
        self.store, self.z_sem, self.y_sem = store, z_sem, y_sem
        self.me, self.z, self.y, self.pair, self.z_peer = tp_places()

    def z_gather(self, b, j):
        ref = self.store.at[b, self.me]
        return remote(ref, ref, self.z_sem, (b, j - 1), 'tp', self.z_peer[j])

    def y_gather(self, b, j):
        ref = self.store.at[b, 2 * lax.rem(self.z - j + 4, 4) + self.y]
        return remote(ref, ref, self.y_sem, (b, j), 'tp', self.pair)

    def publish(self, b, out):
        self.store[b, self.me] = out
        for j in Z_STEPS:
            self.z_gather(b, j).start()
        self.y_gather(b, 0).start()

    def forward(self, b):
        for j in Z_STEPS:
            self.z_gather(b, j).wait_recv()
            self.y_gather(b, j).start()

    def arrive(self, b):
        for j in range(4):
            self.y_gather(b, j).wait_recv()
        for j in range(4):
            self.y_gather(b, j).wait_send()
        for j in Z_STEPS:
            self.z_gather(b, j).wait_send()

    def rows(self, b):
        return jnp.concatenate([self.store[b, t] for t in range(self.store.shape[1])], axis=1)


class Trade:
    def __init__(self, store, sem, layer):
        self.store, self.sem, self.layer = store, sem, layer
        self.me, self.mate, self.across, self.diagonal = cp_places()

    def copy(self, b, r):
        ref = self.store.at[b, self.across if r == 2 else self.me]
        return remote(ref, ref, self.sem, (self.layer, r, b), 'cp', self.across if r == 1 else self.mate)

    def give(self, b):
        self.copy(b, 1).start()
        self.copy(b, 0).start()

    def pass_on(self, b):
        self.copy(b, 1).wait_recv()
        self.copy(b, 2).start()

    def take(self, b):
        self.copy(b, 0).wait_recv()
        self.copy(b, 2).wait_recv()

    def finish(self, b):
        for r in range(3):
            self.copy(b, r).wait_send()


class Wide:
    def __init__(self, src, dst, sem, index):
        self.src, self.dst, self.sem, self.index = src, dst, sem, index
        me, *self.peers = cp_places()
        mate, across, diagonal = self.peers
        self.peers = (mate, across, diagonal)
        self.core = lax.rem(me, 2)

    def copy(self, r, window):
        n = self.dst.shape[-1]
        want = self.core if r == 1 else 1 - self.core
        columns = pl.ds(pl.multiple_of(want * n, n), n)
        return remote(self.src.at[window].at[..., columns], self.dst.at[r].at[window], self.sem, (self.index, r), 'cp', self.peers[r])

    def give(self, b):
        for r in (1, 2, 0):
            self.copy(r, pl.ds(b, 1)).start()

    def pass_on(self):
        pass

    def finish(self):
        for r in range(3):
            self.copy(r, pl.ds(0, self.src.shape[0])).wait()


class Narrow:
    def __init__(self, src, dst, sem, index):
        self.src, self.dst, self.sem, self.index = src, dst, sem, index
        _, self.mate, self.across, _ = cp_places()

    def copy(self, r, window):
        src = self.src if r < 2 else self.dst.at[1]
        return remote(src.at[window], self.dst.at[r].at[window], self.sem, (self.index, r), 'cp', self.across if r == 1 else self.mate)

    def give(self, b):
        for r in (1, 0):
            self.copy(r, pl.ds(b, 1)).start()

    def pass_on(self):
        every = pl.ds(0, self.src.shape[0])
        self.copy(1, every).wait_recv()
        self.copy(2, every).start()

    def finish(self):
        every = pl.ds(0, self.src.shape[0])
        self.copy(0, every).wait()
        self.copy(1, every).wait_send()
        self.copy(2, every).wait()


class Spill:
    def __init__(self, slots, sem):
        self.slots, self.sem = slots, sem

    def copy(self, out, b):
        slot = lax.rem(b, 2)
        return pltpu.make_async_copy(self.slots.at[slot], out.at[b], self.sem.at[slot])

    def put(self, out, b, value):
        self.slots[lax.rem(b, 2)] = value
        self.copy(out, b).start()


def norm_rows(rows, gain):
    return rms_parts(rows.astype(F32), gain)


def rms_pull(total, x_shard, gain, res, d_gain_ref):
    d_norm = total.astype(BF16).astype(F32)
    x_f = x_shard.astype(F32)
    inv_rms = lax.rsqrt(jnp.mean(x_f * x_f, axis=-1, keepdims=True) + NORM_EPS)
    normed = x_f * inv_rms
    d_gain_ref[:] += jnp.sum(d_norm * normed, axis=0, keepdims=True)
    d_normed = d_norm * gain
    d_x = inv_rms * (d_normed - normed * jnp.mean(d_normed * normed, axis=-1, keepdims=True))
    return (res.astype(F32) + d_x).astype(BF16)


def mlp_pull(d_u, gate, lin):
    d_u = d_u.astype(BF16).astype(F32)
    value, slope = gelu_parts(gate)
    return jnp.concatenate([(d_u * lin * slope).astype(BF16), (d_u * value).astype(BF16)], axis=1)


def row_sum(x):
    return jnp.sum(x, axis=1, keepdims=True)


def row_max(x):
    return jnp.max(x, axis=1, keepdims=True)


def mask_row(mask_ref, b):
    return jnp.concatenate([mask_ref[c, b] for c in range(mask_ref.shape[0])], axis=1)


def attend(heads, q, kv, bias, mask):
    rows, width = q.shape
    scores = dot_nt(stack_heads(q, heads), kv[:, :width]) + bias + mask
    top = row_max(scores)
    probs = jnp.exp(scores - top)
    total = row_sum(probs)
    out = dot_nn(probs.astype(BF16), kv[:, width:]) / total
    return pick_heads(out, heads, rows).astype(BF16)


def attend_rows_back(heads, qdo, kv, bias, mask, ds_ref):
    rows, wide = qdo.shape
    width = wide // 2
    keys, vals = kv[:, :width], kv[:, width:]
    scores = dot_nt(stack_heads(qdo[:, :width], heads), keys) + bias + mask
    top = row_max(scores)
    unnorm = jnp.exp(scores - top)
    total = row_sum(unnorm)
    log_norm = top + jnp.log(total)
    probs = unnorm * (1.0 / total)
    d_probs = dot_nt(stack_heads(qdo[:, width:], heads), vals)
    row_dot = row_sum(probs * d_probs)
    lane = lax.broadcasted_iota(jnp.int32, (rows, rows), 1)
    table = jnp.zeros((rows, rows), F32)
    for h in range(heads):
        table = jnp.where(lane == h, log_norm[h * rows:(h + 1) * rows], table)
        table = jnp.where(lane == heads + h, row_dot[h * rows:(h + 1) * rows], table)
    d_scores = probs * (d_probs - row_dot)
    ds_ref[:] += d_scores
    d_q = dot_nn(d_scores.astype(BF16), keys)
    return pick_heads(d_q, heads, rows).astype(BF16), jnp.transpose(table)[:2 * heads]


def attend_cols_back(heads, own_kv, mask_col, bias_ref, qdo_of, stats_of):
    rows, wide = own_kv.shape
    width = wide // 2
    keys, vals = own_kv[:, :width], own_kv[:, width:]

    def block(src, acc):
        d_k, d_v = acc
        qdo, stats = qdo_of(src), stats_of(src)
        log_norm = jnp.concatenate([stats[h:h + 1] for h in range(heads)], axis=1)
        row_dot = jnp.concatenate([stats[heads + h:heads + h + 1] for h in range(heads)], axis=1)
        q_st = stack_heads(qdo[:, :width], heads)
        do_st = stack_heads(qdo[:, width:], heads)
        probs = jnp.exp(dot_nt(keys, q_st) + bias_ref[src] + mask_col - log_norm)
        d_scores = probs * (dot_nt(vals, do_st) - row_dot)
        return d_k + dot_nn(d_scores.astype(BF16), q_st), d_v + dot_nn(probs.astype(BF16), do_st)

    zero = jnp.zeros((rows, width), F32)
    d_k, d_v = lax.fori_loop(0, bias_ref.shape[0], block, (zero, zero))
    return jnp.concatenate([d_k, d_v], axis=1).astype(BF16)


def bias_tables(table_ref, me, rows_ref, cols_ref):
    n_buckets, heads = table_ref.shape
    rows = rows_ref.shape[0] // heads
    seq = rows_ref.shape[1]

    def strip(i, carry):
        first = pl.multiple_of(i * 8, 8)
        rel = lax.broadcasted_iota(jnp.int32, (8, seq), 1) - lax.broadcasted_iota(jnp.int32, (8, seq), 0) - me * rows - first
        for is_col in (False, True):
            buckets = rel_bucket(-rel if is_col else rel)
            vals = [jnp.zeros((8, seq), F32) for _ in range(heads)]
            for k in range(n_buckets):
                hit = buckets == k
                vals = [jnp.where(hit, table_ref[k, h], v) for h, v in enumerate(vals)]
            for h, v in enumerate(vals):
                if is_col:
                    for q in range(seq // rows):
                        cols_ref[q, pl.ds(first, 8), h * rows:(h + 1) * rows] = v[:, q * rows:(q + 1) * rows]
                else:
                    rows_ref[pl.ds(pl.multiple_of(h * rows + first, 8), 8), :] = v
        return carry

    lax.fori_loop(0, rows // 8, strip, 0)


def bucket_sums(ds_ref, me, out_ref):
    n_buckets, heads, seq = out_ref.shape
    rows = ds_ref.shape[0] // heads
    rel = lax.broadcasted_iota(jnp.int32, (rows, seq), 1) - lax.broadcasted_iota(jnp.int32, (rows, seq), 0) - me * rows

    def step(k, carry):
        hit = rel_bucket(rel) == k
        out_ref[k] = jnp.concatenate([jnp.sum(jnp.where(hit, ds_ref[h * rows:(h + 1) * rows], 0.0), axis=0, keepdims=True) for h in range(heads)], axis=0)
        return carry

    lax.fori_loop(0, n_buckets, step, 0)


class Refs:
    pass


WIDE = ('h0', 'h1', 'm0', 'm1', 'dy', 'd0')
NARROW = ('u0', 'u1', 'gl0', 'gl1', 'qkv0', 'qkv1')
LETTERS = string.ascii_letters
STEPS = '0212221212110211211110011010110101112'
ORDER = 'jDAFnGlykdCKuHfIteqExvJhcbosapzgmiwrB'
GIVES = tuple(zip(('h0', 'dy', 'm0', 'h1', 'u0', 'gl1', 'qkv1', 'm1', 'gl0', 'qkv0', 'u1', 'd0'), map(LETTERS.index, 'dhnuvBCEHIKK')))


def mega_kernel(names, heads, *refs):
    r = Refs()
    for key, ref in zip(names, refs):
        setattr(r, key, ref)
    batch, n_seg, seg, d_model = r.x.shape
    rows = n_seg * seg
    ff = r.w_out.shape[1]
    width = heads * HEAD_DIM
    ring = Ring(*[getattr(r, 'ring_%d' % i) for i in range(8)])
    gather_o = Columns(r.o_all, r.sem_oz, r.sem_oy)
    gather_x = Columns(r.x_all, r.sem_xz, r.sem_xy)
    me, mate, across, diagonal = cp_places()
    tp_me = gather_o.me
    others = (mate, across, diagonal)
    my_columns = pl.ds(pl.multiple_of(tp_me * width, width), width)

    def weight(buf, sem, sources, layer):
        out, col = [], 0
        for i, src in enumerate(sources):
            n = src.shape[-1]
            out.append(pltpu.make_async_copy(src.at[layer], buf.at[:, pl.ds(col, n)] if len(sources) > 1 else buf, sem.at[i]))
            col += n
        return out

    weights = dict(qkv=(r.wqkv, r.sem_qkv, (r.w_q, r.w_k, r.w_v)), o=(r.wo, r.sem_o, (r.w_o,)), gl=(r.wgl, r.sem_gl, (r.w_gate, r.w_lin)), out=(r.wout, r.sem_out, (r.w_out,)))

    def load(key, layer):
        def go():
            for copy in weight(*weights[key], layer):
                copy.start()
        return go

    def loaded(key, layer):
        def go():
            for copy in weight(*weights[key], layer):
                copy.wait()
        return go

    for key, layer in (('qkv', 0), ('o', 1), ('gl', 0), ('out', 0)):
        load(key, layer)()
    rows_in = [pltpu.make_async_copy(r.x.at[b], ring.full.at[b], r.sem_in.at[b]) for b in range(batch)]
    shards_in = [(r.x.at[:, ring.seg], r.xs0), (r.dy.at[:, ring.seg], r.ds1), (r.x_rows.at[:, :, my_columns], r.x_col)]
    shards_in = [pltpu.make_async_copy(src, dst, r.sem_in.at[batch + i]) for i, (src, dst) in enumerate(shards_in)]
    deal_own = [pltpu.make_async_copy(r.w_deal.at[l, me, :, my_columns], r.w_cols.at[l, me, tp_me], r.sem_deal_in.at[l]) for l in range(2)]
    for copy in rows_in + shards_in + deal_own:
        copy.start()
    r.key_add[:] = jnp.where(r.key_mask[:] > 0, 0.0, MASK_NEG).astype(F32)[:, None, :]
    peers = [lax.rem(tp_me + j, n_seg) for j in range(n_seg)]
    meet(peers[1:], others)
    masks = [remote(r.key_add, r.mask_all.at[me], r.sem_mask, (i,), 'cp', peer) for i, peer in enumerate(others)]
    for copy in masks:
        copy.start()
    r.mask_all[me] = r.key_add[:]

    def deal(l, j):
        window = pl.ds(pl.multiple_of(peers[j] * width, width), width)
        return remote(r.w_deal.at[l, me, :, window], r.w_cols.at[l, me, tp_me], r.sem_deal, (l, j), 'tp', peers[j])

    def share(l, i):
        ref = r.w_cols.at[l, across if i == 2 else me]
        return remote(ref, ref, r.sem_share, (l, i), 'cp', across if i == 1 else mate)

    for l in range(2):
        for j in range(1, n_seg):
            deal(l, j).start()

    def share_start(l):
        def go():
            for j in range(1, n_seg):
                deal(l, j).wait()
            deal_own[l].wait()
            share(l, 1).start()
            share(l, 0).start()
        return go

    def share_pass(l):
        def go():
            share(l, 1).wait_recv()
            share(l, 2).start()
        return go

    def shared(l):
        def go():
            share(l, 0).wait()
            share(l, 1).wait_send()
            share(l, 2).wait()
            for c in range(r.w_cols.shape[1]):
                for t in range(n_seg):
                    r.w_now[t, c] = r.w_cols[l, c, t]
        return go

    for ref in (r.ds_sum, r.dga0, r.dga1, r.dgm0, r.dgm1):
        ref[:] = jnp.zeros_like(ref)
    for copy in rows_in + shards_in:
        copy.wait()
    loaded('qkv', 0)()

    hold = dict(h=Spill(r.hbuf, r.sem_h), u=Spill(r.ubuf, r.sem_u), gl=Spill(r.gbuf, r.sem_g), qkv=Spill(r.qbuf, r.sem_q), o=Spill(r.obuf, r.sem_ob))
    moves = {}
    for i, key in enumerate(WIDE):
        moves[key] = Wide(r.dy_rows if key == 'dy' else getattr(r, 'out_' + key), getattr(r, 'got_' + key), r.sem_wide, i)
    for i, key in enumerate(NARROW):
        moves[key] = Narrow(getattr(r, 'out_' + key), getattr(r, 'got_' + key), r.sem_narrow, i)
    kv = [Trade(store, r.sem_kv, l) for l, store in enumerate((r.kv0, r.kv1))]
    qdo = [Trade(store, r.sem_qdo, l) for l, store in enumerate((r.qdo0, r.qdo1))]
    q_own = (r.q0, r.q1)
    stats = (r.stats0, r.stats1)

    def send_stats(l, b, i):
        ref = stats[l].at[b, me]
        return remote(ref, ref, r.sem_stats, (l, i, b), 'cp', others[i])

    def out(key, l):
        return getattr(r, 'out_%s%d' % (key, l))

    def project(l, b, flat):
        h = norm_rows(flat, r.g_attn[l:l + 1])
        hold['h'].put(out('h', l), b, h)
        qkv = dot_nn(h, r.wqkv[:]).astype(BF16)
        q_own[l][b] = qkv[:, :width]
        kv[l].store[b, me] = qkv[:, width:]
        kv[l].give(b)

    def stage_first(b):
        project(0, b, ring.rows(b))

    def stage_attend(l):
        def go(b):
            kv[l].take(b)
            pairs = kv[l].store[b].reshape(-1, 2 * width)
            o = attend(heads, q_own[l][b], pairs, r.bias_rows[:], mask_row(r.mask_all, b))
            gather_o.publish(b, o)
            hold['o'].put(out('o', l), b, o)
        return go

    def stage_columns(l):
        def go(b):
            gather_o.arrive(b)
            prod = dot_nn(gather_o.rows(b), r.w_now[:].reshape(d_model, width))
            gather_x.publish(b, (r.x_col[b].astype(F32) + prod).astype(BF16))
        return go

    def add_stage(res, dst):
        def go(b):
            total = ring.reduced(b)
            value = (res[b].astype(F32) + total).astype(BF16)
            dst[b] = value
            ring.publish(b, value)
        return go

    def pull_stage(x_shard, gain, l, res, dst, d_gain):
        def go(b):
            value = rms_pull(ring.reduced(b), x_shard[b], gain[l:l + 1], res[b], d_gain)
            if dst is not None:
                dst[b] = value
            ring.publish(b, value)
        return go

    def mlp_forward(l, b, shard):
        gather_x.arrive(b)
        window = pl.ds(pl.multiple_of(ring.seg * seg, seg), seg)
        shard[b] = jnp.concatenate([r.x_all[b, t, window] for t in range(n_seg)], axis=1)
        h2 = norm_rows(gather_x.rows(b), r.g_mlp[l:l + 1])
        hold['h'].put(out('m', l), b, h2)
        both = dot_nn(h2, r.wgl[:])
        gate, lin = both[:, :ff], both[:, ff:]
        u = (gelu_parts(gate)[0] * lin).astype(BF16)
        hold['u'].put(out('u', l), b, u)
        return gate, lin, u

    def stage_mlp0(b):
        gate, lin, u = mlp_forward(0, b, r.x1s0)
        r.gate[b] = gate
        r.lin[b] = lin
        ring.send_partial(b, dot_nn(u, r.wout[:]))

    def stage_next(b):
        ring.arrive(b)
        r.x_col[b] = ring.full[b, :, :, my_columns].reshape(rows, width)
        project(1, b, ring.rows(b))

    def dy_in(b):
        slot = lax.rem(b, 2)
        return pltpu.make_async_copy(r.dy_rows.at[b], r.dybuf.at[slot], r.sem_dy.at[slot])

    def mlp_backward(l, b, d, gate, lin, copy=None):
        dgl = mlp_pull(dot_nt(d, r.wout[:]), gate, lin)
        hold['gl'].put(out('gl', l), b, dgl)
        if copy is not None:
            copy.wait()
        ring.send_partial(b, dot_nt(dgl, r.wgl[:]))

    def stage_mlp1(b):
        gate, lin, _ = mlp_forward(1, b, r.x1s1)
        dy_in(b).wait()
        mlp_backward(1, b, r.dybuf[lax.rem(b, 2)], gate, lin)

    def keep(dst, b):
        copy = pltpu.make_async_copy(ring.full.at[b], dst.at[b], r.sem_keep.at[b])
        copy.start()
        return copy

    def stage_rows_back(l, dst):
        def go(b):
            ring.arrive(b)
            copy = keep(dst, b)
            d_o = dot_nt(ring.rows(b), r.wo[:]).astype(BF16)
            both = jnp.concatenate([q_own[l][b], d_o], axis=1)
            qdo[l].store[b, me] = both
            qdo[l].give(b)
            pairs = kv[l].store[b].reshape(-1, 2 * width)
            d_q, table = attend_rows_back(heads, both, pairs, r.bias_rows[:], mask_row(r.mask_all, b), r.ds_sum)
            stats[l][b, me] = table
            r.dq[b] = d_q
            for i in range(3):
                send_stats(l, b, i).start()
            copy.wait()
        return go

    def stage_cols_back(l):
        def go(b):
            qdo[l].take(b)
            for i in range(3):
                send_stats(l, b, i).wait_recv()
            mask_col = jnp.transpose(jnp.broadcast_to(r.key_add[b], (rows, rows)))[:, :1]
            d_kv = attend_cols_back(heads, kv[l].store[b, me], mask_col, r.bias_cols, lambda s: qdo[l].store[b, s], lambda s: stats[l][b, s])
            d_qkv = jnp.concatenate([r.dq[b], d_kv], axis=1)
            hold['qkv'].put(out('qkv', l), b, d_qkv)
            ring.send_partial(b, dot_nt(d_qkv, r.wqkv[:]))
        return go

    def stage_mlp_back0(b):
        ring.arrive(b)
        copy = keep(r.out_d0, b)
        mlp_backward(0, b, ring.rows(b), r.gate[b], r.lin[b], copy)

    def stage_last(b):
        ring.arrive(b)
        keep(r.out_dx, b).wait()

    def by_columns(tag, l):
        return [('at' + tag, stage_attend(l)), ('', gather_o.forward), ('col' + tag, stage_columns(l)), ('', gather_x.forward)]

    def by_sum(tag, start, finish):
        return [(tag, start), ('', ring.reduce_pair), ('', finish), ('', ring.forward)]

    stages = (
        [('first', stage_first), ('', kv[0].pass_on)] + by_columns('0', 0)
        + by_sum('mlp0', stage_mlp0, add_stage(r.x1s0, r.xs1))
        + [('next', stage_next), ('', kv[1].pass_on)] + by_columns('1', 1)
        + by_sum('mlp1', stage_mlp1, pull_stage(r.x1s1, r.g_mlp, 1, r.ds1, r.dms1, r.dgm1))
        + [('rows1', stage_rows_back(1, r.out_dm1)), ('', qdo[1].pass_on)]
        + by_sum('cols1', stage_cols_back(1), pull_stage(r.xs1, r.g_attn, 1, r.dms1, r.ds0, r.dga1))
        + by_sum('back0', stage_mlp_back0, pull_stage(r.x1s0, r.g_mlp, 0, r.ds0, r.dms0, r.dgm0))
        + [('rows0', stage_rows_back(0, r.out_dm0)), ('', qdo[0].pass_on)]
        + by_sum('cols0', stage_cols_back(0), pull_stage(r.xs0, r.g_attn, 0, r.dms0, None, r.dga0))
        + [('last', stage_last)])
    lags = list(itertools.accumulate(int(step) for step in STEPS))
    order = [LETTERS.index(letter) for letter in ORDER]
    lag_of = {tag: lag for (tag, _), lag in zip(stages, lags)}
    use = lambda tag: lag_of[tag]
    after = lambda tag: lag_of[tag] + batch

    def tables():
        bias_tables(r.rel_bias, me, r.bias_rows, r.bias_cols)
        for copy in masks:
            copy.wait()

    once = [
        (use('at0'), tables), (use('mlp0'), loaded('gl', 0)), (use('mlp0'), loaded('out', 0)),
        (2, share_start(0)), (3, share_pass(0)), (use('col0'), shared(0)), (use('col0'), share_start(1)), (after('col0'), share_pass(1)), (use('col1'), shared(1)),
        (after('first'), load('qkv', 1)), (use('next'), loaded('qkv', 1)),
        (after('mlp0'), load('gl', 1)), (after('mlp0'), load('out', 1)), (use('mlp1'), loaded('gl', 1)), (use('mlp1'), loaded('out', 1)),
        (after('mlp1'), load('gl', 0)), (after('mlp1'), load('out', 0)), (use('back0'), loaded('gl', 0)), (use('back0'), loaded('out', 0)),
        (use('rows1'), loaded('o', 1)), (after('rows1'), load('o', 0)), (use('rows0'), loaded('o', 0)),
        (after('cols1'), load('qkv', 0)), (use('cols0'), loaded('qkv', 0)),
        (after('rows0'), lambda: bucket_sums(r.ds_sum, me, r.bias_sum)),
    ]
    early = [(use(tag) + 1, hold[key], ref) for tag, key, ref in (
        ('first', 'h', r.out_h0), ('at0', 'o', r.out_o0), ('mlp0', 'h', r.out_m0), ('mlp0', 'u', r.out_u0), ('next', 'h', r.out_h1), ('at1', 'o', r.out_o1),
        ('mlp1', 'h', r.out_m1), ('mlp1', 'u', r.out_u1), ('mlp1', 'gl', r.out_gl1), ('cols1', 'qkv', r.out_qkv1), ('back0', 'gl', r.out_gl0), ('cols0', 'qkv', r.out_qkv0))]
    gives = dict(GIVES)
    passes = [(gives[key] + 2 * batch, moves[key].pass_on) for key in NARROW]
    n_slots = batch + lags[-1]

    def chunk_at(slot, lag, work):
        @pl.when(jnp.logical_and(slot >= lag, slot < batch + lag))
        def _():
            work(slot - lag)

    def slot_step(slot, carry):
        for at, work in once + passes:
            if at < n_slots:
                pl.when(slot == at)(work)
        for lag, spill, ref in early:
            chunk_at(slot, lag, lambda b: spill.copy(ref, b).wait())
        chunk_at(slot, use('mlp1') - 1, lambda b: dy_in(b).start())
        for k in order:
            chunk_at(slot, lags[k], stages[k][1])
        for key, lag in GIVES:
            chunk_at(slot, lag, moves[key].give)
        return carry

    lax.fori_loop(0, n_slots, slot_step, 0)
    for at, work in passes:
        if at >= n_slots:
            work()

    def finish(b, carry):
        for l in range(2):
            kv[l].finish(b)
            qdo[l].finish(b)
            for i in range(3):
                send_stats(l, b, i).wait_send()
        return carry

    lax.fori_loop(0, batch, finish, 0)
    for key in WIDE + NARROW:
        moves[key].finish()


def mega(x, dy, key_mask, rel_bias, g_attn, g_mlp, w_q, w_k, w_v, w_o, w_gate, w_lin, w_out, cid):
    batch, rows, d_model = x.shape
    heads = rel_bias.shape[1]
    width, ff = heads * HEAD_DIM, w_gate.shape[2]
    n_cp, n_tp = 4, 8
    seg = rows // n_tp
    quarter = width // n_cp
    dma = pltpu.SemaphoreType.DMA
    any_spec = pl.BlockSpec(memory_space=pl.ANY)
    by_seg = lambda a: a.reshape(batch, n_tp, seg, d_model)
    in_hbm = dict(x=by_seg(x), x_rows=x, dy=by_seg(dy), dy_rows=dy, w_q=w_q, w_k=w_k, w_v=w_v, w_o=w_o, w_deal=w_o.reshape(-1, n_cp, quarter, d_model), w_gate=w_gate, w_lin=w_lin, w_out=w_out)
    ins = {key: (value, any_spec) for key, value in in_hbm.items()}
    ins.update(key_mask=(key_mask, VMEM_SPEC), rel_bias=(rel_bias, SMEM_SPEC), g_attn=(g_attn, VMEM_SPEC), g_mlp=(g_mlp, VMEM_SPEC))
    size = dict(h=d_model, m=d_model, u=ff, gl=2 * ff, qkv=3 * width, o=width)
    outs = {}
    for key, n in size.items():
        for l in range(2):
            outs['out_%s%d' % (key, l)] = ((batch, rows, n), BF16)
    for key in ('d0', 'dm0', 'dm1', 'dx'):
        outs['out_' + key] = ((batch, n_tp, seg, d_model), BF16)
    for key in WIDE:
        shape = outs['out_' + key][0] if key != 'dy' else x.shape
        outs['got_' + key] = ((3,) + shape[:-1] + (d_model // 2,), BF16)
    for key in NARROW:
        outs['got_' + key] = ((3,) + outs['out_' + key][0], BF16)
    n_any = len(outs)
    for key in ('dga0', 'dga1', 'dgm0', 'dgm1'):
        outs[key] = ((1, d_model), F32)
    outs['bias_sum'] = ((rel_bias.shape[0], heads, n_cp * rows), F32)
    vmem = lambda *shape: pltpu.VMEM(shape, BF16)
    wide = lambda *shape: pltpu.VMEM(shape, F32)
    scratch = dict(wqkv=vmem(d_model, 3 * width), wo=vmem(width, d_model), wgl=vmem(d_model, 2 * ff), wout=vmem(ff, d_model), w_cols=vmem(2, n_cp, n_tp, quarter, width), w_now=vmem(n_tp, n_cp, quarter, width),
                   o_all=vmem(batch, n_tp, rows, width), x_all=vmem(batch, n_tp, rows, width), key_add=wide(batch, 1, rows), mask_all=wide(n_cp, batch, 1, rows),
                   bias_rows=wide(heads * rows, n_cp * rows), bias_cols=wide(n_cp, rows, heads * rows), ds_sum=wide(heads * rows, n_cp * rows), gate=wide(batch, rows, ff), lin=wide(batch, rows, ff))
    for key in ('xs0', 'x1s0', 'xs1', 'x1s1', 'ds1', 'dms1', 'ds0', 'dms0'):
        scratch[key] = vmem(batch, seg, d_model)
    for key in ('kv0', 'kv1', 'qdo0', 'qdo1'):
        scratch[key] = vmem(batch, n_cp, rows, 2 * width)
    for key in ('stats0', 'stats1'):
        scratch[key] = wide(batch, n_cp, 2 * heads, rows)
    for key in ('q0', 'q1', 'dq', 'x_col'):
        scratch[key] = vmem(batch, rows, width)
    for key, n in (('hbuf', d_model), ('ubuf', ff), ('gbuf', 2 * ff), ('qbuf', 3 * width), ('obuf', width), ('dybuf', d_model)):
        scratch[key] = vmem(2, rows, n)
    for key in ('o', 'out', 'gl', 'h', 'u', 'g', 'q', 'ob', 'dy', 'deal_in'):
        scratch['sem_' + key] = dma((2,))
    scratch.update(sem_qkv=dma((3,)), sem_in=dma((batch + 3,)), sem_keep=dma((batch,)), sem_mask=dma((2, 3)), sem_deal=dma((2, 2, n_tp)), sem_share=dma((2, 2, 3)),
                   sem_wide=dma((2, len(WIDE), 3)), sem_narrow=dma((2, len(NARROW), 3)))
    for key in ('kv', 'qdo', 'stats'):
        scratch['sem_' + key] = dma((2, 2, 3, batch))
    for key in ('o', 'x'):
        scratch['sem_%sz' % key] = dma((2, batch, 3))
        scratch['sem_%sy' % key] = dma((2, batch, 4))
    for i, piece in enumerate(Ring.scratch(batch, seg, d_model)):
        scratch['ring_%d' % i] = piece
    result = pl.pallas_call(
        functools.partial(mega_kernel, list(ins) + list(outs) + list(scratch), heads),
        out_shape=tuple(jax.ShapeDtypeStruct(*v) for v in outs.values()),
        in_specs=[v[1] for v in ins.values()],
        out_specs=tuple([any_spec] * n_any + [VMEM_SPEC] * (len(outs) - n_any)),
        scratch_shapes=list(scratch.values()),
        compiler_params=comm_params(cid, 63),
        cost_estimate=cost(300),
        name='mega',
    )(*[v[0] for v in ins.values()])
    return dict(zip(outs, result))


def swap_kernel(n, *refs):
    halves, wo_part, small, mates, wo_own, wo_mate, total = refs[:n], refs[n], refs[n + 1], refs[n + 2:2 * n + 2], refs[2 * n + 2], refs[2 * n + 3], refs[2 * n + 4]
    wo_in, wo_sum, wo_x, stage, by_z, sem, s_sem, w_sem = refs[2 * n + 5:]
    _, z, y, pair, z_peer = tp_places()
    me, mate, across, _ = cp_places()
    core, chip = lax.rem(me, 2), me // 2
    half = wo_in.shape[-1]
    meet([pair] + z_peer[1:], [mate, across])

    def columns(which):
        return pl.ds(pl.multiple_of(which * half, half), half)

    first = remote(wo_part.at[:, :, columns(1 - core)], wo_in, w_sem, (0,), 'cp', mate)
    first.start()
    swaps = [remote(halves[i], mates[i], sem, (i,), 'cp', mate) for i in range(n)]
    for copy in swaps:
        copy.start()
    first.wait()
    wo_sum[:] = wo_part[:, :, columns(core)] + wo_in[:]
    second = remote(wo_sum.at[1 - chip], wo_x, w_sem, (1,), 'cp', across)
    second.start()
    mine = small
    for k, (axis, peer) in enumerate((('cp', mate), ('cp', across), ('tp', pair))):
        copy = remote(mine, stage.at[2 * k], s_sem, (k,), axis, peer)
        copy.start()
        copy.wait()
        if k < 2:
            stage[2 * k + 1] = mine[:] + stage[2 * k]
            mine = stage.at[2 * k + 1]
        else:
            by_z[z] = mine[:] + stage[2 * k]
    copies = [remote(by_z.at[z], by_z.at[z], s_sem, (2 + j,), 'tp', z_peer[j]) for j in (1, 2, 3)]
    for copy in copies:
        copy.start()
    second.wait()
    wo_own[chip] = (wo_sum[chip] + wo_x[:]).astype(BF16)
    third = remote(wo_own.at[chip], wo_own.at[chip], w_sem, (2,), 'cp', across)
    third.start()
    for copy in copies:
        copy.wait()
    total[:] = by_z[0] + by_z[1] + by_z[2] + by_z[3]
    third.wait()
    last = remote(wo_own, wo_mate, w_sem, (3,), 'cp', mate)
    last.start()
    for copy in swaps + [last]:
        copy.wait()


def swap(halves, wo_part, small, cid):
    n = len(halves)
    layers, width, d_model = wo_part.shape
    half = d_model // 2
    any_spec = pl.BlockSpec(memory_space=pl.ANY)
    dma = pltpu.SemaphoreType.DMA
    wo_shape = jax.ShapeDtypeStruct((layers, width, half), BF16)
    result = pl.pallas_call(
        functools.partial(swap_kernel, n),
        out_shape=tuple(jax.ShapeDtypeStruct(h.shape, h.dtype) for h in halves) + (wo_shape, wo_shape, jax.ShapeDtypeStruct(small.shape, F32)),
        in_specs=[any_spec] * n + [VMEM_SPEC] * 2,
        out_specs=tuple([any_spec] * n + [VMEM_SPEC] * 3),
        scratch_shapes=[pltpu.VMEM((layers, width, half), F32), pltpu.VMEM((layers, width, half), F32), pltpu.VMEM((width, half), F32),
                        pltpu.VMEM((5,) + small.shape, F32), pltpu.VMEM((4,) + small.shape, F32), dma((2, n)), dma((2, 6)), dma((2, 4))],
        compiler_params=comm_params(cid, 24),
        name='swap',
    )(*halves, wo_part, small)
    return list(result[:n]), result[n], result[n + 1], result[n + 2]


def place_kernel(plan, n_out, *refs):
    n = len(plan)
    owns, mates, outs = refs[:n], refs[n:2 * n], refs[2 * n:2 * n + n_out]
    bufs, in_sem, out_sem = refs[2 * n + n_out:4 * n + n_out], refs[4 * n + n_out], refs[4 * n + n_out + 1]
    core = lax.rem(lax.axis_index('cp'), 2)
    loads = [pltpu.make_async_copy(src, buf, in_sem.at[i]) for i, (src, buf) in enumerate(zip(owns + mates, bufs))]
    for load in loads:
        load.start()
    stores = []
    for i, load in enumerate(loads):
        layer, by_rows, first_out, n_pieces = plan[i % n]
        which = core if i < n else 1 - core
        buf = bufs[i]
        load.wait()
        width = buf.shape[1] // n_pieces
        for p in range(n_pieces):
            src = buf if n_pieces == 1 else buf.at[:, pl.ds(p * width, width)]
            size = buf.shape[0] if by_rows else width
            window = pl.ds(pl.multiple_of(which * size, size), size)
            out = outs[first_out + p].at[layer]
            dst = out.at[window, :] if by_rows else out.at[:, window]
            stores.append(pltpu.make_async_copy(src, dst, out_sem.at[len(stores)]))
            stores[-1].start()
    for store in stores:
        store.wait()


def place(plan, owns, mates, out_shapes):
    n = len(plan)
    any_spec = pl.BlockSpec(memory_space=pl.ANY)
    n_stores = 2 * sum(p[3] for p in plan)
    return pl.pallas_call(
        functools.partial(place_kernel, plan, len(out_shapes)),
        out_shape=tuple(jax.ShapeDtypeStruct(s, BF16) for s in out_shapes),
        in_specs=[any_spec] * (2 * n),
        out_specs=tuple([any_spec] * len(out_shapes)),
        scratch_shapes=[pltpu.VMEM(a.shape, BF16) for a in list(owns) + list(mates)] + [pltpu.SemaphoreType.DMA((2 * n,)), pltpu.SemaphoreType.DMA((n_stores,))],
        compiler_params=pltpu.CompilerParams(vmem_limit_bytes=40 * MIB),
        name='place',
    )(*owns, *mates)


def solution(mesh):
    seq_spec = P(None, 'cp', None)
    col_spec = P(None, None, 'tp')
    row_spec = P(None, 'tp', None)
    weight_specs = (P(), P(), col_spec, col_spec, col_spec, row_spec, col_spec, col_spec, row_spec)

    def local_program(x_in, d_y, key_mask, rel_bias, g_attn, g_mlp, w_q, w_k, w_v, w_o, w_gate, w_lin, w_out):
        batch, rows, d_model = x_in.shape
        tokens = batch * rows
        n_layers = w_q.shape[0]
        n_buckets, heads = rel_bias.shape
        tp_index = lax.axis_index('tp')
        core = lax.rem(lax.axis_index('cp'), 2)
        half = d_model // 2

        m = mega(x_in, d_y, key_mask, rel_bias, g_attn, g_mlp, w_q, w_k, w_v, w_o, w_gate, w_lin, w_out, 0)

        def flat(array):
            return array.reshape(-1, array.shape[-1])

        def own_half(array):
            return lax.dynamic_slice_in_dim(array.reshape(tokens, d_model), core * half, half, axis=1)

        def grad(left, right, left_wide):
            a, b = [d_y if key == 'dy' else m['out_' + key] for key in (left, right)]
            a_g, b_g = flat(m['got_' + left]), flat(m['got_' + right])
            a, b = (own_half(a), flat(b)) if left_wide else (flat(a), own_half(b))
            return (dot_tn(a, b) + dot_tn(a_g, b_g)).astype(BF16)

        owns = [grad('h0', 'qkv0', True), grad('h1', 'qkv1', True), grad('m0', 'gl0', True), grad('m1', 'gl1', True), grad('u0', 'd0', False), grad('u1', 'dy', False)]
        wo_part = jnp.stack([dot_tn(flat(m['out_o%d' % l]), m['out_dm%d' % l].reshape(tokens, d_model)) for l in range(n_layers)])
        slots = jnp.zeros((8, n_buckets * heads), F32)
        slots = lax.dynamic_update_slice(slots, jnp.sum(m['bias_sum'], axis=-1).reshape(1, -1), (tp_index, jnp.int32(0)))
        small = jnp.concatenate([part.reshape(-1, 128) for part in (m['dga0'], m['dga1'], m['dgm0'], m['dgm1'], slots)], axis=0)
        mates, wo_own, wo_mate, small = swap(owns, wo_part, small, 1)
        n_gain = n_layers * d_model // 128
        d_g_attn = small[:n_gain].reshape(n_layers, d_model)
        d_g_mlp = small[n_gain:2 * n_gain].reshape(n_layers, d_model)
        d_rel = lax.dynamic_slice(small[2 * n_gain:], (tp_index, jnp.int32(0)), (1, n_buckets * heads)).reshape(n_buckets, heads)
        plan = tuple((layer, by_rows, first, n) for by_rows, first, n in ((True, 0, 3), (True, 4, 2), (False, 6, 1), (False, 3, 1)) for layer in range(n_layers))
        wo_halves = [[w[l] for l in range(n_layers)] for w in (wo_own, wo_mate)]
        grads = place(plan, owns + wo_halves[0], mates + wo_halves[1], [w.shape for w in (w_q, w_k, w_v, w_o, w_gate, w_lin, w_out)])
        return (m['out_dx'].reshape(batch, rows, d_model), d_rel, d_g_attn, d_g_mlp) + tuple(grads)

    return jax.shard_map(local_program, mesh=mesh, in_specs=(seq_spec, seq_spec, P(None, 'cp'), P(None, 'tp')) + weight_specs, out_specs=(seq_spec, P(None, 'tp')) + weight_specs, check_vma=False)
```

```python
import functools
import itertools
import string

import jax
import jax.numpy as jnp
from jax import lax
from jax.experimental import pallas as pl
from jax.experimental.pallas import tpu as pltpu
from jax.sharding import PartitionSpec as P

NORM_EPS = 1e-6
MASK_NEG = -1e9
BF16 = jnp.bfloat16
F32 = jnp.float32
VMEM = pltpu.VMEM
MESH = pl.DeviceIdType.MESH
MIB = 2 ** 20
HEAD_DIM = 64
VMEM_SPEC = pl.BlockSpec(memory_space=pltpu.VMEM)
SMEM_SPEC = pl.BlockSpec(memory_space=pltpu.SMEM)


def rel_bucket(rel_pos):
    distance = jnp.minimum(jnp.abs(rel_pos), 128)
    distance_sq = distance * distance
    log_part = 8 + sum((distance_sq >= 64 * 2 ** power).astype(jnp.int32) for power in range(1, 8))
    return jnp.where(distance < 8, distance, log_part) + 16 * (rel_pos > 0).astype(jnp.int32)


def comm_params(cid, mib):
    return pltpu.CompilerParams(collective_id=cid, has_side_effects=True, vmem_limit_bytes=mib * MIB)


def cost(gflops):
    return pl.CostEstimate(flops=gflops * 1000 * MIB, bytes_accessed=8 * MIB, transcendentals=MIB)


def dot_nt(a, b):
    return lax.dot_general(a, b, (((1,), (1,)), ((), ())), preferred_element_type=F32)


def dot_nn(a, b):
    return lax.dot_general(a, b, (((1,), (0,)), ((), ())), preferred_element_type=F32)


def dot_tn(a, b):
    return lax.dot_general(a, b, (((0,), (0,)), ((), ())), preferred_element_type=F32)


def stack_heads(block, heads):
    wide = block.astype(F32)
    lane_head = lax.broadcasted_iota(jnp.int32, block.shape, 1) // HEAD_DIM
    return jnp.concatenate([jnp.where(lane_head == h, wide, 0.0).astype(BF16) for h in range(heads)], axis=0)


def pick_heads(stacked, heads, rows):
    lane_head = lax.broadcasted_iota(jnp.int32, (rows, stacked.shape[1]), 1) // HEAD_DIM
    out = stacked[:rows]
    for h in range(1, heads):
        out = jnp.where(lane_head == h, stacked[h * rows:(h + 1) * rows], out)
    return out


def cp_places():
    me = lax.axis_index('cp')
    mate = me + 1 - 2 * lax.rem(me, 2)
    across = lax.rem(me + 2, 4)
    diagonal = lax.rem(mate + 2, 4)
    return me, mate, across, diagonal


def rms_parts(x_f, gain):
    inv_rms = lax.rsqrt(jnp.mean(x_f * x_f, axis=-1, keepdims=True) + NORM_EPS)
    return (x_f * inv_rms * gain).astype(BF16)


GELU_C = 0.7978845608028654
GELU_A = 0.044715


def gelu_parts(x):
    t = jnp.tanh(GELU_C * (x + GELU_A * x * x * x))
    cdf = 0.5 * (1.0 + t)
    return x * cdf, cdf + 0.5 * x * (1.0 - t * t) * GELU_C * (1.0 + 3.0 * GELU_A * x * x)


Z_STEPS = (2, 1, 3)


def remote(src, dst, sem, at, axis, peer):
    return pltpu.make_async_remote_copy(src_ref=src, dst_ref=dst, send_sem=sem.at[(0,) + at], recv_sem=sem.at[(1,) + at], device_id={axis: peer}, device_id_type=MESH)


def tp_places():
    me = lax.axis_index('tp')
    z, y = me // 2, lax.rem(me, 2)
    pair = me + 1 - 2 * y
    return me, z, y, pair, [2 * lax.rem(z + j, 4) + y for j in range(4)]


def meet(tp_peers, cp_peers):
    barrier = pltpu.get_barrier_semaphore()
    for axis, peers in (('tp', tp_peers), ('cp', cp_peers)):
        for peer in peers:
            pl.semaphore_signal(barrier, inc=1, device_id={axis: peer}, device_id_type=MESH)
    pl.semaphore_wait(barrier, len(tp_peers) + len(cp_peers))


class Ring:
    def __init__(self, part, from_y, from_z, full, *sems):
        self.part, self.from_y, self.from_z, self.full = part, from_y, from_z, full
        self.sem_ys, self.sem_zs, self.sem_zg, self.sem_yg = sems
        _, self.z, self.y, self.pair, self.z_peer = tp_places()
        self.seg = self.y * 4 + self.z

    @staticmethod
    def scratch(batch, seg, d_model):
        dma = pltpu.SemaphoreType.DMA
        return [
            pltpu.VMEM((batch, 2, 4, seg, d_model), F32),
            pltpu.VMEM((batch, 4, seg, d_model), F32),
            pltpu.VMEM((batch, 3, seg, d_model), F32),
            pltpu.VMEM((batch, 8, seg, d_model), BF16),
            dma((2, batch)), dma((2, batch, 3)), dma((2, batch, 3)), dma((2, batch, 4)),
        ]

    def y_sum(self, b):
        return remote(self.part.at[b, 1 - self.y], self.from_y.at[b], self.sem_ys, (b,), 'tp', self.pair)

    def z_sum(self, b, j):
        return remote(self.part.at[b, self.y, lax.rem(self.z + j, 4)], self.from_z.at[b, j - 1], self.sem_zs, (b, j - 1), 'tp', self.z_peer[j])

    def z_gather(self, b, j):
        ref = self.full.at[b, self.seg]
        return remote(ref, ref, self.sem_zg, (b, j - 1), 'tp', self.z_peer[j])

    def y_gather(self, b, j):
        ref = self.full.at[b, self.y * 4 + lax.rem(self.z - j + 4, 4)]
        return remote(ref, ref, self.sem_yg, (b, j), 'tp', self.pair)

    def send_partial(self, b, partial):
        self.part[b] = partial.reshape(self.part.shape[1:])
        self.y_sum(b).start()

    def reduce_pair(self, b):
        self.y_sum(b).wait_recv()
        self.part[b, self.y] = self.part[b, self.y] + self.from_y[b]
        for j in Z_STEPS:
            self.z_sum(b, j).start()

    def reduced(self, b):
        for j in Z_STEPS:
            self.z_sum(b, j).wait_recv()
        return self.part[b, self.y, self.z] + self.from_z[b, 0] + self.from_z[b, 1] + self.from_z[b, 2]

    def publish(self, b, out):
        self.full[b, self.seg] = out
        for j in Z_STEPS:
            self.z_gather(b, j).start()
        self.y_gather(b, 0).start()

    def forward(self, b):
        for j in Z_STEPS:
            self.z_gather(b, j).wait_recv()
            self.y_gather(b, j).start()

    def arrive(self, b):
        for j in range(4):
            self.y_gather(b, j).wait_recv()
        self.y_sum(b).wait_send()
        for j in range(4):
            self.y_gather(b, j).wait_send()
        for j in Z_STEPS:
            self.z_sum(b, j).wait_send()
            self.z_gather(b, j).wait_send()

    def rows(self, b):
        return self.full[b].reshape(-1, self.full.shape[-1])


class Columns:
    def __init__(self, store, z_sem, y_sem):
        self.store, self.z_sem, self.y_sem = store, z_sem, y_sem
        self.me, self.z, self.y, self.pair, self.z_peer = tp_places()

    def z_gather(self, b, j):
        ref = self.store.at[b, self.me]
        return remote(ref, ref, self.z_sem, (b, j - 1), 'tp', self.z_peer[j])

    def y_gather(self, b, j):
        ref = self.store.at[b, 2 * lax.rem(self.z - j + 4, 4) + self.y]
        return remote(ref, ref, self.y_sem, (b, j), 'tp', self.pair)

    def publish(self, b, out):
        self.store[b, self.me] = out
        for j in Z_STEPS:
            self.z_gather(b, j).start()
        self.y_gather(b, 0).start()

    def forward(self, b):
        for j in Z_STEPS:
            self.z_gather(b, j).wait_recv()
            self.y_gather(b, j).start()

    def arrive(self, b):
        for j in range(4):
            self.y_gather(b, j).wait_recv()
        for j in range(4):
            self.y_gather(b, j).wait_send()
        for j in Z_STEPS:
            self.z_gather(b, j).wait_send()

    def rows(self, b):
        return jnp.concatenate([self.store[b, t] for t in range(self.store.shape[1])], axis=1)


class Trade:
    def __init__(self, store, sem, layer):
        self.store, self.sem, self.layer = store, sem, layer
        self.me, self.mate, self.across, self.diagonal = cp_places()

    def copy(self, b, r):
        ref = self.store.at[b, self.across if r == 2 else self.me]
        return remote(ref, ref, self.sem, (self.layer, r, b), 'cp', self.across if r == 1 else self.mate)

    def give(self, b):
        self.copy(b, 1).start()
        self.copy(b, 0).start()

    def pass_on(self, b):
        self.copy(b, 1).wait_recv()
        self.copy(b, 2).start()

    def take(self, b):
        self.copy(b, 0).wait_recv()
        self.copy(b, 2).wait_recv()

    def finish(self, b):
        for r in range(3):
            self.copy(b, r).wait_send()


class Wide:
    def __init__(self, src, dst, sem, index):
        self.src, self.dst, self.sem, self.index = src, dst, sem, index
        me, *self.peers = cp_places()
        mate, across, diagonal = self.peers
        self.peers = (mate, across, diagonal)
        self.core = lax.rem(me, 2)

    def copy(self, r, window):
        n = self.dst.shape[-1]
        want = self.core if r == 1 else 1 - self.core
        columns = pl.ds(pl.multiple_of(want * n, n), n)
        return remote(self.src.at[window].at[..., columns], self.dst.at[r].at[window], self.sem, (self.index, r), 'cp', self.peers[r])

    def give(self, b):
        for r in (1, 2, 0):
            self.copy(r, pl.ds(b, 1)).start()

    def pass_on(self):
        pass

    def finish(self):
        for r in range(3):
            self.copy(r, pl.ds(0, self.src.shape[0])).wait()


class Narrow:
    def __init__(self, src, dst, sem, index):
        self.src, self.dst, self.sem, self.index = src, dst, sem, index
        _, self.mate, self.across, _ = cp_places()

    def copy(self, r, window):
        src = self.src if r < 2 else self.dst.at[1]
        return remote(src.at[window], self.dst.at[r].at[window], self.sem, (self.index, r), 'cp', self.across if r == 1 else self.mate)

    def give(self, b):
        for r in (1, 0):
            self.copy(r, pl.ds(b, 1)).start()

    def pass_on(self):
        every = pl.ds(0, self.src.shape[0])
        self.copy(1, every).wait_recv()
        self.copy(2, every).start()

    def finish(self):
        every = pl.ds(0, self.src.shape[0])
        self.copy(0, every).wait()
        self.copy(1, every).wait_send()
        self.copy(2, every).wait()


class Spill:
    def __init__(self, slots, sem):
        self.slots, self.sem = slots, sem

    def copy(self, out, b):
        slot = lax.rem(b, 2)
        return pltpu.make_async_copy(self.slots.at[slot], out.at[b], self.sem.at[slot])

    def put(self, out, b, value):
        self.slots[lax.rem(b, 2)] = value
        self.copy(out, b).start()


def norm_rows(rows, gain):
    return rms_parts(rows.astype(F32), gain)


def rms_pull(total, x_shard, gain, res, d_gain_ref):
    d_norm = total.astype(BF16).astype(F32)
    x_f = x_shard.astype(F32)
    inv_rms = lax.rsqrt(jnp.mean(x_f * x_f, axis=-1, keepdims=True) + NORM_EPS)
    normed = x_f * inv_rms
    d_gain_ref[:] += jnp.sum(d_norm * normed, axis=0, keepdims=True)
    d_normed = d_norm * gain
    d_x = inv_rms * (d_normed - normed * jnp.mean(d_normed * normed, axis=-1, keepdims=True))
    return (res.astype(F32) + d_x).astype(BF16)


def mlp_pull(d_u, gate, lin):
    d_u = d_u.astype(BF16).astype(F32)
    value, slope = gelu_parts(gate)
    return jnp.concatenate([(d_u * lin * slope).astype(BF16), (d_u * value).astype(BF16)], axis=1)


def row_sum(x):
    return jnp.sum(x, axis=1, keepdims=True)


def row_max(x):
    return jnp.max(x, axis=1, keepdims=True)


def mask_row(mask_ref, b):
    return jnp.concatenate([mask_ref[c, b] for c in range(mask_ref.shape[0])], axis=1)


def attend(heads, q, kv, bias, mask):
    rows, width = q.shape
    scores = dot_nt(stack_heads(q, heads), kv[:, :width]) + bias + mask
    top = row_max(scores)
    probs = jnp.exp(scores - top)
    total = row_sum(probs)
    out = dot_nn(probs.astype(BF16), kv[:, width:]) / total
    return pick_heads(out, heads, rows).astype(BF16)


def attend_rows_back(heads, qdo, kv, bias, mask, ds_ref):
    rows, wide = qdo.shape
    width = wide // 2
    keys, vals = kv[:, :width], kv[:, width:]
    scores = dot_nt(stack_heads(qdo[:, :width], heads), keys) + bias + mask
    top = row_max(scores)
    unnorm = jnp.exp(scores - top)
    total = row_sum(unnorm)
    log_norm = top + jnp.log(total)
    probs = unnorm * (1.0 / total)
    d_probs = dot_nt(stack_heads(qdo[:, width:], heads), vals)
    row_dot = row_sum(probs * d_probs)
    lane = lax.broadcasted_iota(jnp.int32, (rows, rows), 1)
    table = jnp.zeros((rows, rows), F32)
    for h in range(heads):
        table = jnp.where(lane == h, log_norm[h * rows:(h + 1) * rows], table)
        table = jnp.where(lane == heads + h, row_dot[h * rows:(h + 1) * rows], table)
    d_scores = probs * (d_probs - row_dot)
    ds_ref[:] += d_scores
    d_q = dot_nn(d_scores.astype(BF16), keys)
    return pick_heads(d_q, heads, rows).astype(BF16), jnp.transpose(table)[:2 * heads]


def attend_cols_back(heads, own_kv, mask_col, bias_ref, qdo_of, stats_of):
    rows, wide = own_kv.shape
    width = wide // 2
    keys, vals = own_kv[:, :width], own_kv[:, width:]

    def block(src, acc):
        d_k, d_v = acc
        qdo, stats = qdo_of(src), stats_of(src)
        log_norm = jnp.concatenate([stats[h:h + 1] for h in range(heads)], axis=1)
        row_dot = jnp.concatenate([stats[heads + h:heads + h + 1] for h in range(heads)], axis=1)
        q_st = stack_heads(qdo[:, :width], heads)
        do_st = stack_heads(qdo[:, width:], heads)
        probs = jnp.exp(dot_nt(keys, q_st) + bias_ref[src] + mask_col - log_norm)
        d_scores = probs * (dot_nt(vals, do_st) - row_dot)
        return d_k + dot_nn(d_scores.astype(BF16), q_st), d_v + dot_nn(probs.astype(BF16), do_st)

    zero = jnp.zeros((rows, width), F32)
    d_k, d_v = lax.fori_loop(0, bias_ref.shape[0], block, (zero, zero))
    return jnp.concatenate([d_k, d_v], axis=1).astype(BF16)


def bias_tables(table_ref, me, rows_ref, cols_ref):
    n_buckets, heads = table_ref.shape
    rows = rows_ref.shape[0] // heads
    seq = rows_ref.shape[1]

    def strip(i, carry):
        first = pl.multiple_of(i * 8, 8)
        rel = lax.broadcasted_iota(jnp.int32, (8, seq), 1) - lax.broadcasted_iota(jnp.int32, (8, seq), 0) - me * rows - first
        for is_col in (False, True):
            buckets = rel_bucket(-rel if is_col else rel)
            vals = [jnp.zeros((8, seq), F32) for _ in range(heads)]
            for k in range(n_buckets):
                hit = buckets == k
                vals = [jnp.where(hit, table_ref[k, h], v) for h, v in enumerate(vals)]
            for h, v in enumerate(vals):
                if is_col:
                    for q in range(seq // rows):
                        cols_ref[q, pl.ds(first, 8), h * rows:(h + 1) * rows] = v[:, q * rows:(q + 1) * rows]
                else:
                    rows_ref[pl.ds(pl.multiple_of(h * rows + first, 8), 8), :] = v
        return carry

    lax.fori_loop(0, rows // 8, strip, 0)


def bucket_sums(ds_ref, heads, n_buckets, me):
    rows, seq = ds_ref.shape[0] // heads, ds_ref.shape[1]
    rel = lax.broadcasted_iota(jnp.int32, (rows, seq), 1) - lax.broadcasted_iota(jnp.int32, (rows, seq), 0) - me * rows
    lane = lax.broadcasted_iota(jnp.int32, (1, n_buckets * heads), 1)

    def step(k, acc):
        hit = rel_bucket(rel) == k
        for h in range(heads):
            total = jnp.sum(row_sum(jnp.where(hit, ds_ref[h * rows:(h + 1) * rows], 0.0)), axis=0, keepdims=True)
            acc = jnp.where(lane == k * heads + h, total, acc)
        return acc

    return lax.fori_loop(0, n_buckets, step, jnp.zeros(lane.shape, F32))


class Refs:
    pass


WIDE = ('h0', 'h1', 'm0', 'm1', 'dy', 'd0')
NARROW = ('u0', 'u1', 'gl0', 'gl1', 'qkv0', 'qkv1')
LETTERS = string.ascii_letters
STEPS = '0303221222210111101101010101101101123'
ORDER = 'FaKGeCtbdqpHlkExvozmjiwshfuBJnDIcAgyr'
PASS_FROM = 34
GIVES = tuple(zip(('h0', 'dy', 'u0', 'm0', 'h1', 'u1', 'm1', 'gl1', 'd0', 'qkv1', 'gl0', 'qkv0'), map(LETTERS.index, 'ddmvxzABDHHJ')))


def mega_kernel(names, heads, *refs):
    r = Refs()
    for key, ref in zip(names, refs):
        setattr(r, key, ref)
    batch, n_seg, seg, d_model = r.x.shape
    rows = n_seg * seg
    ff = r.w_out.shape[1]
    width = heads * HEAD_DIM
    ring = Ring(*[getattr(r, 'ring_%d' % i) for i in range(8)])
    gather_o = Columns(r.o_all, r.sem_oz, r.sem_oy)
    gather_x = Columns(r.x_all, r.sem_xz, r.sem_xy)
    me, mate, across, diagonal = cp_places()
    tp_me = gather_o.me
    others = (mate, across, diagonal)
    my_columns = pl.ds(pl.multiple_of(tp_me * width, width), width)

    def weight(buf, sem, sources, layer):
        out, col = [], 0
        for i, src in enumerate(sources):
            n = src.shape[-1]
            out.append(pltpu.make_async_copy(src.at[layer], buf.at[:, pl.ds(col, n)] if len(sources) > 1 else buf, sem.at[i]))
            col += n
        return out

    weights = dict(qkv=(r.wqkv, r.sem_qkv, (r.w_q, r.w_k, r.w_v)), o=(r.wo, r.sem_o, (r.w_o,)), gl=(r.wgl, r.sem_gl, (r.w_gate, r.w_lin)), out=(r.wout, r.sem_out, (r.w_out,)))

    def load(key, layer):
        def go():
            for copy in weight(*weights[key], layer):
                copy.start()
        return go

    def loaded(key, layer):
        def go():
            for copy in weight(*weights[key], layer):
                copy.wait()
        return go

    chip, core = me // 2, lax.rem(me, 2)
    half = d_model // 2

    def half_of(which):
        return pl.ds(pl.multiple_of(which * half, half), half)

    def wo_send(l, step):
        src, dst, peer = (
            (r.wo_acc.at[:, half_of(1 - core)], r.wo_in.at[l], mate),
            (r.wo_in.at[l, pl.ds(pl.multiple_of((1 - chip) * (width // 2), 8), width // 2)], r.wo_x.at[l], across),
            (r.wo_half.at[l, chip], r.wo_half.at[l, chip], across))[step]
        return remote(src, dst, r.sem_wo, (l, step), 'cp', peer)

    def wo_first(l):
        return lambda: wo_send(l, 0).start()

    def wo_second(l):
        def go():
            wo_send(l, 0).wait()
            r.wo_in[l] = r.wo_in[l] + r.wo_acc[:, half_of(core)]
            wo_send(l, 1).start()
        return go

    def wo_third(l):
        def go():
            wo_send(l, 1).wait()
            mine = r.wo_in[l, pl.ds(pl.multiple_of(chip * (width // 2), 8), width // 2)]
            r.wo_half[l, chip] = (mine + r.wo_x[l]).astype(BF16)
            wo_send(l, 2).start()
        return go

    for key, layer in (('qkv', 0), ('o', 1), ('gl', 0), ('out', 0)):
        load(key, layer)()
    rows_in = [pltpu.make_async_copy(r.x.at[b], ring.full.at[b], r.sem_in.at[b]) for b in range(batch)]
    shards_in = [(r.x.at[:, ring.seg], r.xs0), (r.dy.at[:, ring.seg], r.ds1), (r.x_rows.at[:, :, my_columns], r.x_col)]
    shards_in = [pltpu.make_async_copy(src, dst, r.sem_in.at[batch + i]) for i, (src, dst) in enumerate(shards_in)]
    deal_own = [pltpu.make_async_copy(r.w_deal.at[l, me, :, my_columns], r.w_cols.at[l, me, tp_me], r.sem_deal_in.at[l]) for l in range(2)]
    for copy in rows_in + shards_in + deal_own:
        copy.start()
    r.key_add[:] = jnp.where(r.key_mask[:] > 0, 0.0, MASK_NEG).astype(F32)[:, None, :]
    peers = [lax.rem(tp_me + j, n_seg) for j in range(n_seg)]
    meet(peers[1:], others)
    masks = [remote(r.key_add, r.mask_all.at[me], r.sem_mask, (i,), 'cp', peer) for i, peer in enumerate(others)]
    for copy in masks:
        copy.start()
    r.mask_all[me] = r.key_add[:]

    def deal(l, j):
        window = pl.ds(pl.multiple_of(peers[j] * width, width), width)
        return remote(r.w_deal.at[l, me, :, window], r.w_cols.at[l, me, tp_me], r.sem_deal, (l, j), 'tp', peers[j])

    def share(l, i):
        ref = r.w_cols.at[l, across if i == 2 else me]
        return remote(ref, ref, r.sem_share, (l, i), 'cp', across if i == 1 else mate)

    for l in range(2):
        for j in range(1, n_seg):
            deal(l, j).start()

    def share_start(l):
        def go():
            for j in range(1, n_seg):
                deal(l, j).wait()
            deal_own[l].wait()
            share(l, 1).start()
            share(l, 0).start()
        return go

    def share_pass(l):
        def go():
            share(l, 1).wait_recv()
            share(l, 2).start()
        return go

    def shared(l):
        def go():
            share(l, 0).wait()
            share(l, 1).wait_send()
            share(l, 2).wait()
            for c in range(r.w_cols.shape[1]):
                for t in range(n_seg):
                    r.w_now[t, c] = r.w_cols[l, c, t]
        return go

    for ref in (r.ds_sum, r.dga0, r.dga1, r.dgm0, r.dgm1):
        ref[:] = jnp.zeros_like(ref)
    bias_tables(r.rel_bias, me, r.bias_rows, r.bias_cols)
    for copy in rows_in + shards_in:
        copy.wait()
    loaded('qkv', 0)()

    hold = dict(h=Spill(r.hbuf, r.sem_h), u=Spill(r.ubuf, r.sem_u), gl=Spill(r.gbuf, r.sem_g), qkv=Spill(r.qbuf, r.sem_q))
    moves = {}
    for i, key in enumerate(WIDE):
        moves[key] = Wide(r.dy_rows if key == 'dy' else getattr(r, 'out_' + key), getattr(r, 'got_' + key), r.sem_wide, i)
    for i, key in enumerate(NARROW):
        moves[key] = Narrow(getattr(r, 'out_' + key), getattr(r, 'got_' + key), r.sem_narrow, i)
    kv = [Trade(store, r.sem_kv, l) for l, store in enumerate((r.kv0, r.kv1))]
    qdo = [Trade(store, r.sem_qdo, l) for l, store in enumerate((r.qdo0, r.qdo1))]
    q_own = (r.q0, r.q1)
    stats = (r.stats0, r.stats1)

    def send_stats(l, b, i):
        ref = stats[l].at[b, me]
        return remote(ref, ref, r.sem_stats, (l, i, b), 'cp', others[i])

    def out(key, l):
        return getattr(r, 'out_%s%d' % (key, l))

    def project(l, b, flat):
        h = norm_rows(flat, r.g_attn[l:l + 1])
        hold['h'].put(out('h', l), b, h)
        qkv = dot_nn(h, r.wqkv[:]).astype(BF16)
        q_own[l][b] = qkv[:, :width]
        kv[l].store[b, me] = qkv[:, width:]
        kv[l].give(b)

    def stage_first(b):
        project(0, b, ring.rows(b))

    def stage_attend(l):
        def go(b):
            kv[l].take(b)
            pairs = kv[l].store[b].reshape(-1, 2 * width)
            o = attend(heads, q_own[l][b], pairs, r.bias_rows[:], mask_row(r.mask_all, b))
            gather_o.publish(b, o)
            r.o_own[l, b] = o
        return go

    def stage_columns(l):
        def go(b):
            gather_o.arrive(b)
            prod = dot_nn(gather_o.rows(b), r.w_now[:].reshape(d_model, width))
            gather_x.publish(b, (r.x_col[b].astype(F32) + prod).astype(BF16))
        return go

    def add_stage(res, dst):
        def go(b):
            total = ring.reduced(b)
            value = (res[b].astype(F32) + total).astype(BF16)
            dst[b] = value
            ring.publish(b, value)
        return go

    def pull_stage(x_shard, gain, l, res, dst, d_gain):
        def go(b):
            value = rms_pull(ring.reduced(b), x_shard[b], gain[l:l + 1], res[b], d_gain)
            if dst is not None:
                dst[b] = value
            ring.publish(b, value)
        return go

    def mlp_forward(l, b, shard):
        gather_x.arrive(b)
        window = pl.ds(pl.multiple_of(ring.seg * seg, seg), seg)
        shard[b] = jnp.concatenate([r.x_all[b, t, window] for t in range(n_seg)], axis=1)
        h2 = norm_rows(gather_x.rows(b), r.g_mlp[l:l + 1])
        hold['h'].put(out('m', l), b, h2)
        both = dot_nn(h2, r.wgl[:])
        gate, lin = both[:, :ff], both[:, ff:]
        u = (gelu_parts(gate)[0] * lin).astype(BF16)
        hold['u'].put(out('u', l), b, u)
        return gate, lin, u

    def stage_mlp0(b):
        gate, lin, u = mlp_forward(0, b, r.x1s0)
        r.gate[b] = gate
        r.lin[b] = lin
        ring.send_partial(b, dot_nn(u, r.wout[:]))

    def stage_next(b):
        ring.arrive(b)
        r.x_col[b] = ring.full[b, :, :, my_columns].reshape(rows, width)
        project(1, b, ring.rows(b))

    def dy_in(b):
        slot = lax.rem(b, 2)
        return pltpu.make_async_copy(r.dy_rows.at[b], r.dybuf.at[slot], r.sem_dy.at[slot])

    def mlp_backward(l, b, d, gate, lin, copy=None):
        dgl = mlp_pull(dot_nt(d, r.wout[:]), gate, lin)
        hold['gl'].put(out('gl', l), b, dgl)
        if copy is not None:
            copy.wait()
        ring.send_partial(b, dot_nt(dgl, r.wgl[:]))

    def stage_mlp1(b):
        gate, lin, _ = mlp_forward(1, b, r.x1s1)
        dy_in(b).wait()
        mlp_backward(1, b, r.dybuf[lax.rem(b, 2)], gate, lin)

    def keep(dst, b):
        copy = pltpu.make_async_copy(ring.full.at[b], dst.at[b], r.sem_keep.at[b])
        copy.start()
        return copy

    def stage_rows_back(l):
        def go(b):
            ring.arrive(b)
            d_mid = ring.rows(b)
            d_o = dot_nt(d_mid, r.wo[:]).astype(BF16)
            both = jnp.concatenate([q_own[l][b], d_o], axis=1)
            qdo[l].store[b, me] = both
            qdo[l].give(b)
            pairs = kv[l].store[b].reshape(-1, 2 * width)
            d_q, table = attend_rows_back(heads, both, pairs, r.bias_rows[:], mask_row(r.mask_all, b), r.ds_sum)
            stats[l][b, me] = table
            r.dq[b] = d_q
            for i in range(3):
                send_stats(l, b, i).start()
            d_wo = dot_tn(r.o_own[l, b], d_mid)

            @pl.when(b == 0)
            def _():
                r.wo_acc[:] = d_wo

            @pl.when(b > 0)
            def _():
                r.wo_acc[:] += d_wo
        return go

    def stage_cols_back(l):
        def go(b):
            qdo[l].take(b)
            for i in range(3):
                send_stats(l, b, i).wait_recv()
            mask_col = jnp.transpose(jnp.broadcast_to(r.key_add[b], (rows, rows)))[:, :1]
            d_kv = attend_cols_back(heads, kv[l].store[b, me], mask_col, r.bias_cols, lambda s: qdo[l].store[b, s], lambda s: stats[l][b, s])
            d_qkv = jnp.concatenate([r.dq[b], d_kv], axis=1)
            hold['qkv'].put(out('qkv', l), b, d_qkv)
            ring.send_partial(b, dot_nt(d_qkv, r.wqkv[:]))
        return go

    def stage_mlp_back0(b):
        ring.arrive(b)
        copy = keep(r.out_d0, b)
        mlp_backward(0, b, ring.rows(b), r.gate[b], r.lin[b], copy)

    def stage_last(b):
        ring.arrive(b)
        keep(r.out_dx, b).wait()

    def by_columns(tag, l):
        return [('at' + tag, stage_attend(l)), ('', gather_o.forward), ('col' + tag, stage_columns(l)), ('', gather_x.forward)]

    def by_sum(tag, start, finish):
        return [(tag, start), ('', ring.reduce_pair), ('', finish), ('', ring.forward)]

    stages = (
        [('first', stage_first), ('', kv[0].pass_on)] + by_columns('0', 0)
        + by_sum('mlp0', stage_mlp0, add_stage(r.x1s0, r.xs1))
        + [('next', stage_next), ('', kv[1].pass_on)] + by_columns('1', 1)
        + by_sum('mlp1', stage_mlp1, pull_stage(r.x1s1, r.g_mlp, 1, r.ds1, r.dms1, r.dgm1))
        + [('rows1', stage_rows_back(1)), ('', qdo[1].pass_on)]
        + by_sum('cols1', stage_cols_back(1), pull_stage(r.xs1, r.g_attn, 1, r.dms1, r.ds0, r.dga1))
        + by_sum('back0', stage_mlp_back0, pull_stage(r.x1s0, r.g_mlp, 0, r.ds0, r.dms0, r.dgm0))
        + [('rows0', stage_rows_back(0)), ('', qdo[0].pass_on)]
        + by_sum('cols0', stage_cols_back(0), pull_stage(r.xs0, r.g_attn, 0, r.dms0, None, r.dga0))
        + [('last', stage_last)])
    lags = list(itertools.accumulate(int(step) for step in STEPS))
    order = [LETTERS.index(letter) for letter in ORDER]
    lag_of = {tag: lag for (tag, _), lag in zip(stages, lags)}
    use = lambda tag: lag_of[tag]
    after = lambda tag: lag_of[tag] + batch

    def masked():
        for copy in masks:
            copy.wait()

    def count_buckets():
        r.small[-n_seg:] = jnp.where(lax.broadcasted_iota(jnp.int32, (n_seg, 128), 0) == tp_me, bucket_sums(r.ds_sum, heads, r.rel_bias.shape[0], me), 0.0)

    once = [
        (use('at0'), masked), (use('mlp0'), loaded('gl', 0)), (use('mlp0'), loaded('out', 0)),
        (batch, share_start(0)), (batch + 1, share_pass(0)), (use('col0'), shared(0)), (batch, share_start(1)), (after('col0'), share_pass(1)), (use('col1'), shared(1)),
        (after('first'), load('qkv', 1)), (use('next'), loaded('qkv', 1)),
        (after('mlp0'), load('gl', 1)), (after('mlp0'), load('out', 1)), (use('mlp1'), loaded('gl', 1)), (use('mlp1'), loaded('out', 1)),
        (after('mlp1'), load('gl', 0)), (after('mlp1'), load('out', 0)), (use('back0'), loaded('gl', 0)), (use('back0'), loaded('out', 0)),
        (use('rows1'), loaded('o', 1)), (after('rows1'), load('o', 0)), (use('rows0'), loaded('o', 0)),
        (after('cols1'), load('qkv', 0)), (use('cols0'), loaded('qkv', 0)),
        (after('rows1'), wo_first(1)), (after('rows1') + 1, wo_second(1)), (after('rows1') + 4, wo_third(1)),
        (after('rows0'), wo_first(0)), (after('rows0') + 1, wo_second(0)),
    ]
    early = [(use(tag) + 1, hold[key], ref) for tag, key, ref in (
        ('first', 'h', r.out_h0), ('mlp0', 'h', r.out_m0), ('mlp0', 'u', r.out_u0), ('next', 'h', r.out_h1),
        ('mlp1', 'h', r.out_m1), ('mlp1', 'u', r.out_u1), ('mlp1', 'gl', r.out_gl1), ('cols1', 'qkv', r.out_qkv1), ('back0', 'gl', r.out_gl0), ('cols0', 'qkv', r.out_qkv0))]
    gives = dict(GIVES)
    passes = [(max(gives[key] + 2 * batch, PASS_FROM), moves[key].pass_on) for key in NARROW]
    n_slots = batch + lags[-1]

    def chunk_at(slot, lag, work):
        @pl.when(jnp.logical_and(slot >= lag, slot < batch + lag))
        def _():
            work(slot - lag)

    def slot_step(slot, carry):
        for at, work in once + passes:
            if at < n_slots:
                pl.when(slot == at)(work)
        for lag, spill, ref in early:
            chunk_at(slot, lag, lambda b: spill.copy(ref, b).wait())
        chunk_at(slot, use('mlp1') - 1, lambda b: dy_in(b).start())
        for k in order:
            chunk_at(slot, lags[k], stages[k][1])
        for key, lag in GIVES:
            chunk_at(slot, lag, moves[key].give)
        pl.when(slot == n_slots - batch)(count_buckets)
        return carry

    lax.fori_loop(0, n_slots, slot_step, 0)
    wo_third(0)()
    for at, work in passes:
        if at >= n_slots:
            work()
    n_lines = d_model // 128
    for i, ref in enumerate((r.dga0, r.dga1, r.dgm0, r.dgm1)):
        for k in range(n_lines):
            r.small[i * n_lines + k:i * n_lines + k + 1] = ref[:, k * 128:(k + 1) * 128]

    def finish(b, carry):
        for l in range(2):
            kv[l].finish(b)
            qdo[l].finish(b)
            for i in range(3):
                send_stats(l, b, i).wait_send()
        return carry

    lax.fori_loop(0, batch, finish, 0)
    for key in WIDE + NARROW:
        moves[key].finish()
    for l, _ in enumerate(kv):
        wo_send(l, 2).wait()


def mega(x, dy, key_mask, rel_bias, g_attn, g_mlp, w_q, w_k, w_v, w_o, w_gate, w_lin, w_out, cid):
    batch, rows, d_model = x.shape
    heads = rel_bias.shape[1]
    width, ff = heads * HEAD_DIM, w_gate.shape[2]
    n_cp, n_tp = 4, 8
    seg = rows // n_tp
    quarter = width // n_cp
    dma = pltpu.SemaphoreType.DMA
    any_spec = pl.BlockSpec(memory_space=pl.ANY)
    by_seg = lambda a: a.reshape(batch, n_tp, seg, d_model)
    in_hbm = dict(x=by_seg(x), x_rows=x, dy=by_seg(dy), dy_rows=dy, w_q=w_q, w_k=w_k, w_v=w_v, w_o=w_o, w_deal=w_o.reshape(-1, n_cp, quarter, d_model), w_gate=w_gate, w_lin=w_lin, w_out=w_out)
    ins = {key: (value, any_spec) for key, value in in_hbm.items()}
    ins.update(key_mask=(key_mask, VMEM_SPEC), rel_bias=(rel_bias, SMEM_SPEC), g_attn=(g_attn, VMEM_SPEC), g_mlp=(g_mlp, VMEM_SPEC))
    size = dict(h=d_model, m=d_model, u=ff, gl=2 * ff, qkv=3 * width)
    outs = {}
    for key, n in size.items():
        for l in range(2):
            outs['out_%s%d' % (key, l)] = ((batch, rows, n), BF16)
    for key in ('d0', 'dx'):
        outs['out_' + key] = ((batch, n_tp, seg, d_model), BF16)
    for key in WIDE:
        shape = outs['out_' + key][0] if key != 'dy' else x.shape
        outs['got_' + key] = ((3,) + shape[:-1] + (d_model // 2,), BF16)
    for key in NARROW:
        outs['got_' + key] = ((3,) + outs['out_' + key][0], BF16)
    n_any = len(outs)
    outs['small'] = ((4 * d_model // 128 + n_tp, 128), F32)
    outs['wo_half'] = ((2, 2, width // 2, d_model // 2), BF16)
    vmem = lambda *shape: pltpu.VMEM(shape, BF16)
    wide = lambda *shape: pltpu.VMEM(shape, F32)
    scratch = dict(wqkv=vmem(d_model, 3 * width), wo=vmem(width, d_model), wgl=vmem(d_model, 2 * ff), wout=vmem(ff, d_model), w_cols=vmem(2, n_cp, n_tp, quarter, width), w_now=vmem(n_tp, n_cp, quarter, width),
                   o_all=vmem(batch, n_tp, rows, width), x_all=vmem(batch, n_tp, rows, width), key_add=wide(batch, 1, rows), mask_all=wide(n_cp, batch, 1, rows),
                   bias_rows=wide(heads * rows, n_cp * rows), bias_cols=wide(n_cp, rows, heads * rows), ds_sum=wide(heads * rows, n_cp * rows), gate=wide(batch, rows, ff), lin=wide(batch, rows, ff))
    for key in ('xs0', 'x1s0', 'xs1', 'x1s1', 'ds1', 'dms1', 'ds0', 'dms0'):
        scratch[key] = vmem(batch, seg, d_model)
    for key in ('kv0', 'kv1', 'qdo0', 'qdo1'):
        scratch[key] = vmem(batch, n_cp, rows, 2 * width)
    for key in ('stats0', 'stats1'):
        scratch[key] = wide(batch, n_cp, 2 * heads, rows)
    for key in ('q0', 'q1', 'dq', 'x_col'):
        scratch[key] = vmem(batch, rows, width)
    for key in ('dga0', 'dga1', 'dgm0', 'dgm1'):
        scratch[key] = wide(1, d_model)
    scratch.update(o_own=vmem(2, batch, rows, width), wo_acc=wide(width, d_model), wo_in=wide(2, width, d_model // 2), wo_x=wide(2, width // 2, d_model // 2), sem_wo=dma((2, 2, 3)))
    for key, n in (('hbuf', d_model), ('ubuf', ff), ('gbuf', 2 * ff), ('qbuf', 3 * width), ('dybuf', d_model)):
        scratch[key] = vmem(2, rows, n)
    for key in ('o', 'out', 'gl', 'h', 'u', 'g', 'q', 'dy', 'deal_in'):
        scratch['sem_' + key] = dma((2,))
    scratch.update(sem_qkv=dma((3,)), sem_in=dma((batch + 3,)), sem_keep=dma((batch,)), sem_mask=dma((2, 3)), sem_deal=dma((2, 2, n_tp)), sem_share=dma((2, 2, 3)),
                   sem_wide=dma((2, len(WIDE), 3)), sem_narrow=dma((2, len(NARROW), 3)))
    for key in ('kv', 'qdo', 'stats'):
        scratch['sem_' + key] = dma((2, 2, 3, batch))
    for key in ('o', 'x'):
        scratch['sem_%sz' % key] = dma((2, batch, 3))
        scratch['sem_%sy' % key] = dma((2, batch, 4))
    for i, piece in enumerate(Ring.scratch(batch, seg, d_model)):
        scratch['ring_%d' % i] = piece
    result = pl.pallas_call(
        functools.partial(mega_kernel, list(ins) + list(outs) + list(scratch), heads),
        out_shape=tuple(jax.ShapeDtypeStruct(*v) for v in outs.values()),
        in_specs=[v[1] for v in ins.values()],
        out_specs=tuple([any_spec] * n_any + [VMEM_SPEC] * (len(outs) - n_any)),
        scratch_shapes=list(scratch.values()),
        compiler_params=comm_params(cid, 63),
        cost_estimate=cost(300),
        name='mega',
    )(*[v[0] for v in ins.values()])
    return dict(zip(outs, result))


def sums_kernel(small, g_attn, g_mlp, g_bias, stage, by_z, sem):
    _, z, y, pair, z_peer = tp_places()
    _, mate, across, _ = cp_places()
    meet([pair] + z_peer[1:], [mate, across])
    mine = small
    for k, (axis, peer) in enumerate((('cp', mate), ('cp', across), ('tp', pair))):
        copy = remote(mine, stage.at[2 * k], sem, (k,), axis, peer)
        copy.start()
        copy.wait()
        if k < 2:
            stage[2 * k + 1] = mine[:] + stage[2 * k]
            mine = stage.at[2 * k + 1]
        else:
            by_z[z] = mine[:] + stage[2 * k]
    copies = [remote(by_z.at[z], by_z.at[z], sem, (2 + j,), 'tp', z_peer[j]) for j in (1, 2, 3)]
    for copy in copies:
        copy.start()
    for copy in copies:
        copy.wait()
    total = by_z[0] + by_z[1] + by_z[2] + by_z[3]
    lanes = total.shape[1]
    n_lines = g_attn.shape[1] // lanes
    for i, ref in enumerate((g_attn, g_mlp)):
        for l in range(2):
            for k in range(n_lines):
                first = (2 * i + l) * n_lines + k
                ref[l:l + 1, k * lanes:(k + 1) * lanes] = total[first:first + 1]
    own = lax.broadcasted_iota(jnp.int32, (8, lanes), 0) == lax.axis_index('tp')
    g_bias[:] = jnp.sum(jnp.where(own, total[4 * n_lines:], 0.0), axis=0, keepdims=True)


def sums(small, d_model, cid):
    return pl.pallas_call(
        sums_kernel,
        out_shape=(jax.ShapeDtypeStruct((2, d_model), F32), jax.ShapeDtypeStruct((2, d_model), F32), jax.ShapeDtypeStruct((1, 128), F32)),
        in_specs=[VMEM_SPEC],
        out_specs=(VMEM_SPEC,) * 3,
        scratch_shapes=[pltpu.VMEM((5,) + small.shape, F32), pltpu.VMEM((4,) + small.shape, F32), pltpu.SemaphoreType.DMA((2, 6))],
        compiler_params=comm_params(cid, 4),
        cost_estimate=cost(10),
        name='sums',
    )(small)


def place_kernel(plan, n_out, *refs):
    n = len(plan)
    owns, mates, outs = refs[:n], refs[n:2 * n], refs[2 * n:2 * n + n_out]
    bufs, in_sem, out_sem = refs[2 * n + n_out:4 * n + n_out], refs[4 * n + n_out], refs[4 * n + n_out + 1]
    core = lax.rem(lax.axis_index('cp'), 2)
    loads = []
    for src, buf in zip(owns + mates, bufs):
        if len(src.shape) > len(buf.shape):
            src = src.at[plan[len(loads) % n][0]]
        loads.append(pltpu.make_async_copy(src, buf, in_sem.at[len(loads)]))
    for load in loads:
        load.start()
    stores = []
    for i, load in enumerate(loads):
        layer, by_rows, first_out, n_pieces = plan[i % n]
        which = core if i < n else 1 - core
        buf = bufs[i]
        load.wait()
        width = buf.shape[1] // n_pieces
        for p in range(n_pieces):
            src = buf if n_pieces == 1 else buf.at[:, pl.ds(p * width, width)]
            size = buf.shape[0] if by_rows else width
            window = pl.ds(pl.multiple_of(which * size, size), size)
            out = outs[first_out + p].at[layer]
            dst = out.at[window, :] if by_rows else out.at[:, window]
            stores.append(pltpu.make_async_copy(src, dst, out_sem.at[len(stores)]))
            stores[-1].start()
    for store in stores:
        store.wait()


def place(plan, owns, mates, out_shapes):
    n = len(plan)
    any_spec = pl.BlockSpec(memory_space=pl.ANY)
    n_stores = 2 * sum(p[3] for p in plan)
    return pl.pallas_call(
        functools.partial(place_kernel, plan, len(out_shapes)),
        out_shape=tuple(jax.ShapeDtypeStruct(s, BF16) for s in out_shapes),
        in_specs=[any_spec] * (2 * n),
        out_specs=tuple([any_spec] * len(out_shapes)),
        scratch_shapes=[pltpu.VMEM(a.shape[-2:], BF16) for a in list(owns) + list(mates)] + [pltpu.SemaphoreType.DMA((2 * n,)), pltpu.SemaphoreType.DMA((n_stores,))],
        compiler_params=pltpu.CompilerParams(vmem_limit_bytes=40 * MIB),
        name='place',
    )(*owns, *mates)


def solution(mesh):
    seq_spec = P(None, 'cp', None)
    col_spec = P(None, None, 'tp')
    row_spec = P(None, 'tp', None)
    weight_specs = (P(), P(), col_spec, col_spec, col_spec, row_spec, col_spec, col_spec, row_spec)

    def local_program(x_in, d_y, key_mask, rel_bias, g_attn, g_mlp, w_q, w_k, w_v, w_o, w_gate, w_lin, w_out):
        batch, rows, d_model = x_in.shape
        tokens = batch * rows
        n_layers = w_q.shape[0]
        n_buckets, heads = rel_bias.shape
        core = lax.rem(lax.axis_index('cp'), 2)
        half = d_model // 2

        m = mega(x_in, d_y, key_mask, rel_bias, g_attn, g_mlp, w_q, w_k, w_v, w_o, w_gate, w_lin, w_out, 0)

        def flat(array):
            return array.reshape(-1, array.shape[-1])

        def own_half(array):
            return lax.dynamic_slice_in_dim(array.reshape(tokens, d_model), core * half, half, axis=1)

        def grad(left, right, left_wide):
            a, b = [d_y if key == 'dy' else m['out_' + key] for key in (left, right)]
            a_g, b_g = flat(m['got_' + left]), flat(m['got_' + right])
            a, b = (own_half(a), flat(b)) if left_wide else (flat(a), own_half(b))
            return (dot_tn(a, b) + dot_tn(a_g, b_g)).astype(BF16)

        owns = [grad('h0', 'qkv0', True), grad('h1', 'qkv1', True), grad('m0', 'gl0', True), grad('m1', 'gl1', True), grad('u0', 'd0', False), grad('u1', 'dy', False)]
        owns += [m['wo_half'].reshape(n_layers, -1, half)]
        mates = [lax.ppermute(part, 'cp', [(0, 1), (1, 0), (2, 3), (3, 2)]) for part in owns]
        d_g_attn, d_g_mlp, d_rel = sums(m['small'], d_model, 1)
        plan = tuple((layer, by_rows, first, n) for by_rows, first, n in ((True, 0, 3), (True, 4, 2), (False, 6, 1), (False, 3, 1)) for layer in range(n_layers))
        grads = place(plan, owns + owns[-1:], mates + mates[-1:], [w.shape for w in (w_q, w_k, w_v, w_o, w_gate, w_lin, w_out)])
        return (m['out_dx'].reshape(batch, rows, d_model), d_rel.reshape(n_buckets, heads), d_g_attn, d_g_mlp) + tuple(grads)

    return jax.shard_map(local_program, mesh=mesh, in_specs=(seq_spec, seq_spec, P(None, 'cp'), P(None, 'tp')) + weight_specs, out_specs=(seq_spec, P(None, 'tp')) + weight_specs, check_vma=False)
```

```python
import functools
import itertools
import string

import jax
import jax.numpy as jnp
from jax import lax
from jax.experimental import pallas as pl
from jax.experimental.pallas import tpu as pltpu
from jax.sharding import PartitionSpec as P

NORM_EPS = 1e-6
MASK_NEG = -1e9
BF16 = jnp.bfloat16
F32 = jnp.float32
VMEM = pltpu.VMEM
MESH = pl.DeviceIdType.MESH
MIB = 2 ** 20
HEAD_DIM = 64
VMEM_SPEC = pl.BlockSpec(memory_space=pltpu.VMEM)
SMEM_SPEC = pl.BlockSpec(memory_space=pltpu.SMEM)


def rel_bucket(rel_pos):
    distance = jnp.minimum(jnp.abs(rel_pos), 128)
    distance_sq = distance * distance
    log_part = 8 + sum((distance_sq >= 64 * 2 ** power).astype(jnp.int32) for power in range(1, 8))
    return jnp.where(distance < 8, distance, log_part) + 16 * (rel_pos > 0).astype(jnp.int32)


def comm_params(cid, mib):
    return pltpu.CompilerParams(collective_id=cid, has_side_effects=True, vmem_limit_bytes=mib * MIB)


def cost(gflops):
    return pl.CostEstimate(flops=gflops * 1000 * MIB, bytes_accessed=8 * MIB, transcendentals=MIB)


def dot_nt(a, b):
    return lax.dot_general(a, b, (((1,), (1,)), ((), ())), preferred_element_type=F32)


def dot_nn(a, b):
    return lax.dot_general(a, b, (((1,), (0,)), ((), ())), preferred_element_type=F32)


def dot_tn(a, b):
    return lax.dot_general(a, b, (((0,), (0,)), ((), ())), preferred_element_type=F32)


def stack_heads(block, heads):
    wide = block.astype(F32)
    lane_head = lax.broadcasted_iota(jnp.int32, block.shape, 1) // HEAD_DIM
    return jnp.concatenate([jnp.where(lane_head == h, wide, 0.0).astype(BF16) for h in range(heads)], axis=0)


def pick_heads(stacked, heads, rows):
    lane_head = lax.broadcasted_iota(jnp.int32, (rows, stacked.shape[1]), 1) // HEAD_DIM
    out = stacked[:rows]
    for h in range(1, heads):
        out = jnp.where(lane_head == h, stacked[h * rows:(h + 1) * rows], out)
    return out


def cp_places():
    me = lax.axis_index('cp')
    mate = me + 1 - 2 * lax.rem(me, 2)
    across = lax.rem(me + 2, 4)
    diagonal = lax.rem(mate + 2, 4)
    return me, mate, across, diagonal


def rms_parts(x_f, gain):
    inv_rms = lax.rsqrt(jnp.mean(x_f * x_f, axis=-1, keepdims=True) + NORM_EPS)
    return (x_f * inv_rms * gain).astype(BF16)


GELU_C = 0.7978845608028654
GELU_A = 0.044715


def gelu_parts(x):
    t = jnp.tanh(GELU_C * (x + GELU_A * x * x * x))
    cdf = 0.5 * (1.0 + t)
    return x * cdf, cdf + 0.5 * x * (1.0 - t * t) * GELU_C * (1.0 + 3.0 * GELU_A * x * x)


Z_STEPS = (2, 1, 3)


def remote(src, dst, sem, at, axis, peer):
    return pltpu.make_async_remote_copy(src_ref=src, dst_ref=dst, send_sem=sem.at[(0,) + at], recv_sem=sem.at[(1,) + at], device_id={axis: peer}, device_id_type=MESH)


def tp_places():
    me = lax.axis_index('tp')
    z, y = me // 2, lax.rem(me, 2)
    pair = me + 1 - 2 * y
    return me, z, y, pair, [2 * lax.rem(z + j, 4) + y for j in range(4)]


def meet(tp_peers, cp_peers):
    barrier = pltpu.get_barrier_semaphore()
    for axis, peers in (('tp', tp_peers), ('cp', cp_peers)):
        for peer in peers:
            pl.semaphore_signal(barrier, inc=1, device_id={axis: peer}, device_id_type=MESH)
    pl.semaphore_wait(barrier, len(tp_peers) + len(cp_peers))


class Ring:
    def __init__(self, part, from_y, from_z, full, *sems):
        self.part, self.from_y, self.from_z, self.full = part, from_y, from_z, full
        self.sem_ys, self.sem_zs, self.sem_zg, self.sem_yg = sems
        _, self.z, self.y, self.pair, self.z_peer = tp_places()
        self.seg = self.y * 4 + self.z

    @staticmethod
    def scratch(batch, seg, d_model):
        dma = pltpu.SemaphoreType.DMA
        return [
            pltpu.VMEM((batch, 2, 4, seg, d_model), F32),
            pltpu.VMEM((batch, 4, seg, d_model), F32),
            pltpu.VMEM((batch, 3, seg, d_model), F32),
            pltpu.VMEM((batch, 8, seg, d_model), BF16),
            dma((2, batch)), dma((2, batch, 3)), dma((2, batch, 3)), dma((2, batch, 4)),
        ]

    def y_sum(self, b):
        return remote(self.part.at[b, 1 - self.y], self.from_y.at[b], self.sem_ys, (b,), 'tp', self.pair)

    def z_sum(self, b, j):
        return remote(self.part.at[b, self.y, lax.rem(self.z + j, 4)], self.from_z.at[b, j - 1], self.sem_zs, (b, j - 1), 'tp', self.z_peer[j])

    def z_gather(self, b, j):
        ref = self.full.at[b, self.seg]
        return remote(ref, ref, self.sem_zg, (b, j - 1), 'tp', self.z_peer[j])

    def y_gather(self, b, j):
        ref = self.full.at[b, self.y * 4 + lax.rem(self.z - j + 4, 4)]
        return remote(ref, ref, self.sem_yg, (b, j), 'tp', self.pair)

    def send_partial(self, b, partial):
        self.part[b] = partial.reshape(self.part.shape[1:])
        self.y_sum(b).start()

    def reduce_pair(self, b):
        self.y_sum(b).wait_recv()
        self.part[b, self.y] = self.part[b, self.y] + self.from_y[b]
        for j in Z_STEPS:
            self.z_sum(b, j).start()

    def reduced(self, b):
        for j in Z_STEPS:
            self.z_sum(b, j).wait_recv()
        return self.part[b, self.y, self.z] + self.from_z[b, 0] + self.from_z[b, 1] + self.from_z[b, 2]

    def publish(self, b, out):
        self.full[b, self.seg] = out
        for j in Z_STEPS:
            self.z_gather(b, j).start()
        self.y_gather(b, 0).start()

    def forward(self, b):
        for j in Z_STEPS:
            self.z_gather(b, j).wait_recv()
            self.y_gather(b, j).start()

    def arrive(self, b):
        for j in range(4):
            self.y_gather(b, j).wait_recv()
        self.y_sum(b).wait_send()
        for j in range(4):
            self.y_gather(b, j).wait_send()
        for j in Z_STEPS:
            self.z_sum(b, j).wait_send()
            self.z_gather(b, j).wait_send()

    def rows(self, b):
        return self.full[b].reshape(-1, self.full.shape[-1])


class Columns:
    def __init__(self, store, z_sem, y_sem):
        self.store, self.z_sem, self.y_sem = store, z_sem, y_sem
        self.me, self.z, self.y, self.pair, self.z_peer = tp_places()

    def z_gather(self, b, j):
        ref = self.store.at[b, self.me]
        return remote(ref, ref, self.z_sem, (b, j - 1), 'tp', self.z_peer[j])

    def y_gather(self, b, j):
        ref = self.store.at[b, 2 * lax.rem(self.z - j + 4, 4) + self.y]
        return remote(ref, ref, self.y_sem, (b, j), 'tp', self.pair)

    def publish(self, b, out):
        self.store[b, self.me] = out
        for j in Z_STEPS:
            self.z_gather(b, j).start()
        self.y_gather(b, 0).start()

    def forward(self, b):
        for j in Z_STEPS:
            self.z_gather(b, j).wait_recv()
            self.y_gather(b, j).start()

    def arrive(self, b):
        for j in range(4):
            self.y_gather(b, j).wait_recv()
        for j in range(4):
            self.y_gather(b, j).wait_send()
        for j in Z_STEPS:
            self.z_gather(b, j).wait_send()

    def rows(self, b):
        return jnp.concatenate([self.store[b, t] for t in range(self.store.shape[1])], axis=1)


class Trade:
    def __init__(self, store, sem, layer):
        self.store, self.sem, self.layer = store, sem, layer
        self.me, self.mate, self.across, self.diagonal = cp_places()

    def copy(self, b, r):
        ref = self.store.at[b, self.across if r == 2 else self.me]
        return remote(ref, ref, self.sem, (self.layer, r, b), 'cp', self.across if r == 1 else self.mate)

    def give(self, b):
        self.copy(b, 1).start()
        self.copy(b, 0).start()

    def pass_on(self, b):
        self.copy(b, 1).wait_recv()
        self.copy(b, 2).start()

    def take(self, b):
        self.copy(b, 0).wait_recv()
        self.copy(b, 2).wait_recv()

    def finish(self, b):
        for r in range(3):
            self.copy(b, r).wait_send()


class Wide:
    def __init__(self, src, dst, sem, index):
        self.src, self.dst, self.sem, self.index = src, dst, sem, index
        me, *self.peers = cp_places()
        mate, across, diagonal = self.peers
        self.peers = (mate, across, diagonal)
        self.core = lax.rem(me, 2)

    def copy(self, r, window):
        n = self.dst.shape[-1]
        want = self.core if r == 1 else 1 - self.core
        columns = pl.ds(pl.multiple_of(want * n, n), n)
        return remote(self.src.at[window].at[..., columns], self.dst.at[r].at[window], self.sem, (self.index, r), 'cp', self.peers[r])

    def give(self, b):
        for r in (1, 2, 0):
            self.copy(r, pl.ds(b, 1)).start()

    def pass_on(self):
        pass

    def finish(self):
        for r in range(3):
            self.copy(r, pl.ds(0, self.src.shape[0])).wait()


class Narrow:
    def __init__(self, dst, sem, index):
        self.src, self.dst, self.sem, self.index = dst.at[3], dst, sem, index
        _, self.mate, self.across, _ = cp_places()

    def copy(self, r, window):
        src = self.src if r < 2 else self.dst.at[1]
        return remote(src.at[window], self.dst.at[r].at[window], self.sem, (self.index, r), 'cp', self.across if r == 1 else self.mate)

    def give(self, b):
        for r in (1, 0):
            self.copy(r, pl.ds(b, 1)).start()

    def pass_on(self):
        every = pl.ds(0, self.src.shape[0])
        self.copy(1, every).wait_recv()
        self.copy(2, every).start()

    def finish(self):
        every = pl.ds(0, self.src.shape[0])
        self.copy(0, every).wait()
        self.copy(1, every).wait_send()
        self.copy(2, every).wait()


class Spill:
    def __init__(self, slots, sem, columns=None):
        self.slots, self.sem, self.columns = slots, sem, columns

    def copies(self, out, own, b):
        slot = lax.rem(b, 2)
        src = self.slots.at[slot]
        copies = [] if out is None else [pltpu.make_async_copy(src, out.at[b], self.sem.at[1, slot])]
        if self.columns is not None:
            src = src.at[:, self.columns]
        return copies + [pltpu.make_async_copy(src, own.at[3, b], self.sem.at[0, slot])]

    def put(self, out, own, b, value):
        self.slots[lax.rem(b, 2)] = value
        for copy in self.copies(out, own, b):
            copy.start()

    def wait(self, out, own, b):
        for copy in self.copies(out, own, b):
            copy.wait()


def norm_rows(rows, gain):
    return rms_parts(rows.astype(F32), gain)


def rms_pull(total, x_shard, gain, res, d_gain_ref):
    d_norm = total.astype(BF16).astype(F32)
    x_f = x_shard.astype(F32)
    inv_rms = lax.rsqrt(jnp.mean(x_f * x_f, axis=-1, keepdims=True) + NORM_EPS)
    normed = x_f * inv_rms
    d_gain_ref[:] += col_sum(d_norm * normed)
    d_normed = d_norm * gain
    d_x = inv_rms * (d_normed - normed * jnp.mean(d_normed * normed, axis=-1, keepdims=True))
    return (res.astype(F32) + d_x).astype(BF16)


def mlp_pull(d_u, gate, lin):
    d_u = d_u.astype(BF16).astype(F32)
    value, slope = gelu_parts(gate)
    return jnp.concatenate([(d_u * lin * slope).astype(BF16), (d_u * value).astype(BF16)], axis=1)


def row_sum(x):
    return jnp.sum(x, axis=1, keepdims=True)


def col_sum(x):
    return jnp.sum(x, axis=0, keepdims=True)


def row_max(x):
    return jnp.max(x, axis=1, keepdims=True)


def mask_row(mask_ref, b):
    return jnp.concatenate([mask_ref[c, b] for c in range(mask_ref.shape[0])], axis=1)


def attend(heads, q, kv, bias, mask):
    rows, width = q.shape
    scores = dot_nt(stack_heads(q, heads), kv[:, :width]) + bias + mask
    top = row_max(scores)
    probs = jnp.exp(scores - top)
    total = row_sum(probs)
    out = dot_nn(probs.astype(BF16), kv[:, width:]) / total
    return pick_heads(out, heads, rows).astype(BF16)


def attend_rows_back(heads, qdo, kv, bias, mask, ds_ref):
    rows, wide = qdo.shape
    width = wide // 2
    keys, vals = kv[:, :width], kv[:, width:]
    scores = dot_nt(stack_heads(qdo[:, :width], heads), keys) + bias + mask
    top = row_max(scores)
    unnorm = jnp.exp(scores - top)
    total = row_sum(unnorm)
    log_norm = top + jnp.log(total)
    probs = unnorm * (1.0 / total)
    d_probs = dot_nt(stack_heads(qdo[:, width:], heads), vals)
    row_dot = row_sum(probs * d_probs)
    lane = lax.broadcasted_iota(jnp.int32, (rows, rows), 1)
    table = jnp.zeros((rows, rows), F32)
    for h in range(heads):
        table = jnp.where(lane == h, log_norm[h * rows:(h + 1) * rows], table)
        table = jnp.where(lane == heads + h, row_dot[h * rows:(h + 1) * rows], table)
    d_scores = probs * (d_probs - row_dot)
    ds_ref[:] += d_scores
    d_q = dot_nn(d_scores.astype(BF16), keys)
    return pick_heads(d_q, heads, rows).astype(BF16), jnp.transpose(table)[:2 * heads]


def attend_cols_back(heads, own_kv, mask_col, bias_ref, qdo_of, stats_of):
    rows, wide = own_kv.shape
    width = wide // 2
    keys, vals = own_kv[:, :width], own_kv[:, width:]

    def block(src, acc):
        d_k, d_v = acc
        qdo, stats = qdo_of(src), stats_of(src)
        log_norm = jnp.concatenate([stats[h:h + 1] for h in range(heads)], axis=1)
        row_dot = jnp.concatenate([stats[heads + h:heads + h + 1] for h in range(heads)], axis=1)
        q_st = stack_heads(qdo[:, :width], heads)
        do_st = stack_heads(qdo[:, width:], heads)
        probs = jnp.exp(dot_nt(keys, q_st) + bias_ref[src] + mask_col - log_norm)
        d_scores = probs * (dot_nt(vals, do_st) - row_dot)
        return d_k + dot_nn(d_scores.astype(BF16), q_st), d_v + dot_nn(probs.astype(BF16), do_st)

    zero = jnp.zeros((rows, width), F32)
    d_k, d_v = lax.fori_loop(0, bias_ref.shape[0], block, (zero, zero))
    return jnp.concatenate([d_k, d_v], axis=1).astype(BF16)


def bias_tables(table_ref, me, rows_ref, cols_ref):
    n_buckets, heads = table_ref.shape
    rows = rows_ref.shape[0] // heads
    seq = rows_ref.shape[1]

    def strip(i, carry):
        first = pl.multiple_of(i * SUBLANES, SUBLANES)
        rel = lax.broadcasted_iota(jnp.int32, (SUBLANES, seq), 1) - lax.broadcasted_iota(jnp.int32, (SUBLANES, seq), 0) - me * rows - first
        for is_col in (False, True):
            buckets = rel_bucket(-rel if is_col else rel)
            vals = [jnp.zeros((SUBLANES, seq), F32) for _ in range(heads)]
            for k in range(n_buckets):
                hit = buckets == k
                vals = [jnp.where(hit, table_ref[k, h], v) for h, v in enumerate(vals)]
            for h, v in enumerate(vals):
                if is_col:
                    for q in range(seq // rows):
                        cols_ref[q, pl.ds(first, SUBLANES), h * rows:(h + 1) * rows] = v[:, q * rows:(q + 1) * rows]
                else:
                    rows_ref[pl.ds(pl.multiple_of(h * rows + first, SUBLANES), SUBLANES), :] = v
        return carry

    lax.fori_loop(0, rows // SUBLANES, strip, 0)


def bucket_sums(ds_ref, heads, lines_ref, me):
    rows, seq = ds_ref.shape[0] // heads, ds_ref.shape[1]
    rel = lax.broadcasted_iota(jnp.int32, (rows, seq), 1) - lax.broadcasted_iota(jnp.int32, (rows, seq), 0) - me * rows
    buckets = rel_bucket(rel)

    def step(k, carry):
        hit = buckets == k
        lines_ref[k] = jnp.concatenate([col_sum(jnp.where(hit, ds_ref[h * rows:(h + 1) * rows], 0.0)) for h in range(heads)], axis=0)
        return carry

    lax.fori_loop(0, lines_ref.shape[0], step, 0)
    totals = row_sum(jnp.concatenate([lines_ref[k] for k in range(lines_ref.shape[0])], axis=0))
    return jnp.transpose(jnp.broadcast_to(totals, (totals.shape[0],) * 2))[:1]


class Refs:
    pass


WIDE = ('h0', 'h1', 'm0', 'm1', 'dy', 'd0')
NARROW = ('u0', 'u1', 'gl0', 'gl1', 'qkv0', 'qkv1')
LANES = 128
SUBLANES = 8
LETTERS = string.ascii_letters
STEPS = '0302321222210111101101010101101101123'
ORDER = 'FaKGeCtbdqpHlkExvozmjiwshfuBJynDIcAgr'
GIVES = tuple(zip(('h0', 'dy', 'u0', 'm0', 'h1', 'u1', 'm1', 'gl1', 'd0', 'qkv1', 'gl0', 'qkv0'), map(LETTERS.index, 'demvxzABDGHJ')))


def mega_kernel(names, heads, *refs):
    r = Refs()
    for key, ref in zip(names, refs):
        setattr(r, key, ref)
    batch, n_seg, seg, d_model = r.x.shape
    rows = n_seg * seg
    ff = r.w_out.shape[1]
    width = heads * HEAD_DIM
    ring = Ring(*[getattr(r, 'ring_%d' % i) for i in range(8)])
    gather_o = Columns(r.o_all, r.sem_oz, r.sem_oy)
    gather_x = Columns(r.x_all, r.sem_xz, r.sem_xy)
    me, mate, across, diagonal = cp_places()
    tp_me = gather_o.me
    others = (mate, across, diagonal)
    my_columns = pl.ds(pl.multiple_of(tp_me * width, width), width)

    def weight(buf, sem, sources, layer):
        out, col = [], 0
        for i, src in enumerate(sources):
            n = src.shape[-1]
            out.append(pltpu.make_async_copy(src.at[layer], buf.at[:, pl.ds(col, n)] if len(sources) > 1 else buf, sem.at[i]))
            col += n
        return out

    weights = dict(qkv=(r.wqkv, r.sem_qkv, (r.w_q, r.w_k, r.w_v)), o=(r.wo, r.sem_o, (r.w_o,)), gl=(r.wgl, r.sem_gl, (r.w_gate, r.w_lin)), out=(r.wout, r.sem_out, (r.w_out,)))

    def load(key, layer):
        def go():
            for copy in weight(*weights[key], layer):
                copy.start()
        return go

    def loaded(key, layer):
        def go():
            for copy in weight(*weights[key], layer):
                copy.wait()
        return go

    chip, core = me // 2, lax.rem(me, 2)
    half = d_model // 2

    def half_of(which):
        return pl.ds(pl.multiple_of(which * half, half), half)

    def wo_send(l, step):
        src, dst, peer = (
            (r.wo_acc.at[:, half_of(1 - core)], r.wo_in.at[l], mate),
            (r.wo_in.at[l, pl.ds(pl.multiple_of((1 - chip) * (width // 2), SUBLANES), width // 2)], r.wo_x.at[l], across),
            (r.wo_half.at[l, chip], r.wo_half.at[l, chip], across))[step]
        return remote(src, dst, r.sem_wo, (l, step), 'cp', peer)

    def wo_first(l):
        return lambda: wo_send(l, 0).start()

    def wo_second(l):
        def go():
            wo_send(l, 0).wait()
            r.wo_in[l] = r.wo_in[l] + r.wo_acc[:, half_of(core)]
            wo_send(l, 1).start()
        return go

    def wo_third(l):
        def go():
            wo_send(l, 1).wait()
            mine = r.wo_in[l, pl.ds(pl.multiple_of(chip * (width // 2), SUBLANES), width // 2)]
            r.wo_half[l, chip] = (mine + r.wo_x[l]).astype(BF16)
            wo_send(l, 2).start()
        return go

    for key, layer in (('qkv', 0), ('o', 1), ('gl', 0), ('out', 0)):
        load(key, layer)()
    rows_in = [pltpu.make_async_copy(r.x.at[b], ring.full.at[b], r.sem_in.at[b]) for b in range(batch)]
    shards_in = [(r.x.at[:, ring.seg], r.xs0), (r.dy.at[:, ring.seg], r.ds1), (r.x_rows.at[:, :, my_columns], r.x_col)]
    shards_in = [pltpu.make_async_copy(src, dst, r.sem_in.at[batch + i]) for i, (src, dst) in enumerate(shards_in)]
    deal_own = [pltpu.make_async_copy(r.w_deal.at[l, me, :, my_columns], r.w_cols.at[l, me, tp_me], r.sem_deal_in.at[l]) for l in range(2)]
    for copy in rows_in + shards_in + deal_own:
        copy.start()
    r.key_add[:] = jnp.where(r.key_mask[:] > 0, 0.0, MASK_NEG).astype(F32)[:, None, :]
    peers = [lax.rem(tp_me + j, n_seg) for j in range(n_seg)]
    meet(peers[1:], others)
    masks = [remote(r.key_add, r.mask_all.at[me], r.sem_mask, (i,), 'cp', peer) for i, peer in enumerate(others)]
    for copy in masks:
        copy.start()
    r.mask_all[me] = r.key_add[:]

    def deal(l, j):
        window = pl.ds(pl.multiple_of(peers[j] * width, width), width)
        return remote(r.w_deal.at[l, me, :, window], r.w_cols.at[l, me, tp_me], r.sem_deal, (l, j), 'tp', peers[j])

    def share(l, i):
        ref = r.w_cols.at[l, across if i == 2 else me]
        return remote(ref, ref, r.sem_share, (l, i), 'cp', across if i == 1 else mate)

    for l in range(2):
        for j in range(1, n_seg):
            deal(l, j).start()

    def share_start(l):
        def go():
            for j in range(1, n_seg):
                deal(l, j).wait()
            deal_own[l].wait()
            share(l, 1).start()
            share(l, 0).start()
        return go

    def share_pass(l):
        def go():
            share(l, 1).wait_recv()
            share(l, 2).start()
        return go

    def shared(l):
        def go():
            share(l, 0).wait()
            share(l, 1).wait_send()
            share(l, 2).wait()
            for c in range(r.w_cols.shape[1]):
                for t in range(n_seg):
                    r.w_now[t, c] = r.w_cols[l, c, t]
        return go

    for ref in (r.ds_sum, r.dga0, r.dga1, r.dgm0, r.dgm1):
        ref[:] = jnp.zeros_like(ref)
    for copy in rows_in + shards_in:
        copy.wait()
    loaded('qkv', 0)()

    hold = dict(h=Spill(r.hbuf, r.sem_h, half_of(core)), u=Spill(r.ubuf, r.sem_u), gl=Spill(r.gbuf, r.sem_g), qkv=Spill(r.qbuf, r.sem_q))
    moves = {}
    for i, key in enumerate(WIDE):
        moves[key] = Wide(r.dy_rows if key == 'dy' else getattr(r, 'out_' + key), getattr(r, 'got_' + key), r.sem_wide, i)
    for i, key in enumerate(NARROW):
        moves[key] = Narrow(getattr(r, 'got_' + key), r.sem_narrow, i)
    kv = [Trade(store, r.sem_kv, l) for l, store in enumerate((r.kv0, r.kv1))]
    qdo = [Trade(store, r.sem_qdo, l) for l, store in enumerate((r.qdo0, r.qdo1))]
    q_own = (r.q0, r.q1)
    stats = (r.stats0, r.stats1)

    def send_stats(l, b, i):
        ref = stats[l].at[b, me]
        return remote(ref, ref, r.sem_stats, (l, i, b), 'cp', others[i])

    def places(key, l):
        tag = '%s%d' % (key, l)
        return getattr(r, 'out_' + tag, None), getattr(r, 'got_' + tag)

    def project(l, b, flat):
        h = norm_rows(flat, r.g_attn[l:l + 1])
        hold['h'].put(*places('h', l), b, h)
        qkv = dot_nn(h, r.wqkv[:]).astype(BF16)
        q_own[l][b] = qkv[:, :width]
        kv[l].store[b, me] = qkv[:, width:]
        kv[l].give(b)

    def stage_first(b):
        project(0, b, ring.rows(b))

    def stage_attend(l):
        def go(b):
            kv[l].take(b)
            pairs = kv[l].store[b].reshape(-1, 2 * width)
            o = attend(heads, q_own[l][b], pairs, r.bias_rows[:], mask_row(r.mask_all, b))
            gather_o.publish(b, o)
            r.o_own[l, b] = o
        return go

    def stage_columns(l):
        def go(b):
            gather_o.arrive(b)
            prod = dot_nn(gather_o.rows(b), r.w_now[:].reshape(d_model, width))
            gather_x.publish(b, (r.x_col[b].astype(F32) + prod).astype(BF16))
        return go

    def add_stage(res, dst):
        def go(b):
            total = ring.reduced(b)
            value = (res[b].astype(F32) + total).astype(BF16)
            dst[b] = value
            ring.publish(b, value)
        return go

    def pull_stage(x_shard, gain, l, res, dst, d_gain):
        def go(b):
            value = rms_pull(ring.reduced(b), x_shard[b], gain[l:l + 1], res[b], d_gain)
            if dst is not None:
                dst[b] = value
            ring.publish(b, value)
        return go

    def mlp_forward(l, b, shard):
        gather_x.arrive(b)
        window = pl.ds(pl.multiple_of(ring.seg * seg, seg), seg)
        shard[b] = jnp.concatenate([r.x_all[b, t, window] for t in range(n_seg)], axis=1)
        h2 = norm_rows(gather_x.rows(b), r.g_mlp[l:l + 1])
        hold['h'].put(*places('m', l), b, h2)
        both = dot_nn(h2, r.wgl[:])
        gate, lin = both[:, :ff], both[:, ff:]
        u = (gelu_parts(gate)[0] * lin).astype(BF16)
        hold['u'].put(*places('u', l), b, u)
        return gate, lin, u

    def stage_mlp0(b):
        gate, lin, u = mlp_forward(0, b, r.x1s0)
        r.gate[b] = gate
        r.lin[b] = lin
        ring.send_partial(b, dot_nn(u, r.wout[:]))

    def stage_next(b):
        ring.arrive(b)
        r.x_col[b] = ring.full[b, :, :, my_columns].reshape(rows, width)
        project(1, b, ring.rows(b))

    def dy_in(b):
        slot = lax.rem(b, 2)
        return pltpu.make_async_copy(r.dy_rows.at[b], r.dybuf.at[slot], r.sem_dy.at[slot])

    def dy_own(b):
        slot = lax.rem(b, 2)
        return pltpu.make_async_copy(r.dybuf.at[slot, :, half_of(core)], r.got_dy.at[3, b], r.sem_dy_own.at[slot])

    def mlp_backward(l, b, d, gate, lin, copies=()):
        dgl = mlp_pull(dot_nt(d, r.wout[:]), gate, lin)
        hold['gl'].put(*places('gl', l), b, dgl)
        for copy in copies:
            copy.wait()
        ring.send_partial(b, dot_nt(dgl, r.wgl[:]))

    def stage_mlp1(b):
        gate, lin, _ = mlp_forward(1, b, r.x1s1)
        dy_in(b).wait()
        dy_own(b).start()
        mlp_backward(1, b, r.dybuf[lax.rem(b, 2)], gate, lin)

    def keep(dst, b):
        copy = pltpu.make_async_copy(ring.full.at[b], dst.at[b], r.sem_keep.at[b])
        copy.start()
        return copy

    def stage_rows_back(l):
        def go(b):
            ring.arrive(b)
            d_mid = ring.rows(b)
            d_o = dot_nt(d_mid, r.wo[:]).astype(BF16)
            both = jnp.concatenate([q_own[l][b], d_o], axis=1)
            qdo[l].store[b, me] = both
            qdo[l].give(b)
            pairs = kv[l].store[b].reshape(-1, 2 * width)
            d_q, table = attend_rows_back(heads, both, pairs, r.bias_rows[:], mask_row(r.mask_all, b), r.ds_sum)
            stats[l][b, me] = table
            r.dq[b] = d_q
            for i in range(3):
                send_stats(l, b, i).start()
            d_wo = dot_tn(r.o_own[l, b], d_mid)

            @pl.when(b == 0)
            def _():
                r.wo_acc[:] = d_wo

            @pl.when(b > 0)
            def _():
                r.wo_acc[:] += d_wo
        return go

    def stage_cols_back(l):
        def go(b):
            qdo[l].take(b)
            for i in range(3):
                send_stats(l, b, i).wait_recv()
            mask_col = jnp.transpose(jnp.broadcast_to(r.key_add[b], (rows, rows)))[:, :1]
            d_kv = attend_cols_back(heads, kv[l].store[b, me], mask_col, r.bias_cols, lambda s: qdo[l].store[b, s], lambda s: stats[l][b, s])
            d_qkv = jnp.concatenate([r.dq[b], d_kv], axis=1)
            hold['qkv'].put(*places('qkv', l), b, d_qkv)
            ring.send_partial(b, dot_nt(d_qkv, r.wqkv[:]))
        return go

    def stage_mlp_back0(b):
        ring.arrive(b)
        copies = [keep(r.out_d0, b), pltpu.make_async_copy(ring.full.at[b, :, :, half_of(core)], r.got_d0.at[3, b], r.sem_d0.at[b])]
        copies[1].start()
        mlp_backward(0, b, ring.rows(b), r.gate[b], r.lin[b], copies)

    def stage_last(b):
        ring.arrive(b)
        keep(r.out_dx, b).wait()

    def by_columns(tag, l):
        return [('at' + tag, stage_attend(l)), ('', gather_o.forward), ('col' + tag, stage_columns(l)), ('', gather_x.forward)]

    def by_sum(tag, start, finish):
        return [(tag, start), ('', ring.reduce_pair), ('sum' + tag[-1], finish), ('', ring.forward)]

    stages = (
        [('first', stage_first), ('', kv[0].pass_on)] + by_columns('0', 0)
        + by_sum('mlp0', stage_mlp0, add_stage(r.x1s0, r.xs1))
        + [('next', stage_next), ('', kv[1].pass_on)] + by_columns('1', 1)
        + by_sum('mlp1', stage_mlp1, pull_stage(r.x1s1, r.g_mlp, 1, r.ds1, r.dms1, r.dgm1))
        + [('rows1', stage_rows_back(1)), ('', qdo[1].pass_on)]
        + by_sum('cols1', stage_cols_back(1), pull_stage(r.xs1, r.g_attn, 1, r.dms1, r.ds0, r.dga1))
        + by_sum('back0', stage_mlp_back0, pull_stage(r.x1s0, r.g_mlp, 0, r.ds0, r.dms0, r.dgm0))
        + [('rows0', stage_rows_back(0)), ('', qdo[0].pass_on)]
        + by_sum('cols0', stage_cols_back(0), pull_stage(r.xs0, r.g_attn, 0, r.dms0, None, r.dga0))
        + [('last', stage_last)])
    lags = list(itertools.accumulate(int(step) for step in STEPS))
    order = [LETTERS.index(letter) for letter in ORDER]
    lag_of = {tag: lag for (tag, _), lag in zip(stages, lags)}
    use = lambda tag: lag_of[tag]
    after = lambda tag: lag_of[tag] + batch

    def tables():
        bias_tables(r.rel_bias, me, r.bias_rows, r.bias_cols)
        for copy in masks:
            copy.wait()

    n_lines = d_model // LANES

    def count_buckets():
        r.by_z[ring.z, 4 * n_lines:] = jnp.where(lax.broadcasted_iota(jnp.int32, (n_seg, LANES), 0) == tp_me, bucket_sums(r.ds_sum, heads, r.lines, me), 0.0)

    def all_gather_z(j):
        ref = r.by_z.at[ring.z]
        return remote(ref, ref, r.sem_all, (j,), 'tp', ring.z_peer[j])

    def all_start():
        for i, ref in enumerate((r.dga0, r.dga1, r.dgm0, r.dgm1)):
            for k in range(n_lines):
                r.by_z[ring.z, i * n_lines + k:i * n_lines + k + 1] = ref[:, k * LANES:(k + 1) * LANES]
        for j in Z_STEPS:
            all_gather_z(j).start()

    def all_step(k):
        axis, peer = (('tp', ring.pair), ('cp', mate), ('cp', across))[k]
        return remote(r.stage.at[k], r.stage_in.at[k], r.sem_all, (4 + k,), axis, peer)

    def all_sum(k):
        all_step(k).wait()
        return r.stage[k] + r.stage_in[k]

    def all_next(k):
        def go():
            if k == 0:
                for j in Z_STEPS:
                    all_gather_z(j).wait()
                r.stage[k] = r.by_z[0] + r.by_z[1] + r.by_z[2] + r.by_z[3]
            else:
                r.stage[k] = all_sum(k - 1)
            all_step(k).start()
        return go

    def all_end():
        total = all_sum(2)
        for i, ref in enumerate((r.g_attn_out, r.g_mlp_out)):
            for l in range(2):
                for k in range(n_lines):
                    first = (2 * i + l) * n_lines + k
                    ref[l:l + 1, k * LANES:(k + 1) * LANES] = total[first:first + 1]
        own = lax.broadcasted_iota(jnp.int32, (n_seg, LANES), 0) == tp_me
        r.g_bias[:] = col_sum(jnp.where(own, total[4 * n_lines:], 0.0))

    once = [
        (use('at0'), tables), (use('mlp0'), loaded('gl', 0)), (use('mlp0'), loaded('out', 0)),
        (batch - 1, share_start(0)), (batch - 1, share_start(1)), (batch + 1, share_pass(0)), (use('col0'), shared(0)), (use('col0'), share_pass(1)), (use('col1'), shared(1)),
        (after('first'), load('qkv', 1)), (use('next'), loaded('qkv', 1)),
        (after('mlp0'), load('gl', 1)), (after('mlp0'), load('out', 1)), (use('mlp1'), loaded('gl', 1)), (use('mlp1'), loaded('out', 1)),
        (after('mlp1'), load('gl', 0)), (after('mlp1'), load('out', 0)), (use('back0'), loaded('gl', 0)), (use('back0'), loaded('out', 0)),
        (use('rows1'), loaded('o', 1)), (after('rows1'), load('o', 0)), (use('rows0'), loaded('o', 0)),
        (after('cols1'), load('qkv', 0)), (use('cols0'), loaded('qkv', 0)),
        (after('rows1'), wo_first(1)), (after('rows1') + 1, wo_second(1)), (after('rows0'), wo_third(1)),
        (after('rows0'), wo_first(0)), (after('rows0'), count_buckets), (after('rows0') + 1, wo_second(0)),
        (after('sum0'), all_start), (after('sum0') + 1, all_next(0)), (after('sum0') + 2, all_next(1)), (after('sum0') + 3, all_next(2)),
        (len(lags) * batch, wo_third(0)), (len(lags) * batch, all_end),
    ]
    early = [(use(tag) + 1, hold[key], places(name, l)) for tag, key, name, l in (
        ('first', 'h', 'h', 0), ('mlp0', 'h', 'm', 0), ('mlp0', 'u', 'u', 0), ('next', 'h', 'h', 1), ('mlp1', 'h', 'm', 1), ('mlp1', 'u', 'u', 1), ('mlp1', 'gl', 'gl', 1),
        ('cols1', 'qkv', 'qkv', 1), ('back0', 'gl', 'gl', 0), ('cols0', 'qkv', 'qkv', 0))]
    gives = dict(GIVES)
    n_slots = batch + lags[-1]
    passes = [(n_slots - 3 if gives[key] + 2 * batch < n_slots else n_slots, moves[key].pass_on) for key in NARROW]

    def chunk_at(slot, lag, work):
        @pl.when(jnp.logical_and(slot >= lag, slot < batch + lag))
        def _():
            work(slot - lag)

    def slot_step(slot, carry):
        for at, work in once + passes:
            if at < n_slots:
                pl.when(slot == at)(work)
        for lag, spill, where in early:
            chunk_at(slot, lag, lambda b: spill.wait(*where, b))
        chunk_at(slot, use('mlp1') + 1, lambda b: dy_own(b).wait())
        chunk_at(slot, use('mlp1') - 1, lambda b: dy_in(b).start())
        for k in order:
            chunk_at(slot, lags[k], stages[k][1])
        for key, lag in GIVES:
            chunk_at(slot, lag, moves[key].give)
        return carry

    lax.fori_loop(0, n_slots, slot_step, 0)
    for at, work in sorted(passes + once, key=lambda entry: entry[0]):
        if at >= n_slots:
            work()

    def finish(b, carry):
        for l in range(2):
            kv[l].finish(b)
            qdo[l].finish(b)
            for i in range(3):
                send_stats(l, b, i).wait_send()
        return carry

    lax.fori_loop(0, batch, finish, 0)
    for key in WIDE + NARROW:
        moves[key].finish()
    for l, _ in enumerate(kv):
        wo_send(l, 2).wait()


def mega(x, dy, key_mask, rel_bias, g_attn, g_mlp, w_q, w_k, w_v, w_o, w_gate, w_lin, w_out, cid):
    batch, rows, d_model = x.shape
    heads = rel_bias.shape[1]
    width, ff = heads * HEAD_DIM, w_gate.shape[2]
    n_cp, n_tp = 4, 8
    seg = rows // n_tp
    quarter = width // n_cp
    dma = pltpu.SemaphoreType.DMA
    any_spec = pl.BlockSpec(memory_space=pl.ANY)
    by_seg = lambda a: a.reshape(batch, n_tp, seg, d_model)
    in_hbm = dict(x=by_seg(x), x_rows=x, dy=by_seg(dy), dy_rows=dy, w_q=w_q, w_k=w_k, w_v=w_v, w_o=w_o, w_deal=w_o.reshape(-1, n_cp, quarter, d_model), w_gate=w_gate, w_lin=w_lin, w_out=w_out)
    ins = {key: (value, any_spec) for key, value in in_hbm.items()}
    ins.update(key_mask=(key_mask, VMEM_SPEC), rel_bias=(rel_bias, SMEM_SPEC), g_attn=(g_attn, VMEM_SPEC), g_mlp=(g_mlp, VMEM_SPEC))
    size = dict(u=ff, gl=2 * ff, qkv=3 * width)
    outs = {}
    for key in ('h0', 'h1', 'm0', 'm1'):
        outs['out_' + key] = (x.shape, BF16)
    for key in ('d0', 'dx'):
        outs['out_' + key] = ((batch, n_tp, seg, d_model), BF16)
    for key in WIDE:
        shape = outs['out_' + key][0] if key != 'dy' else x.shape
        outs['got_' + key] = ((4,) + shape[:-1] + (d_model // 2,), BF16)
    for key in NARROW:
        outs['got_' + key] = ((4, batch, rows, size[key[:-1]]), BF16)
    n_any = len(outs)
    outs['g_attn_out'] = outs['g_mlp_out'] = (g_attn.shape, F32)
    outs['g_bias'] = ((1, LANES), F32)
    outs['wo_half'] = ((2, 2, width // 2, d_model // 2), BF16)
    vmem = lambda *shape: pltpu.VMEM(shape, BF16)
    wide = lambda *shape: pltpu.VMEM(shape, F32)
    scratch = dict(wqkv=vmem(d_model, 3 * width), wo=vmem(width, d_model), wgl=vmem(d_model, 2 * ff), wout=vmem(ff, d_model), w_cols=vmem(2, n_cp, n_tp, quarter, width), w_now=vmem(n_tp, n_cp, quarter, width),
                   o_all=vmem(batch, n_tp, rows, width), x_all=vmem(batch, n_tp, rows, width), key_add=wide(batch, 1, rows), mask_all=wide(n_cp, batch, 1, rows),
                   bias_rows=wide(heads * rows, n_cp * rows), bias_cols=wide(n_cp, rows, heads * rows), ds_sum=wide(heads * rows, n_cp * rows), gate=wide(batch, rows, ff), lin=wide(batch, rows, ff))
    for key in ('xs0', 'x1s0', 'xs1', 'x1s1', 'ds1', 'dms1', 'ds0', 'dms0'):
        scratch[key] = vmem(batch, seg, d_model)
    for key in ('kv0', 'kv1', 'qdo0', 'qdo1'):
        scratch[key] = vmem(batch, n_cp, rows, 2 * width)
    for key in ('stats0', 'stats1'):
        scratch[key] = wide(batch, n_cp, 2 * heads, rows)
    for key in ('q0', 'q1', 'dq', 'x_col'):
        scratch[key] = vmem(batch, rows, width)
    for key in ('dga0', 'dga1', 'dgm0', 'dgm1'):
        scratch[key] = wide(1, d_model)
    scratch.update(o_own=vmem(2, batch, rows, width), wo_acc=wide(width, d_model), wo_in=wide(2, width, d_model // 2), wo_x=wide(2, width // 2, d_model // 2), sem_wo=dma((2, 2, 3)))
    for key, n in (('hbuf', d_model), ('ubuf', ff), ('gbuf', 2 * ff), ('qbuf', 3 * width), ('dybuf', d_model)):
        scratch[key] = vmem(2, rows, n)
    for key in ('o', 'out', 'gl', 'dy', 'dy_own', 'deal_in'):
        scratch['sem_' + key] = dma((2,))
    for key in 'hugq':
        scratch['sem_' + key] = dma((2, 2))
    scratch.update(sem_qkv=dma((3,)), sem_in=dma((batch + 3,)), sem_keep=dma((batch,)), sem_d0=dma((batch,)), sem_mask=dma((2, 3)), sem_deal=dma((2, 2, n_tp)), sem_share=dma((2, 2, 3)),
                   sem_wide=dma((2, len(WIDE), 3)), sem_narrow=dma((2, len(NARROW), 3)))
    for key in ('kv', 'qdo', 'stats'):
        scratch['sem_' + key] = dma((2, 2, 3, batch))
    for key in ('o', 'x'):
        scratch['sem_%sz' % key] = dma((2, batch, 3))
        scratch['sem_%sy' % key] = dma((2, batch, 4))
    n_small = 4 * d_model // LANES + n_tp
    scratch.update(by_z=wide(4, n_small, LANES), stage=wide(3, n_small, LANES), stage_in=wide(3, n_small, LANES), sem_all=dma((2, 7)), lines=wide(rel_bias.shape[0], heads, n_cp * rows))
    for i, piece in enumerate(Ring.scratch(batch, seg, d_model)):
        scratch['ring_%d' % i] = piece
    result = pl.pallas_call(
        functools.partial(mega_kernel, list(ins) + list(outs) + list(scratch), heads),
        out_shape=tuple(jax.ShapeDtypeStruct(*v) for v in outs.values()),
        in_specs=[v[1] for v in ins.values()],
        out_specs=tuple([any_spec] * n_any + [VMEM_SPEC] * (len(outs) - n_any)),
        scratch_shapes=list(scratch.values()),
        compiler_params=comm_params(cid, 63),
        cost_estimate=cost(300),
        name='mega',
    )(*[v[0] for v in ins.values()])
    return dict(zip(outs, result))


def place_kernel(plan, n_out, *refs):
    n = len(plan)
    owns, mates, outs = refs[:n], refs[n:2 * n], refs[2 * n:2 * n + n_out]
    bufs, in_sem, out_sem = refs[2 * n + n_out:4 * n + n_out], refs[4 * n + n_out], refs[4 * n + n_out + 1]
    core = lax.rem(lax.axis_index('cp'), 2)
    loads = []
    for src, buf in zip(owns + mates, bufs):
        if len(src.shape) > len(buf.shape):
            src = src.at[plan[len(loads) % n][0]]
        loads.append(pltpu.make_async_copy(src, buf, in_sem.at[len(loads)]))
    for load in loads:
        load.start()
    stores = []
    for i, load in enumerate(loads):
        layer, by_rows, first_out, n_pieces = plan[i % n]
        which = core if i < n else 1 - core
        buf = bufs[i]
        load.wait()
        width = buf.shape[1] // n_pieces
        for p in range(n_pieces):
            src = buf if n_pieces == 1 else buf.at[:, pl.ds(p * width, width)]
            size = buf.shape[0] if by_rows else width
            window = pl.ds(pl.multiple_of(which * size, size), size)
            out = outs[first_out + p].at[layer]
            dst = out.at[window, :] if by_rows else out.at[:, window]
            stores.append(pltpu.make_async_copy(src, dst, out_sem.at[len(stores)]))
            stores[-1].start()
    for store in stores:
        store.wait()


def place(plan, owns, mates, out_shapes):
    n = len(plan)
    any_spec = pl.BlockSpec(memory_space=pl.ANY)
    n_stores = 2 * sum(p[3] for p in plan)
    return pl.pallas_call(
        functools.partial(place_kernel, plan, len(out_shapes)),
        out_shape=tuple(jax.ShapeDtypeStruct(s, BF16) for s in out_shapes),
        in_specs=[any_spec] * (2 * n),
        out_specs=tuple([any_spec] * len(out_shapes)),
        scratch_shapes=[pltpu.VMEM(a.shape[-2:], BF16) for a in list(owns) + list(mates)] + [pltpu.SemaphoreType.DMA((2 * n,)), pltpu.SemaphoreType.DMA((n_stores,))],
        compiler_params=pltpu.CompilerParams(vmem_limit_bytes=40 * MIB),
        name='place',
    )(*owns, *mates)


def solution(mesh):
    seq_spec = P(None, 'cp', None)
    col_spec = P(None, None, 'tp')
    row_spec = P(None, 'tp', None)
    weight_specs = (P(), P(), col_spec, col_spec, col_spec, row_spec, col_spec, col_spec, row_spec)

    def local_program(x_in, d_y, key_mask, rel_bias, g_attn, g_mlp, w_q, w_k, w_v, w_o, w_gate, w_lin, w_out):
        batch, rows, d_model = x_in.shape
        n_layers = w_q.shape[0]
        n_buckets, heads = rel_bias.shape
        half = d_model // 2
        m = mega(x_in, d_y, key_mask, rel_bias, g_attn, g_mlp, w_q, w_k, w_v, w_o, w_gate, w_lin, w_out, 0)

        def flat(key):
            array = m['got_' + key]
            return array.reshape(-1, array.shape[-1])

        owns = [dot_tn(flat(a), flat(b)).astype(BF16) for a, b in (('h0', 'qkv0'), ('h1', 'qkv1'), ('m0', 'gl0'), ('m1', 'gl1'), ('u0', 'd0'), ('u1', 'dy'))]
        owns += [m['wo_half'].reshape(n_layers, -1, half)]
        mates = [lax.ppermute(part, 'cp', [(0, 1), (1, 0), (2, 3), (3, 2)]) for part in owns]
        plan = tuple((layer, by_rows, first, n) for by_rows, first, n in ((True, 0, 3), (True, 4, 2), (False, 6, 1), (False, 3, 1)) for layer in range(n_layers))
        grads = place(plan, owns + owns[-1:], mates + mates[-1:], [w.shape for w in (w_q, w_k, w_v, w_o, w_gate, w_lin, w_out)])
        return (m['out_dx'].reshape(batch, rows, d_model), m['g_bias'].reshape(n_buckets, heads), m['g_attn_out'], m['g_mlp_out']) + tuple(grads)

    return jax.shard_map(local_program, mesh=mesh, in_specs=(seq_spec, seq_spec, P(None, 'cp'), P(None, 'tp')) + weight_specs, out_specs=(seq_spec, P(None, 'tp')) + weight_specs, check_vma=False)
```

```python
import functools
import itertools
import string

import jax
import jax.numpy as jnp
from jax import lax
from jax.experimental import pallas as pl
from jax.experimental.pallas import tpu as pltpu
from jax.sharding import PartitionSpec as P

NORM_EPS = 1e-6
MASK_NEG = -1e9
BF16 = jnp.bfloat16
F32 = jnp.float32
VMEM = pltpu.VMEM
MESH = pl.DeviceIdType.MESH
MIB = 2 ** 20
HEAD_DIM = 64
VMEM_SPEC = pl.BlockSpec(memory_space=pltpu.VMEM)
SMEM_SPEC = pl.BlockSpec(memory_space=pltpu.SMEM)


def rel_bucket(rel_pos):
    distance = jnp.minimum(jnp.abs(rel_pos), 128)
    distance_sq = distance * distance
    log_part = 8 + sum((distance_sq >= 64 * 2 ** power).astype(jnp.int32) for power in range(1, 8))
    return jnp.where(distance < 8, distance, log_part) + 16 * (rel_pos > 0).astype(jnp.int32)


def comm_params(cid, mib):
    return pltpu.CompilerParams(collective_id=cid, has_side_effects=True, vmem_limit_bytes=mib * MIB)


def cost(gflops):
    return pl.CostEstimate(flops=gflops * 1000 * MIB, bytes_accessed=8 * MIB, transcendentals=MIB)


def dot_nt(a, b):
    return lax.dot_general(a, b, (((1,), (1,)), ((), ())), preferred_element_type=F32)


def dot_nn(a, b):
    return lax.dot_general(a, b, (((1,), (0,)), ((), ())), preferred_element_type=F32)


def dot_tn(a, b):
    return lax.dot_general(a, b, (((0,), (0,)), ((), ())), preferred_element_type=F32)


def stack_heads(block, heads):
    wide = block.astype(F32)
    lane_head = lax.broadcasted_iota(jnp.int32, block.shape, 1) // HEAD_DIM
    return jnp.concatenate([jnp.where(lane_head == h, wide, 0.0).astype(BF16) for h in range(heads)], axis=0)


def pick_heads(stacked, heads, rows):
    lane_head = lax.broadcasted_iota(jnp.int32, (rows, stacked.shape[1]), 1) // HEAD_DIM
    out = stacked[:rows]
    for h in range(1, heads):
        out = jnp.where(lane_head == h, stacked[h * rows:(h + 1) * rows], out)
    return out


def cp_places():
    me = lax.axis_index('cp')
    mate = me + 1 - 2 * lax.rem(me, 2)
    across = lax.rem(me + 2, 4)
    diagonal = lax.rem(mate + 2, 4)
    return me, mate, across, diagonal


def rms_parts(x_f, gain):
    inv_rms = lax.rsqrt(jnp.mean(x_f * x_f, axis=-1, keepdims=True) + NORM_EPS)
    return (x_f * inv_rms * gain).astype(BF16)


GELU_C = 0.7978845608028654
GELU_A = 0.044715


def gelu_parts(x):
    t = jnp.tanh(GELU_C * (x + GELU_A * x * x * x))
    cdf = 0.5 * (1.0 + t)
    return x * cdf, cdf + 0.5 * x * (1.0 - t * t) * GELU_C * (1.0 + 3.0 * GELU_A * x * x)


Z_STEPS = (2, 1, 3)


def remote(src, dst, sem, at, axis, peer):
    return pltpu.make_async_remote_copy(src_ref=src, dst_ref=dst, send_sem=sem.at[(0,) + at], recv_sem=sem.at[(1,) + at], device_id={axis: peer}, device_id_type=MESH)


def tp_places():
    me = lax.axis_index('tp')
    z, y = me // 2, lax.rem(me, 2)
    pair = me + 1 - 2 * y
    return me, z, y, pair, [2 * lax.rem(z + j, 4) + y for j in range(4)]


def core_of(place):
    return lax.rem(place, 2)


def chip_of(place):
    return place // 2


def window_of(which, size):
    return pl.ds(pl.multiple_of(which * size, size), size)


def arrive_at(tp_peers, cp_peers):
    barrier = pltpu.get_barrier_semaphore()
    for axis, peers in (('tp', tp_peers), ('cp', cp_peers)):
        for peer in peers:
            pl.semaphore_signal(barrier, inc=1, device_id={axis: peer}, device_id_type=MESH)
    return barrier, len(tp_peers) + len(cp_peers)


class Ring:
    def __init__(self, part, from_y, from_z, full, *sems):
        self.part, self.from_y, self.from_z, self.full = part, from_y, from_z, full
        self.sem_ys, self.sem_zs, self.sem_zg, self.sem_yg = sems
        _, self.z, self.y, self.pair, self.z_peer = tp_places()
        self.seg = self.y * 4 + self.z

    @staticmethod
    def scratch(batch, seg, d_model):
        dma = pltpu.SemaphoreType.DMA
        return [
            pltpu.VMEM((batch, 2, 4, seg, d_model), F32),
            pltpu.VMEM((batch, 4, seg, d_model), F32),
            pltpu.VMEM((batch, 3, seg, d_model), F32),
            pltpu.VMEM((batch, 8, seg, d_model), BF16),
            dma((2, batch)), dma((2, batch, 3)), dma((2, batch, 3)), dma((2, batch, 4)),
        ]

    def y_sum(self, b):
        return remote(self.part.at[b, 1 - self.y], self.from_y.at[b], self.sem_ys, (b,), 'tp', self.pair)

    def z_sum(self, b, j):
        return remote(self.part.at[b, self.y, lax.rem(self.z + j, 4)], self.from_z.at[b, j - 1], self.sem_zs, (b, j - 1), 'tp', self.z_peer[j])

    def z_gather(self, b, j):
        ref = self.full.at[b, self.seg]
        return remote(ref, ref, self.sem_zg, (b, j - 1), 'tp', self.z_peer[j])

    def y_gather(self, b, j):
        ref = self.full.at[b, self.y * 4 + lax.rem(self.z - j + 4, 4)]
        return remote(ref, ref, self.sem_yg, (b, j), 'tp', self.pair)

    def send_partial(self, b, partial):
        self.part[b] = partial.reshape(self.part.shape[1:])
        self.y_sum(b).start()

    def reduce_pair(self, b):
        self.y_sum(b).wait_recv()
        self.part[b, self.y] = self.part[b, self.y] + self.from_y[b]
        for j in Z_STEPS:
            self.z_sum(b, j).start()

    def reduced(self, b):
        for j in Z_STEPS:
            self.z_sum(b, j).wait_recv()
        return self.part[b, self.y, self.z] + self.from_z[b, 0] + self.from_z[b, 1] + self.from_z[b, 2]

    def publish(self, b, out):
        self.full[b, self.seg] = out
        for j in Z_STEPS:
            self.z_gather(b, j).start()
        self.y_gather(b, 0).start()

    def forward(self, b):
        for j in Z_STEPS:
            self.z_gather(b, j).wait_recv()
            self.y_gather(b, j).start()

    def arrive(self, b):
        for j in range(4):
            self.y_gather(b, j).wait_recv()
        self.y_sum(b).wait_send()
        for j in range(4):
            self.y_gather(b, j).wait_send()
        for j in Z_STEPS:
            self.z_sum(b, j).wait_send()
            self.z_gather(b, j).wait_send()

    def rows(self, b):
        return self.full[b].reshape(-1, self.full.shape[-1])


class Columns:
    def __init__(self, store, z_sem, y_sem):
        self.store, self.z_sem, self.y_sem = store, z_sem, y_sem
        self.me, self.z, self.y, self.pair, self.z_peer = tp_places()

    def z_gather(self, b, j):
        ref = self.store.at[b, self.me]
        return remote(ref, ref, self.z_sem, (b, j - 1), 'tp', self.z_peer[j])

    def y_gather(self, b, j):
        ref = self.store.at[b, 2 * lax.rem(self.z - j + 4, 4) + self.y]
        return remote(ref, ref, self.y_sem, (b, j), 'tp', self.pair)

    def publish(self, b, out):
        self.store[b, self.me] = out
        for j in Z_STEPS:
            self.z_gather(b, j).start()
        self.y_gather(b, 0).start()

    def forward(self, b):
        for j in Z_STEPS:
            self.z_gather(b, j).wait_recv()
            self.y_gather(b, j).start()

    def arrive(self, b):
        for j in range(4):
            self.y_gather(b, j).wait_recv()
        for j in range(4):
            self.y_gather(b, j).wait_send()
        for j in Z_STEPS:
            self.z_gather(b, j).wait_send()

    def rows(self, b):
        return jnp.concatenate([self.store[b, t] for t in range(self.store.shape[1])], axis=1)


class Trade:
    def __init__(self, store, sem, layer):
        self.store, self.sem, self.layer = store, sem, layer
        self.me, self.mate, self.across, self.diagonal = cp_places()

    def copy(self, b, r):
        ref = self.store.at[b, self.across if r == 2 else self.me]
        return remote(ref, ref, self.sem, (self.layer, r, b), 'cp', self.across if r == 1 else self.mate)

    def give(self, b):
        self.copy(b, 1).start()
        self.copy(b, 0).start()

    def pass_on(self, b):
        self.copy(b, 1).wait_recv()
        self.copy(b, 2).start()

    def take(self, b):
        self.copy(b, 0).wait_recv()
        self.copy(b, 2).wait_recv()

    def finish(self, b):
        for r in range(3):
            self.copy(b, r).wait_send()


class Wide:
    def __init__(self, src, dst, sem, index):
        self.src, self.dst, self.sem, self.index = src, dst, sem, index
        me, mate, across, diagonal = cp_places()
        self.peers = (mate, across, diagonal, me)

    def columns(self, r):
        n = self.dst.shape[-1]
        core, chip = core_of(self.peers[r]), chip_of(self.peers[r])
        first = core * n if 2 * n == self.src.shape[-1] else (2 * core + chip) * n
        return pl.ds(pl.multiple_of(first, n), n)

    def copy(self, r, window):
        columns = self.columns(r)
        return remote(self.src.at[window].at[..., columns], self.dst.at[r].at[window], self.sem, (self.index, r), 'cp', self.peers[r])

    def give(self, b):
        for r in (1, 2, 0):
            self.copy(r, pl.ds(b, 1)).start()

    def pass_on(self):
        pass

    def finish(self):
        for r in range(3):
            self.copy(r, pl.ds(0, self.src.shape[0])).wait()


class Narrow:
    def __init__(self, dst, sem, index):
        self.src, self.dst, self.sem, self.index = dst.at[3], dst, sem, index
        _, self.mate, self.across, _ = cp_places()

    def copy(self, r, window):
        src = self.src if r < 2 else self.dst.at[1]
        return remote(src.at[window], self.dst.at[r].at[window], self.sem, (self.index, r), 'cp', self.across if r == 1 else self.mate)

    def give(self, b):
        for r in (1, 0):
            self.copy(r, pl.ds(b, 1)).start()

    def pass_on(self):
        every = pl.ds(0, self.src.shape[0])
        self.copy(1, every).wait_recv()
        self.copy(2, every).start()

    def finish(self):
        every = pl.ds(0, self.src.shape[0])
        self.copy(0, every).wait()
        self.copy(1, every).wait_send()
        self.copy(2, every).wait()


class Spill:
    def __init__(self, slots, sem, columns=None):
        self.slots, self.sem, self.columns = slots, sem, columns

    def copies(self, out, own, b):
        slot = lax.rem(b, 2)
        src = self.slots.at[slot]
        copies = [] if out is None else [pltpu.make_async_copy(src, out.at[b], self.sem.at[1, slot])]
        if self.columns is not None:
            src = src.at[:, self.columns]
        return copies + [pltpu.make_async_copy(src, own.at[3, b], self.sem.at[0, slot])]

    def put(self, out, own, b, value):
        self.slots[lax.rem(b, 2)] = value
        for copy in self.copies(out, own, b):
            copy.start()

    def wait(self, out, own, b):
        for copy in self.copies(out, own, b):
            copy.wait()


def norm_rows(rows, gain):
    return rms_parts(rows.astype(F32), gain)


def rms_pull(total, x_shard, gain, res, d_gain_ref):
    d_norm = total.astype(BF16).astype(F32)
    x_f = x_shard.astype(F32)
    inv_rms = lax.rsqrt(jnp.mean(x_f * x_f, axis=-1, keepdims=True) + NORM_EPS)
    normed = x_f * inv_rms
    d_gain_ref[:] += col_sum(d_norm * normed)
    d_normed = d_norm * gain
    d_x = inv_rms * (d_normed - normed * jnp.mean(d_normed * normed, axis=-1, keepdims=True))
    return (res.astype(F32) + d_x).astype(BF16)


def mlp_pull(d_u, gate, lin):
    d_u = d_u.astype(BF16).astype(F32)
    value, slope = gelu_parts(gate)
    return jnp.concatenate([(d_u * lin * slope).astype(BF16), (d_u * value).astype(BF16)], axis=1)


def row_sum(x):
    return jnp.sum(x, axis=1, keepdims=True)


def col_sum(x):
    return jnp.sum(x, axis=0, keepdims=True)


def row_max(x):
    return jnp.max(x, axis=1, keepdims=True)


def mask_row(mask_ref, b):
    return jnp.concatenate([mask_ref[c, b] for c in range(mask_ref.shape[0])], axis=1)


def attend(heads, q, kv, bias, mask):
    rows, width = q.shape
    scores = dot_nt(stack_heads(q, heads), kv[:, :width]) + bias + mask
    top = row_max(scores)
    probs = jnp.exp(scores - top)
    total = row_sum(probs)
    out = dot_nn(probs.astype(BF16), kv[:, width:]) / total
    return pick_heads(out, heads, rows).astype(BF16)


def attend_rows_back(heads, qdo, kv, bias, mask, ds_ref):
    rows, wide = qdo.shape
    width = wide // 2
    keys, vals = kv[:, :width], kv[:, width:]
    scores = dot_nt(stack_heads(qdo[:, :width], heads), keys) + bias + mask
    top = row_max(scores)
    unnorm = jnp.exp(scores - top)
    total = row_sum(unnorm)
    log_norm = top + jnp.log(total)
    probs = unnorm * (1.0 / total)
    d_probs = dot_nt(stack_heads(qdo[:, width:], heads), vals)
    row_dot = row_sum(probs * d_probs)
    lane = lax.broadcasted_iota(jnp.int32, (rows, rows), 1)
    table = jnp.zeros((rows, rows), F32)
    for h in range(heads):
        table = jnp.where(lane == h, log_norm[h * rows:(h + 1) * rows], table)
        table = jnp.where(lane == heads + h, row_dot[h * rows:(h + 1) * rows], table)
    d_scores = probs * (d_probs - row_dot)
    ds_ref[:] += d_scores
    d_q = dot_nn(d_scores.astype(BF16), keys)
    return pick_heads(d_q, heads, rows).astype(BF16), jnp.transpose(table)[:2 * heads]


def attend_cols_back(heads, own_kv, mask_col, bias_ref, qdo_of, stats_of):
    rows, wide = own_kv.shape
    width = wide // 2
    keys, vals = own_kv[:, :width], own_kv[:, width:]

    def block(src, acc):
        d_k, d_v = acc
        qdo, stats = qdo_of(src), stats_of(src)
        log_norm = jnp.concatenate([stats[h:h + 1] for h in range(heads)], axis=1)
        row_dot = jnp.concatenate([stats[heads + h:heads + h + 1] for h in range(heads)], axis=1)
        q_st = stack_heads(qdo[:, :width], heads)
        do_st = stack_heads(qdo[:, width:], heads)
        probs = jnp.exp(dot_nt(keys, q_st) + bias_ref[src] + mask_col - log_norm)
        d_scores = probs * (dot_nt(vals, do_st) - row_dot)
        return d_k + dot_nn(d_scores.astype(BF16), q_st), d_v + dot_nn(probs.astype(BF16), do_st)

    zero = jnp.zeros((rows, width), F32)
    d_k, d_v = lax.fori_loop(0, bias_ref.shape[0], block, (zero, zero))
    return jnp.concatenate([d_k, d_v], axis=1).astype(BF16)


def bias_tables(table_ref, me, rows_ref, cols_ref):
    n_buckets, heads = table_ref.shape
    rows = rows_ref.shape[0] // heads
    seq = rows_ref.shape[1]

    def strip(i, carry):
        first = pl.multiple_of(i * SUBLANES, SUBLANES)
        rel = lax.broadcasted_iota(jnp.int32, (SUBLANES, seq), 1) - lax.broadcasted_iota(jnp.int32, (SUBLANES, seq), 0) - me * rows - first
        for is_col in (False, True):
            buckets = rel_bucket(-rel if is_col else rel)
            vals = [jnp.zeros((SUBLANES, seq), F32) for _ in range(heads)]
            for k in range(n_buckets):
                hit = buckets == k
                vals = [jnp.where(hit, table_ref[k, h], v) for h, v in enumerate(vals)]
            for h, v in enumerate(vals):
                if is_col:
                    for q in range(seq // rows):
                        cols_ref[q, pl.ds(first, SUBLANES), h * rows:(h + 1) * rows] = v[:, q * rows:(q + 1) * rows]
                else:
                    rows_ref[pl.ds(pl.multiple_of(h * rows + first, SUBLANES), SUBLANES), :] = v
        return carry

    lax.fori_loop(0, rows // SUBLANES, strip, 0)


def bucket_sums(ds_ref, heads, lines_ref, me):
    rows, seq = ds_ref.shape[0] // heads, ds_ref.shape[1]
    rel = lax.broadcasted_iota(jnp.int32, (rows, seq), 1) - lax.broadcasted_iota(jnp.int32, (rows, seq), 0) - me * rows
    buckets = rel_bucket(rel)

    def step(k, carry):
        hit = buckets == k
        lines_ref[k] = jnp.concatenate([col_sum(jnp.where(hit, ds_ref[h * rows:(h + 1) * rows], 0.0)) for h in range(heads)], axis=0)
        return carry

    lax.fori_loop(0, lines_ref.shape[0], step, 0)
    totals = row_sum(jnp.concatenate([lines_ref[k] for k in range(lines_ref.shape[0])], axis=0))
    return jnp.transpose(jnp.broadcast_to(totals, (totals.shape[0],) * 2))[:1]


class Refs:
    pass


WIDE = ('h0', 'h1', 'm0', 'm1', 'dy', 'd0')
NARROW = ('u0', 'u1', 'gl0', 'gl1', 'qkv0', 'qkv1')
LANES = 128
LAYERS = (0, 1)
SUBLANES = 8
LETTERS = string.ascii_letters
STEPS = '0203322112010111110101012111110101212'
ORDER = 'byrvzgxDtqIajpoKlhFAGCwBfHeJnkdsEmuic'
GIVES = tuple(zip(('dy', 'h0', 'u0', 'h1', 'm0', 'm1', 'u1', 'qkv1', 'gl1', 'gl0', 'd0', 'qkv0'), map(LETTERS.index, 'flnruxyBDFHK')))


def mega_kernel(names, heads, *refs):
    r = Refs()
    for key, ref in zip(names, refs):
        setattr(r, key, ref)
    batch, n_seg, seg, d_model = r.x.shape
    rows = n_seg * seg
    ff = r.w_out.shape[1]
    width = heads * HEAD_DIM
    ring = Ring(*[getattr(r, 'ring_%d' % i) for i in range(8)])
    gather_o = Columns(r.o_all, r.sem_oz, r.sem_oy)
    gather_x = Columns(r.x_all, r.sem_xz, r.sem_xy)
    me, mate, across, diagonal = cp_places()
    tp_me = gather_o.me
    others = (mate, across, diagonal)
    my_columns = window_of(tp_me, width)

    def weight(buf, sem, sources, layer):
        out, col = [], 0
        for i, src in enumerate(sources):
            n = src.shape[-1]
            out.append(pltpu.make_async_copy(src.at[layer], buf.at[:, pl.ds(col, n)] if len(sources) > 1 else buf, sem.at[i]))
            col += n
        return out

    weights = dict(qkv=(r.wqkv, r.sem_qkv, (r.w_q, r.w_k, r.w_v)), o=(r.wo, r.sem_o, (r.w_o,)), gl=(r.wgl, r.sem_gl, (r.w_gate, r.w_lin)), out=(r.wout, r.sem_out, (r.w_out,)))

    def load(key, layer):
        def go():
            for copy in weight(*weights[key], layer):
                copy.start()
        return go

    def loaded(key, layer):
        def go():
            for copy in weight(*weights[key], layer):
                copy.wait()
        return go

    chip, core = chip_of(me), core_of(me)
    half = d_model // 2

    def half_of(which):
        return window_of(which, half)

    def wo_send(l, step):
        src, dst, peer = (
            (r.wo_acc.at[:, half_of(1 - core)], r.wo_in.at[l], mate),
            (r.wo_in.at[l, window_of(1 - chip, width // 2)], r.wo_x.at[l], across),
            (r.wo_half.at[l, chip], r.wo_half.at[l, chip], across))[step]
        return remote(src, dst, r.sem_wo, (l, step), 'cp', peer)

    def wo_first(l):
        return lambda: wo_send(l, 0).start()

    def wo_second(l):
        def go():
            wo_send(l, 0).wait()
            r.wo_in[l] = r.wo_in[l] + r.wo_acc[:, half_of(core)]
            wo_send(l, 1).start()
        return go

    def wo_third(l):
        def go():
            wo_send(l, 1).wait()
            mine = r.wo_in[l, window_of(chip, width // 2)]
            r.wo_half[l, chip] = (mine + r.wo_x[l]).astype(BF16)
            wo_send(l, 2).start()
        return go

    peers = [lax.rem(tp_me + j, n_seg) for j in range(n_seg)]
    barrier, n_peers = arrive_at(peers[1:], others)
    load('qkv', 0)()
    rows_in = [pltpu.make_async_copy(r.x.at[b], ring.full.at[b], r.sem_in.at[b]) for b in range(batch)]
    shards_in = [(r.x.at[:, ring.seg], r.xs0), (r.dy.at[:, ring.seg], r.ds1), (r.x_rows.at[:, :, my_columns], r.x_col)]
    shards_in = [pltpu.make_async_copy(src, dst, r.sem_in.at[batch + i]) for i, (src, dst) in enumerate(shards_in)]
    deal_own = [pltpu.make_async_copy(r.w_deal.at[l, me, :, my_columns], r.w_cols.at[l, me, tp_me], r.sem_deal_in.at[l]) for l in LAYERS]
    for copy in rows_in + shards_in + deal_own:
        copy.start()
    for key, layer in (('o', 1), ('gl', 0), ('out', 0)):
        load(key, layer)()
    r.key_add[:] = jnp.where(r.key_mask[:] > 0, 0.0, MASK_NEG).astype(F32)[:, None, :]
    for ref in (r.ds_sum, r.dga0, r.dga1, r.dgm0, r.dgm1):
        ref[:] = jnp.zeros_like(ref)
    bias_tables(r.rel_bias, me, r.bias_rows, r.bias_cols)
    pl.semaphore_wait(barrier, n_peers)
    masks = [remote(r.key_add, r.mask_all.at[me], r.sem_mask, (i,), 'cp', peer) for i, peer in enumerate(others)]
    for copy in masks:
        copy.start()
    r.mask_all[me] = r.key_add[:]

    def deal(l, j):
        window = window_of(peers[j], width)
        return remote(r.w_deal.at[l, me, :, window], r.w_cols.at[l, me, tp_me], r.sem_deal, (l, j), 'tp', peers[j])

    def share(l, i):
        ref = r.w_cols.at[l, across if i == 2 else me]
        return remote(ref, ref, r.sem_share, (l, i), 'cp', across if i == 1 else mate)

    for l in LAYERS:
        for j in range(1, n_seg):
            deal(l, j).start()

    def share_start(l):
        def go():
            for j in range(1, n_seg):
                deal(l, j).wait()
            deal_own[l].wait()
            share(l, 1).start()
            share(l, 0).start()
        return go

    def share_pass(l):
        def go():
            share(l, 1).wait_recv()
            share(l, 2).start()
        return go

    def shared(l):
        def go():
            share(l, 0).wait()
            share(l, 1).wait_send()
            share(l, 2).wait()
            for c in range(r.w_cols.shape[1]):
                for t in range(n_seg):
                    r.w_now[t, c] = r.w_cols[l, c, t]
        return go

    for copy in rows_in + shards_in:
        copy.wait()
    loaded('qkv', 0)()

    hold = dict(h=Spill(r.hbuf, r.sem_h, half_of(core)), u=Spill(r.ubuf, r.sem_u), gl=Spill(r.gbuf, r.sem_g), qkv=Spill(r.qbuf, r.sem_q))
    moves = {}
    for i, key in enumerate(WIDE):
        moves[key] = Wide(r.dy_rows if key == 'dy' else getattr(r, 'out_' + key), getattr(r, 'got_' + key), r.sem_wide, i)
    for i, key in enumerate(NARROW):
        moves[key] = Narrow(getattr(r, 'got_' + key), r.sem_narrow, i)
    kv = [Trade(store, r.sem_kv, l) for l, store in enumerate((r.kv0, r.kv1))]
    qdo = [Trade(store, r.sem_qdo, l) for l, store in enumerate((r.qdo0, r.qdo1))]
    q_own = (r.q0, r.q1)
    stats = (r.stats0, r.stats1)

    def send_stats(l, b, i):
        ref = stats[l].at[b, me]
        return remote(ref, ref, r.sem_stats, (l, i, b), 'cp', others[i])

    def places(key, l):
        tag = '%s%d' % (key, l)
        return getattr(r, 'out_' + tag, None), getattr(r, 'got_' + tag)

    def project(l, b, flat):
        h = norm_rows(flat, r.g_attn[l:l + 1])
        hold['h'].put(*places('h', l), b, h)
        qkv = dot_nn(h, r.wqkv[:]).astype(BF16)
        q_own[l][b] = qkv[:, :width]
        kv[l].store[b, me] = qkv[:, width:]
        kv[l].give(b)

    def stage_first(b):
        project(0, b, ring.rows(b))

    def stage_attend(l):
        def go(b):
            kv[l].take(b)
            pairs = kv[l].store[b].reshape(-1, 2 * width)
            o = attend(heads, q_own[l][b], pairs, r.bias_rows[:], mask_row(r.mask_all, b))
            gather_o.publish(b, o)
            r.o_own[l, b] = o
        return go

    def stage_columns(l):
        def go(b):
            gather_o.arrive(b)
            prod = dot_nn(gather_o.rows(b), r.w_now[:].reshape(d_model, width))
            gather_x.publish(b, (r.x_col[b].astype(F32) + prod).astype(BF16))
        return go

    def add_stage(res, dst):
        def go(b):
            total = ring.reduced(b)
            value = (res[b].astype(F32) + total).astype(BF16)
            dst[b] = value
            ring.publish(b, value)
        return go

    def pull_stage(x_shard, gain, l, res, dst, d_gain):
        def go(b):
            value = rms_pull(ring.reduced(b), x_shard[b], gain[l:l + 1], res[b], d_gain)
            if dst is not None:
                dst[b] = value
            ring.publish(b, value)
        return go

    def mlp_forward(l, b, shard):
        gather_x.arrive(b)
        window = window_of(ring.seg, seg)
        shard[b] = jnp.concatenate([r.x_all[b, t, window] for t in range(n_seg)], axis=1)
        h2 = norm_rows(gather_x.rows(b), r.g_mlp[l:l + 1])
        hold['h'].put(*places('m', l), b, h2)
        both = dot_nn(h2, r.wgl[:])
        gate, lin = both[:, :ff], both[:, ff:]
        u = (gelu_parts(gate)[0] * lin).astype(BF16)
        hold['u'].put(*places('u', l), b, u)
        return gate, lin, u

    def stage_mlp0(b):
        gate, lin, u = mlp_forward(0, b, r.x1s0)
        r.gate[b] = gate
        r.lin[b] = lin
        ring.send_partial(b, dot_nn(u, r.wout[:]))

    def stage_next(b):
        ring.arrive(b)
        r.x_col[b] = ring.full[b, :, :, my_columns].reshape(rows, width)
        project(1, b, ring.rows(b))

    def dy_in(b):
        slot = lax.rem(b, 2)
        return pltpu.make_async_copy(r.dy_rows.at[b], r.dybuf.at[slot], r.sem_dy.at[slot])

    def dy_own(b):
        slot = lax.rem(b, 2)
        return pltpu.make_async_copy(r.dybuf.at[slot, :, moves['dy'].columns(3)], r.got_dy.at[3, b], r.sem_dy_own.at[slot])

    def mlp_backward(l, b, d, gate, lin, copies=()):
        dgl = mlp_pull(dot_nt(d, r.wout[:]), gate, lin)
        hold['gl'].put(*places('gl', l), b, dgl)
        for copy in copies:
            copy.wait()
        ring.send_partial(b, dot_nt(dgl, r.wgl[:]))

    def stage_mlp1(b):
        gate, lin, _ = mlp_forward(1, b, r.x1s1)
        dy_in(b).wait()
        dy_own(b).start()
        mlp_backward(1, b, r.dybuf[lax.rem(b, 2)], gate, lin)

    def keep(dst, b):
        copy = pltpu.make_async_copy(ring.full.at[b], dst.at[b], r.sem_keep.at[b])
        copy.start()
        return copy

    def stage_rows_back(l):
        def go(b):
            ring.arrive(b)
            d_mid = ring.rows(b)
            d_o = dot_nt(d_mid, r.wo[:]).astype(BF16)
            both = jnp.concatenate([q_own[l][b], d_o], axis=1)
            qdo[l].store[b, me] = both
            qdo[l].give(b)
            pairs = kv[l].store[b].reshape(-1, 2 * width)
            d_q, table = attend_rows_back(heads, both, pairs, r.bias_rows[:], mask_row(r.mask_all, b), r.ds_sum)
            stats[l][b, me] = table
            r.dq[b] = d_q
            for i in range(3):
                send_stats(l, b, i).start()
            d_wo = dot_tn(r.o_own[l, b], d_mid)

            @pl.when(b == 0)
            def _():
                r.wo_acc[:] = d_wo

            @pl.when(b > 0)
            def _():
                r.wo_acc[:] += d_wo
        return go

    def stage_cols_back(l):
        def go(b):
            qdo[l].take(b)
            for i in range(3):
                send_stats(l, b, i).wait_recv()
            mask_col = jnp.transpose(jnp.broadcast_to(r.key_add[b], (rows, rows)))[:, :1]
            d_kv = attend_cols_back(heads, kv[l].store[b, me], mask_col, r.bias_cols, lambda s: qdo[l].store[b, s], lambda s: stats[l][b, s])
            d_qkv = jnp.concatenate([r.dq[b], d_kv], axis=1)
            hold['qkv'].put(*places('qkv', l), b, d_qkv)
            ring.send_partial(b, dot_nt(d_qkv, r.wqkv[:]))
        return go

    def stage_mlp_back0(b):
        ring.arrive(b)
        copies = [keep(r.out_d0, b), pltpu.make_async_copy(ring.full.at[b, :, :, moves['d0'].columns(3)], r.got_d0.at[3, b], r.sem_d0.at[b])]
        copies[1].start()
        mlp_backward(0, b, ring.rows(b), r.gate[b], r.lin[b], copies)

    def stage_last(b):
        ring.arrive(b)
        keep(r.out_dx, b).wait()

    def by_columns(tag, l):
        return [('at' + tag, stage_attend(l)), ('', gather_o.forward), ('col' + tag, stage_columns(l)), ('', gather_x.forward)]

    def by_sum(tag, start, finish):
        return [(tag, start), ('', ring.reduce_pair), ('sum' + tag[-1], finish), ('', ring.forward)]

    stages = (
        [('first', stage_first), ('', kv[0].pass_on)] + by_columns('0', 0)
        + by_sum('mlp0', stage_mlp0, add_stage(r.x1s0, r.xs1))
        + [('next', stage_next), ('', kv[1].pass_on)] + by_columns('1', 1)
        + by_sum('mlp1', stage_mlp1, pull_stage(r.x1s1, r.g_mlp, 1, r.ds1, r.dms1, r.dgm1))
        + [('rows1', stage_rows_back(1)), ('', qdo[1].pass_on)]
        + by_sum('cols1', stage_cols_back(1), pull_stage(r.xs1, r.g_attn, 1, r.dms1, r.ds0, r.dga1))
        + by_sum('back0', stage_mlp_back0, pull_stage(r.x1s0, r.g_mlp, 0, r.ds0, r.dms0, r.dgm0))
        + [('rows0', stage_rows_back(0)), ('', qdo[0].pass_on)]
        + by_sum('cols0', stage_cols_back(0), pull_stage(r.xs0, r.g_attn, 0, r.dms0, None, r.dga0))
        + [('last', stage_last)])
    lags = list(itertools.accumulate(int(step) for step in STEPS))
    order = [LETTERS.index(letter) for letter in ORDER]
    lag_of = {tag: lag for (tag, _), lag in zip(stages, lags)}
    use = lambda tag: lag_of[tag]
    after = lambda tag: lag_of[tag] + batch

    def masked():
        for copy in masks:
            copy.wait()

    n_lines = d_model // LANES

    def count_buckets():
        r.by_z[ring.z, 4 * n_lines:] = jnp.where(lax.broadcasted_iota(jnp.int32, (n_seg, LANES), 0) == tp_me, bucket_sums(r.ds_sum, heads, r.lines, me), 0.0)

    def all_gather_z(j):
        ref = r.by_z.at[ring.z]
        return remote(ref, ref, r.sem_all, (j,), 'tp', ring.z_peer[j])

    def all_start():
        for i, ref in enumerate((r.dga0, r.dga1, r.dgm0, r.dgm1)):
            for k in range(n_lines):
                r.by_z[ring.z, i * n_lines + k:i * n_lines + k + 1] = ref[:, k * LANES:(k + 1) * LANES]
        for j in Z_STEPS:
            all_gather_z(j).start()

    def all_step(k):
        axis, peer = (('tp', ring.pair), ('cp', mate), ('cp', across))[k]
        return remote(r.stage.at[k], r.stage_in.at[k], r.sem_all, (4 + k,), axis, peer)

    def all_sum(k):
        all_step(k).wait()
        return r.stage[k] + r.stage_in[k]

    def all_next(k):
        def go():
            if k == 0:
                for j in Z_STEPS:
                    all_gather_z(j).wait()
                r.stage[k] = r.by_z[0] + r.by_z[1] + r.by_z[2] + r.by_z[3]
            else:
                r.stage[k] = all_sum(k - 1)
            all_step(k).start()
        return go

    def all_end():
        total = all_sum(2)
        for i, ref in enumerate((r.g_attn_out, r.g_mlp_out)):
            for l in LAYERS:
                for k in range(n_lines):
                    first = (2 * i + l) * n_lines + k
                    ref[l:l + 1, k * LANES:(k + 1) * LANES] = total[first:first + 1]
        own = lax.broadcasted_iota(jnp.int32, (n_seg, LANES), 0) == tp_me
        r.g_bias[:] = col_sum(jnp.where(own, total[4 * n_lines:], 0.0))

    once = [
        (use('at0'), masked), (use('mlp0'), loaded('gl', 0)), (use('mlp0'), loaded('out', 0)),
        (batch + 1, share_start(0)), (batch + 1, share_start(1)), (batch + 3, share_pass(0)), (use('col0'), shared(0)), (after('col0'), share_pass(1)), (use('col1'), shared(1)),
        (after('first'), load('qkv', 1)), (use('next'), loaded('qkv', 1)),
        (after('mlp0'), load('gl', 1)), (after('mlp0'), load('out', 1)), (use('mlp1'), loaded('gl', 1)), (use('mlp1'), loaded('out', 1)),
        (after('mlp1'), load('gl', 0)), (after('mlp1'), load('out', 0)), (use('back0'), loaded('gl', 0)), (use('back0'), loaded('out', 0)),
        (use('rows1'), loaded('o', 1)), (after('rows1'), load('o', 0)), (use('rows0'), loaded('o', 0)),
        (after('cols1'), load('qkv', 0)), (use('cols0'), loaded('qkv', 0)),
        (after('rows1'), wo_first(1)), (after('rows1') + 1, wo_second(1)), (after('rows0'), wo_third(1)),
        (after('rows0'), wo_first(0)), (after('rows0'), count_buckets), (after('rows0') + 1, wo_second(0)),
        (after('sum0'), all_start), (after('sum0') + 1, all_next(0)), (after('sum0') + 2, all_next(1)), (after('sum0') + 3, all_next(2)),
        (len(lags) * batch, wo_third(0)), (len(lags) * batch, all_end),
    ]
    early = [(use(tag) + 1, hold[key], places(name, l)) for tag, key, name, l in (
        ('first', 'h', 'h', 0), ('mlp0', 'h', 'm', 0), ('mlp0', 'u', 'u', 0), ('next', 'h', 'h', 1), ('mlp1', 'h', 'm', 1), ('mlp1', 'u', 'u', 1), ('mlp1', 'gl', 'gl', 1),
        ('cols1', 'qkv', 'qkv', 1), ('back0', 'gl', 'gl', 0), ('cols0', 'qkv', 'qkv', 0))]
    gives = dict(GIVES)
    n_slots = batch + lags[-1]
    passes = [(n_slots - 3 if gives[key] + 2 * batch < n_slots else n_slots, moves[key].pass_on) for key in NARROW]

    def chunk_at(slot, lag, work):
        @pl.when(jnp.logical_and(slot >= lag, slot < batch + lag))
        def _():
            work(slot - lag)

    def slot_step(slot, carry):
        for at, work in once + passes:
            if at < n_slots:
                pl.when(slot == at)(work)
        for lag, spill, where in early:
            chunk_at(slot, lag, lambda b: spill.wait(*where, b))
        chunk_at(slot, use('mlp1') + 1, lambda b: dy_own(b).wait())
        chunk_at(slot, use('mlp1') - 1, lambda b: dy_in(b).start())
        for k in order:
            chunk_at(slot, lags[k], stages[k][1])
        for key, lag in GIVES:
            chunk_at(slot, lag, moves[key].give)
        return carry

    lax.fori_loop(0, n_slots, slot_step, 0)
    for at, work in sorted(passes + once, key=lambda entry: entry[0]):
        if at >= n_slots:
            work()

    def finish(b, carry):
        for l in LAYERS:
            kv[l].finish(b)
            qdo[l].finish(b)
            for i in range(3):
                send_stats(l, b, i).wait_send()
        return carry

    lax.fori_loop(0, batch, finish, 0)
    for key in WIDE + NARROW:
        moves[key].finish()
    for l, _ in enumerate(kv):
        wo_send(l, 2).wait()


def mega(x, dy, key_mask, rel_bias, g_attn, g_mlp, w_q, w_k, w_v, w_o, w_gate, w_lin, w_out, cid):
    batch, rows, d_model = x.shape
    heads = rel_bias.shape[1]
    width, ff = heads * HEAD_DIM, w_gate.shape[2]
    n_cp, n_tp = 4, 8
    seg = rows // n_tp
    quarter = width // n_cp
    dma = pltpu.SemaphoreType.DMA
    any_spec = pl.BlockSpec(memory_space=pl.ANY)
    by_seg = lambda a: a.reshape(batch, n_tp, seg, d_model)
    in_hbm = dict(x=by_seg(x), x_rows=x, dy=by_seg(dy), dy_rows=dy, w_q=w_q, w_k=w_k, w_v=w_v, w_o=w_o, w_deal=w_o.reshape(-1, n_cp, quarter, d_model), w_gate=w_gate, w_lin=w_lin, w_out=w_out)
    ins = {key: (value, any_spec) for key, value in in_hbm.items()}
    ins.update(key_mask=(key_mask, VMEM_SPEC), rel_bias=(rel_bias, SMEM_SPEC), g_attn=(g_attn, VMEM_SPEC), g_mlp=(g_mlp, VMEM_SPEC))
    size = dict(u=ff, gl=2 * ff, qkv=3 * width)
    outs = {}
    for key in ('h0', 'h1', 'm0', 'm1'):
        outs['out_' + key] = (x.shape, BF16)
    for key in ('d0', 'dx'):
        outs['out_' + key] = ((batch, n_tp, seg, d_model), BF16)
    for key in WIDE:
        shape = outs['out_' + key][0] if key != 'dy' else x.shape
        outs['got_' + key] = ((4,) + shape[:-1] + (d_model // (4 if key[0] == 'd' else 2),), BF16)
    for key in NARROW:
        outs['got_' + key] = ((4, batch, rows, size[key[:-1]]), BF16)
    n_any = len(outs)
    outs['g_attn_out'] = outs['g_mlp_out'] = (g_attn.shape, F32)
    outs['g_bias'] = ((1, LANES), F32)
    outs['wo_half'] = ((2, 2, width // 2, d_model // 2), BF16)
    vmem = lambda *shape: pltpu.VMEM(shape, BF16)
    wide = lambda *shape: pltpu.VMEM(shape, F32)
    scratch = dict(wqkv=vmem(d_model, 3 * width), wo=vmem(width, d_model), wgl=vmem(d_model, 2 * ff), wout=vmem(ff, d_model), w_cols=vmem(2, n_cp, n_tp, quarter, width), w_now=vmem(n_tp, n_cp, quarter, width),
                   o_all=vmem(batch, n_tp, rows, width), x_all=vmem(batch, n_tp, rows, width), key_add=wide(batch, 1, rows), mask_all=wide(n_cp, batch, 1, rows),
                   bias_rows=wide(heads * rows, n_cp * rows), bias_cols=wide(n_cp, rows, heads * rows), ds_sum=wide(heads * rows, n_cp * rows), gate=wide(batch, rows, ff), lin=wide(batch, rows, ff))
    for key in ('xs0', 'x1s0', 'xs1', 'x1s1', 'ds1', 'dms1', 'ds0', 'dms0'):
        scratch[key] = vmem(batch, seg, d_model)
    for key in ('kv0', 'kv1', 'qdo0', 'qdo1'):
        scratch[key] = vmem(batch, n_cp, rows, 2 * width)
    for key in ('stats0', 'stats1'):
        scratch[key] = wide(batch, n_cp, 2 * heads, rows)
    for key in ('q0', 'q1', 'dq', 'x_col'):
        scratch[key] = vmem(batch, rows, width)
    for key in ('dga0', 'dga1', 'dgm0', 'dgm1'):
        scratch[key] = wide(1, d_model)
    scratch.update(o_own=vmem(2, batch, rows, width), wo_acc=wide(width, d_model), wo_in=wide(2, width, d_model // 2), wo_x=wide(2, width // 2, d_model // 2), sem_wo=dma((2, 2, 3)))
    for key, n in (('hbuf', d_model), ('ubuf', ff), ('gbuf', 2 * ff), ('qbuf', 3 * width), ('dybuf', d_model)):
        scratch[key] = vmem(2, rows, n)
    for key in ('o', 'out', 'gl', 'dy', 'dy_own', 'deal_in'):
        scratch['sem_' + key] = dma((2,))
    for key in 'hugq':
        scratch['sem_' + key] = dma((2, 2))
    scratch.update(sem_qkv=dma((3,)), sem_in=dma((batch + 3,)), sem_keep=dma((batch,)), sem_d0=dma((batch,)), sem_mask=dma((2, 3)), sem_deal=dma((2, 2, n_tp)), sem_share=dma((2, 2, 3)),
                   sem_wide=dma((2, len(WIDE), 3)), sem_narrow=dma((2, len(NARROW), 3)))
    for key in ('kv', 'qdo', 'stats'):
        scratch['sem_' + key] = dma((2, 2, 3, batch))
    for key in ('o', 'x'):
        scratch['sem_%sz' % key] = dma((2, batch, 3))
        scratch['sem_%sy' % key] = dma((2, batch, 4))
    n_small = 4 * d_model // LANES + n_tp
    scratch.update(by_z=wide(4, n_small, LANES), stage=wide(3, n_small, LANES), stage_in=wide(3, n_small, LANES), sem_all=dma((2, 7)), lines=wide(rel_bias.shape[0], heads, n_cp * rows))
    for i, piece in enumerate(Ring.scratch(batch, seg, d_model)):
        scratch['ring_%d' % i] = piece
    result = pl.pallas_call(
        functools.partial(mega_kernel, list(ins) + list(outs) + list(scratch), heads),
        out_shape=tuple(jax.ShapeDtypeStruct(*v) for v in outs.values()),
        in_specs=[v[1] for v in ins.values()],
        out_specs=tuple([any_spec] * n_any + [VMEM_SPEC] * (len(outs) - n_any)),
        scratch_shapes=list(scratch.values()),
        compiler_params=comm_params(cid, 63),
        cost_estimate=cost(300),
        name='mega',
    )(*[v[0] for v in ins.values()])
    return dict(zip(outs, result))


def place_kernel(plan, n_out, *refs):
    n = len(plan)
    srcs, outs, bufs, in_sem, out_sem = refs[:n], refs[n:n + n_out], refs[n + n_out:2 * n + n_out], refs[2 * n + n_out], refs[2 * n + n_out + 1]
    me = lax.axis_index('cp')
    loads = []
    for src, buf, (_, layer, _, _, _) in zip(srcs, bufs, plan):
        if len(src.shape) > len(buf.shape):
            src = src.at[layer]
        loads.append(pltpu.make_async_copy(src, buf, in_sem.at[len(loads)]))
    for load in loads:
        load.start()
    stores = []
    for load, buf, (first_out, layer, flip, by_rows, n_pieces) in zip(loads, bufs, plan):
        load.wait()
        width = buf.shape[1] // n_pieces
        size = buf.shape[0] if by_rows else width
        owner = me + flip - 2 * core_of(me) * core_of(flip) - 4 * chip_of(me) * chip_of(flip)
        core, chip = core_of(owner), chip_of(owner)
        parts = outs[first_out].shape[1 if by_rows else 2] // size
        which = core if parts == 2 else 2 * core + chip
        window = window_of(which, size)
        for p in range(n_pieces):
            src = buf if n_pieces == 1 else buf.at[:, pl.ds(p * width, width)]
            out = outs[first_out + p].at[layer]
            stores.append(pltpu.make_async_copy(src, out.at[window, :] if by_rows else out.at[:, window], out_sem.at[len(stores)]))
            stores[-1].start()
    for store in stores:
        store.wait()


def place(plan, srcs, out_shapes):
    any_spec = pl.BlockSpec(memory_space=pl.ANY)
    dma = pltpu.SemaphoreType.DMA
    return pl.pallas_call(
        functools.partial(place_kernel, plan, len(out_shapes)),
        out_shape=tuple(jax.ShapeDtypeStruct(s, BF16) for s in out_shapes),
        in_specs=[any_spec] * len(srcs),
        out_specs=tuple([any_spec] * len(out_shapes)),
        scratch_shapes=[pltpu.VMEM(a.shape[-2:], BF16) for a in srcs] + [dma((len(srcs),)), dma((sum(p[-1] for p in plan),))],
        compiler_params=pltpu.CompilerParams(vmem_limit_bytes=40 * MIB),
        name='place',
    )(*srcs)


def solution(mesh):
    seq_spec = P(None, 'cp', None)
    col_spec = P(None, None, 'tp')
    row_spec = P(None, 'tp', None)
    weight_specs = (P(), P(), col_spec, col_spec, col_spec, row_spec, col_spec, col_spec, row_spec)

    def local_program(x_in, d_y, key_mask, rel_bias, g_attn, g_mlp, w_q, w_k, w_v, w_o, w_gate, w_lin, w_out):
        batch, rows, d_model = x_in.shape
        n_layers = w_q.shape[0]
        n_buckets, heads = rel_bias.shape
        half = d_model // 2
        m = mega(x_in, d_y, key_mask, rel_bias, g_attn, g_mlp, w_q, w_k, w_v, w_o, w_gate, w_lin, w_out, 0)

        def flat(key):
            array = m['got_' + key]
            return array.reshape(-1, array.shape[-1])

        def grad(left, right):
            return dot_tn(flat(left), flat(right)).astype(BF16)

        def swap(part, flip):
            return lax.ppermute(part, 'cp', [(c, c ^ flip) for c in range(4)])

        plan, srcs = [], []

        def put(result, layer, by_rows, pieces, part, across=False):
            held = [(0, part)] + ([(2, swap(part, 2))] if across else [])
            for flip, piece in held + [(flip + 1, swap(piece, 1)) for flip, piece in held]:
                plan.append((result, layer, flip, by_rows, pieces))
                srcs.append(piece)

        put(6, 1, False, 1, grad('u1', 'dy'), True)
        put(6, 0, False, 1, grad('u0', 'd0'), True)
        for layer in range(n_layers):
            put(4, layer, True, 2, grad('m%d' % layer, 'gl%d' % layer))
        for layer in range(n_layers):
            put(0, layer, True, 3, grad('h%d' % layer, 'qkv%d' % layer))
        wo = m['wo_half'].reshape(n_layers, -1, half)
        for flip, part in ((0, wo), (1, swap(wo, 1))):
            for layer in range(n_layers):
                plan.append((3, layer, flip, False, 1))
                srcs.append(part)
        grads = place(tuple(plan), srcs, [w.shape for w in (w_q, w_k, w_v, w_o, w_gate, w_lin, w_out)])
        return (m['out_dx'].reshape(batch, rows, d_model), m['g_bias'].reshape(n_buckets, heads), m['g_attn_out'], m['g_mlp_out']) + tuple(grads)

    return jax.shard_map(local_program, mesh=mesh, in_specs=(seq_spec, seq_spec, P(None, 'cp'), P(None, 'tp')) + weight_specs, out_specs=(seq_spec, P(None, 'tp')) + weight_specs, check_vma=False)
```
